32 devices in a mesh: blk: 8 (over z, core), section: 4 (over y, x).
Axes of the slice: x: 2, y: 2, z: 4, core: 2. Of those that a mesh axis runs over, the one named last changes fastest.
Arguments:
- hidden: bfloat16 [4, 2048, 4096], P('section', 'blk'), parts along dimension 1, may hold values from -6 to 6
- exit_layer: int32 [4096], P('blk'), parts along dimension 0, may hold values from 1 to 2
- lengths: int32 [4096], P('blk'), parts along dimension 0, may hold values from 1 to 16, as said below
- kv_cache: bfloat16 [4, 2048, 16, 256], P('section', 'blk'), parts along dimension 1, may hold values from -256 to 256
- norm_gain: bfloat16 [4, 4096], P('section'), may hold values from 0.5 to 1.5
- w_qkv: bfloat16 [4, 4096, 1280], P('section'), may hold values from -0.0625 to 0.0625
- w_out: bfloat16 [4, 1024, 4096], P('section'), may hold values from -0.1875 to 0.1875
Outputs:
- settled: bfloat16 [4096, 8192], P('blk', 'section'), parts along dimension 0
The draws below stay inside these ranges and needn't reach their ends.
There are 8 independent parts, one for each index of `blk`. The reference program is written for one: setup_inputs(seed, part) draws one part's arguments, and reference() takes and returns one part's arrays. A program takes and returns all parts, laid end to end along the dimension named above; an argument that names none is the same for every part. Nothing has to cross between parts.
Inputs may be any that keep to these rules, and one draw needn't show every extreme that they name: `lengths`: some token has length 16.
All inputs are finite; a program needn't handle non-finite values.
Results may differ from the reference program's by a relative error of at most 0.03.
Values may be sent and summed in bfloat16 or wider, within the bound.
A program may use at most 64 MiB of HBM per device.

```python
import jax
import jax.numpy as jnp
from jax import lax

D = 8192
HD = 128
QH = 8
BLOCK = 64
MICRO = 8
CTX = 16
SHARDS = 2
LAYERS = 2
TOKENS = 512


def draw_exit_layer(key, part):
    count_key = jax.random.fold_in(key, 11)
    order_key = jax.random.fold_in(key, 13)
    depth_key = jax.random.fold_in(key, 14)
    counts = jax.random.randint(count_key, (MICRO,), BLOCK // 4, BLOCK // 2 + 1)
    scores = jax.random.randint(order_key, (MICRO, BLOCK), 0, 1 << 20) * BLOCK + jnp.arange(BLOCK)[None, :]
    ranking = jnp.argsort(jnp.argsort(scores, axis=1), axis=1)
    deeper = ranking < counts[:, None]
    depth = jax.random.randint(depth_key, (MICRO, BLOCK), 2, LAYERS + 1)
    return jnp.where(deeper, depth, 1).reshape(-1).astype(jnp.int32)


def draw_lengths(key, part):
    length_key = jax.random.fold_in(key, 21)
    forced_key = jax.random.fold_in(key, 22)
    drawn = jax.random.randint(length_key, (TOKENS,), 1, CTX + 1)
    forced = jax.random.randint(forced_key, (), 0, TOKENS)
    return jnp.where(jnp.arange(TOKENS) == forced, CTX, drawn).astype(jnp.int32)


def draw_kv_cache(key, part):
    keys_key = jax.random.fold_in(key, 31)
    values_key = jax.random.fold_in(key, 32)
    shape = (SHARDS * LAYERS, TOKENS // SHARDS, CTX, HD)
    keys = jax.random.truncated_normal(keys_key, -4.0, 4.0, shape, jnp.float32)
    values = jax.random.truncated_normal(values_key, -4.0, 4.0, shape, jnp.float32)
    return jnp.concatenate([keys, values], axis=-1).astype(jnp.bfloat16)


def steps_of(key, dims, cuts, low, largest):
    def one(dim, shards_of):
        draws = jax.random.uniform(jax.random.fold_in(jax.random.fold_in(key, 6), dim), (shards_of,), jnp.float32, low / len(cuts), largest / len(cuts))
        return jnp.repeat(jnp.exp(draws), dims[dim] // shards_of).reshape((-1,) + (1,) * (len(dims) - dim - 1))

    loudness = one(*cuts[0])
    for cut in cuts[1:]:
        loudness = loudness * one(*cut)
    return loudness


def centred(stream_key, extent, spread, limit, shards=(), held_as=jnp.bfloat16):
    values = spread * jax.random.normal(stream_key, extent, jnp.float32)
    if shards:
        values = values * steps_of(stream_key, extent, shards, -0.22, 0.18)
    return jnp.clip(values, -limit, limit).astype(held_as)


def setup_inputs(seed: int = 0, part: int = 0) -> dict:
    arg_keys = jax.random.split(jax.random.key(seed), 8)
    own_keys = jax.random.split(jax.random.fold_in(arg_keys[7], part), 8)
    hidden = centred(own_keys[0], (SHARDS * LAYERS, TOKENS // LAYERS, D // SHARDS), 1.0, 6.0, ((0, 4),))
    exit_layer = draw_exit_layer(jax.random.fold_in(jax.random.fold_in(arg_keys[7], part), 71), part)
    lengths = draw_lengths(jax.random.fold_in(jax.random.fold_in(arg_keys[7], part), 71), part)
    kv_cache = draw_kv_cache(jax.random.fold_in(jax.random.fold_in(arg_keys[7], part), 71), part)
    norm_gain = jnp.clip(1.0 + 0.1 * jax.random.normal(arg_keys[4], (SHARDS * LAYERS, D // SHARDS), jnp.float32), 0.5, 1.5).astype(jnp.bfloat16)
    w_qkv = centred(arg_keys[5], (SHARDS * LAYERS, D // SHARDS, (QH + 2) * HD), D ** -0.5, 0.0625, ((0, 4),))
    w_out = centred(arg_keys[6], (SHARDS * LAYERS, QH * HD, D // SHARDS), (QH * HD) ** -0.5, 0.1875, ((0, 4),))
    return dict(hidden=hidden, exit_layer=exit_layer, lengths=lengths, kv_cache=kv_cache, norm_gain=norm_gain, w_qkv=w_qkv, w_out=w_out)


EPSILON = 1e-05
NEGATIVE = -1e+30

def attend(state, active, len_rows, cache_rows, gain_row, proj_weight, out_weight):
    query_width = out_weight.shape[0]
    head_size = (proj_weight.shape[1] - query_width) // 2
    heads = query_width // head_size
    rows = state.shape[0]
    context = cache_rows.shape[1]
    widened = state.astype(jnp.float32)
    scaled = (widened * gain_row.astype(jnp.float32)).astype(jnp.bfloat16)
    mean_square = lax.optimization_barrier(jnp.mean(widened * widened, axis=-1))
    projected = jnp.dot(scaled, proj_weight, preferred_element_type=jnp.float32) * lax.rsqrt(mean_square + EPSILON)[:, None]
    query = (projected[:, :query_width] * (1.0 / jnp.sqrt(jnp.float32(head_size)))).astype(jnp.bfloat16)
    query = query.reshape(rows, heads, head_size).astype(jnp.float32)
    key_new = projected[:, query_width:query_width + head_size].astype(jnp.bfloat16).astype(jnp.float32)
    value_new = projected[:, query_width + head_size:].astype(jnp.bfloat16).astype(jnp.float32)
    keys = cache_rows[:, :, :head_size].astype(jnp.float32)
    values = cache_rows[:, :, head_size:].astype(jnp.float32)
    scores = jnp.einsum('rhd,rcd->rhc', query, keys)
    own = jnp.einsum('rhd,rd->rh', query, key_new)
    positions = jnp.arange(context, dtype=jnp.int32)
    usable = (positions[None, :] < len_rows[:, None])[:, None, :]
    scores = jnp.where(usable, scores, NEGATIVE)
    row_top = jnp.maximum(lax.optimization_barrier(jnp.max(scores, axis=-1)), own)
    raw = jnp.where(usable, jnp.exp(scores - row_top[:, :, None]), jnp.float32(0.0))
    raw_own = jnp.exp(own - row_top)
    total = lax.optimization_barrier(jnp.sum(raw, axis=-1)) + raw_own
    weights = (raw / total[:, :, None]).astype(jnp.bfloat16).astype(jnp.float32)
    own_weight = (raw_own / total).astype(jnp.bfloat16).astype(jnp.float32)
    attended = jnp.einsum('rhc,rcd->rhd', weights, values) + own_weight[:, :, None] * value_new[:, None, :]
    attended = attended.astype(jnp.bfloat16).reshape(rows, query_width)
    branch_out = jnp.dot(attended, out_weight, preferred_element_type=jnp.float32)
    updated = (widened + branch_out).astype(jnp.bfloat16)
    return jnp.where(active[:, None], updated, state)

def reference(hidden, exit_layer, lengths, kv_cache, norm_gain, w_qkv, w_out):
    group = BLOCK // SHARDS
    span = D // (SHARDS * LAYERS)
    columns = w_qkv.shape[2]
    query_width = w_out.shape[1]
    width = kv_cache.shape[3]
    rounds = MICRO // LAYERS
    gains = norm_gain.reshape(LAYERS, SHARDS, LAYERS, span).transpose(0, 2, 1, 3).reshape(LAYERS, D)
    projections = w_qkv.reshape(LAYERS, SHARDS, LAYERS, span, columns).transpose(0, 2, 1, 3, 4).reshape(LAYERS, D, columns)
    outputs = w_out.reshape(LAYERS, SHARDS, query_width, LAYERS, span).transpose(0, 2, 3, 1, 4).reshape(LAYERS, query_width, D)
    cache = kv_cache.reshape(LAYERS, SHARDS, MICRO, group, CTX, width).transpose(0, 2, 1, 3, 4, 5).reshape(LAYERS, MICRO * BLOCK, CTX, width)
    arranged = hidden.reshape(LAYERS, SHARDS, rounds, BLOCK, LAYERS, span).transpose(2, 0, 3, 4, 1, 5).reshape(rounds, LAYERS, BLOCK, D)
    arranged = jnp.stack([arranged[:, (LAYERS - place) % LAYERS] for place in range(LAYERS)], axis=1)
    state = arranged.reshape(MICRO * BLOCK, D)
    for layer in range(LAYERS):
        state = attend(state, exit_layer > layer, lengths, cache[layer], gains[layer], projections[layer], outputs[layer])
    return state
```

```python
import functools
import math

import jax
import jax.numpy as jnp
from jax import lax
from jax.experimental import pallas as pl
from jax.experimental.pallas import tpu as pltpu
from jax.sharding import PartitionSpec as P

BLOCK = 64
MICRO = 8


EPSILON = 1e-05
NEGATIVE = -1e30
VMEM_LIMIT = 60 << 20


def partner(value, axis, distance):
    return lax.ppermute(value, axis, [(i, i ^ 1 << distance) for i in range(lax.axis_size(axis))])


def shifted(value, axis, steps):
    count = lax.axis_size(axis)
    pairs = [(source, (source + steps) % count) for source in range(count)]
    return lax.ppermute(value, axis, pairs)


def body(hidden, exit_layer, lengths, kv_cache, norm_gain, w_qkv, w_out):
    devices = lax.axis_size("section")
    index = lax.axis_index("section")
    shards = max(2, devices // 4)
    cycle_size = devices // shards
    segment_bits = cycle_size.bit_length() - 1
    shard_bits = shards.bit_length() - 1
    segment_index = index // shards
    shard_index = index % shards
    own_blocks = hidden[0]
    gain_row = norm_gain[0].astype(jnp.float32)
    proj_weight = w_qkv[0]
    out_weight = w_out[0]
    cache_all = kv_cache[0]
    query_width = out_weight.shape[0]
    head_size = (proj_weight.shape[1] - query_width) // 2
    heads = query_width // head_size
    quarter = proj_weight.shape[0]
    total_width = quarter * shards
    group_rows = BLOCK // shards
    rounds = MICRO // cycle_size
    context = cache_all.shape[1]
    positions = jnp.arange(context, dtype=jnp.int32)
    blank_block = jnp.zeros((BLOCK, quarter), jnp.bfloat16)

    def advance(carry, microstep):
        incoming, arriving, records = carry
        micro_index = microstep - segment_index
        in_range = (micro_index >= 0) & (micro_index < MICRO)
        slot = jnp.clip(micro_index, 0, MICRO - 1)
        on_turn = microstep % cycle_size == 0
        local_slot = jnp.minimum(microstep // cycle_size, rounds - 1)
        own_block = lax.dynamic_slice_in_dim(own_blocks, local_slot * BLOCK, BLOCK, 0)
        exit_rows = lax.dynamic_slice_in_dim(exit_layer, slot * BLOCK, BLOCK)
        own_lengths = lax.dynamic_slice_in_dim(
            lengths, slot * BLOCK + shard_index * group_rows, group_rows
        )
        own_cache = lax.dynamic_slice_in_dim(cache_all, slot * group_rows, group_rows, 0)
        first_input = jnp.where(on_turn, own_block, arriving)
        entering = jnp.where(segment_index == 0, first_input, incoming)
        active = exit_rows > segment_index
        gate = in_range & (jnp.sum(active.astype(jnp.int32)) > 0)

        def local_partials():
            widened = entering.astype(jnp.float32)
            scaled = (widened * gain_row).astype(jnp.bfloat16)
            return (
                jnp.dot(scaled, proj_weight, preferred_element_type=jnp.float32),
                jnp.sum(widened * widened, axis=1),
            )

        def no_partials():
            return (
                jnp.zeros((BLOCK, proj_weight.shape[1]), jnp.float32),
                jnp.zeros((BLOCK,), jnp.float32),
            )

        partial_proj, partial_squares = lax.cond(gate, local_partials, no_partials)
        kept = (partial_proj, partial_squares)
        for level in range(shard_bits):
            bit = shard_bits - 1 - level
            upper = index >> bit & 1
            halves = tuple(
                (piece.reshape((2, piece.shape[0] // 2) + piece.shape[1:]) for piece in kept)
            )
            keep = tuple((jnp.where(upper == 1, half[1], half[0]) for half in halves))
            send = tuple((jnp.where(upper == 1, half[0], half[1]) for half in halves))
            received = partner(send, "section", bit)
            kept = tuple((first + second for first, second in zip(keep, received)))
        own_proj, own_squares = kept

        def local_attention():
            fitted = own_proj * lax.rsqrt(own_squares / total_width + EPSILON)[:, None]
            query = (fitted[:, :query_width] * (1.0 / math.sqrt(head_size))).astype(jnp.bfloat16)
            query = query.reshape(group_rows, heads, head_size)
            key_new = fitted[:, query_width : query_width + head_size].astype(jnp.bfloat16)
            value_new = fitted[:, query_width + head_size :].astype(jnp.bfloat16)
            scores = jnp.einsum(
                "rhd,rcd->rhc",
                query,
                own_cache[:, :, :head_size],
                preferred_element_type=jnp.float32,
            )
            own = jnp.einsum("rhd,rd->rh", query, key_new, preferred_element_type=jnp.float32)
            usable = (positions[None, :] < own_lengths[:, None])[:, None, :]
            scores = jnp.where(usable, scores, NEGATIVE)
            row_top = jnp.maximum(jnp.max(scores, axis=-1), own)
            raw = jnp.where(usable, jnp.exp(scores - row_top[:, :, None]), jnp.float32(0.0))
            raw_own = jnp.exp(own - row_top)
            total = jnp.sum(raw, axis=-1) + raw_own
            weights = (raw / total[:, :, None]).astype(jnp.bfloat16)
            own_weight = (raw_own / total).astype(jnp.bfloat16)
            attended = jnp.einsum(
                "rhc,rcd->rhd",
                weights,
                own_cache[:, :, head_size:],
                preferred_element_type=jnp.float32,
            )
            attended = (
                attended
                + own_weight.astype(jnp.float32)[:, :, None]
                * value_new.astype(jnp.float32)[:, None, :]
            )
            return attended.astype(jnp.bfloat16).reshape(group_rows, query_width)

        def no_attention():
            return jnp.zeros((group_rows, query_width), jnp.bfloat16)

        collected = lax.cond(gate, local_attention, no_attention)
        for level in range(shard_bits):
            bit = level
            other = partner(collected, "section", bit)
            upper = index >> bit & 1
            collected = jnp.where(
                upper == 1,
                jnp.concatenate([other, collected], 0),
                jnp.concatenate([collected, other], 0),
            )

        def local_update():
            branch_out = jnp.dot(collected, out_weight, preferred_element_type=jnp.float32)
            updated = (entering.astype(jnp.float32) + branch_out).astype(jnp.bfloat16)
            return jnp.where(active[:, None], updated, entering)

        def keep_state():
            return entering

        outgoing = lax.cond(gate, local_update, keep_state)
        leaving = in_range & (exit_rows == segment_index + 1)
        previous = lax.dynamic_slice_in_dim(records, slot * BLOCK, BLOCK, 0)
        records = lax.dynamic_update_slice_in_dim(
            records, jnp.where(leaving[:, None], outgoing, previous), slot * BLOCK, 0
        )
        relayed = jnp.where(on_turn & (segment_index > 0), own_block, arriving)
        incoming, arriving = shifted((outgoing, relayed), "section", shards)
        return ((incoming, arriving, records), None)

    start = (blank_block, blank_block, jnp.zeros((MICRO * BLOCK, quarter), jnp.bfloat16))
    carry, _ = lax.scan(advance, start, jnp.arange(MICRO + cycle_size - 1, dtype=jnp.int32))
    kept = carry[2]
    for level in range(segment_bits):
        bit = shard_bits + segment_bits - 1 - level
        upper = index >> bit & 1
        halves = kept.reshape(kept.shape[0], 2, kept.shape[1] // 2)
        keep = jnp.where(upper == 1, halves[:, 1], halves[:, 0])
        send = jnp.where(upper == 1, halves[:, 0], halves[:, 1])
        received = partner(send, "section", bit)
        kept = (keep.astype(jnp.float32) + received.astype(jnp.float32)).astype(jnp.bfloat16)
    return kept


MESH = pl.DeviceIdType.MESH
CHUNKS = 2


def cycle_kernel(
    sizes,
    hidden,
    exits,
    lens,
    cache_hbm,
    gain,
    wq_hbm,
    wo_hbm,
    out,
    wq,
    wo,
    cache,
    stage,
    ready,
    table,
    scaled,
    partial,
    squares,
    psend,
    precv,
    att,
    wx,
    att_in,
    load_sem,
    own_sem,
    wy_send,
    wy_recv,
    up_send,
    up_recv,
    dn_send,
    dn_recv,
    wd_send,
    wd_recv,
    h_send,
    h_recv,
    lo_send,
    lo_recv,
    hi_send,
    hi_recv,
    p_send,
    p_recv,
    a_send,
    a_recv,
    r_send,
    r_recv,
    d_send,
    d_recv,
    x_send,
    x_recv,
):
    shards, head_size, heads = sizes
    index = lax.axis_index("section")
    seg = index // shards
    shard = index % shards
    across = seg * shards + (1 - shard)
    along = (1 - seg) * shards + shard
    corner = (1 - seg) * shards + (1 - shard)
    width = stage.shape[2]
    columns = wq.shape[1]
    query_width = heads * head_size
    half = MICRO // 2
    rows = BLOCK // shards
    span = out.shape[1]
    wide = wx.shape[1]
    low = width - wide
    context = cache.shape[1]
    own_rows = pl.ds(pl.multiple_of(shard * rows, rows), rows)
    other_rows = pl.ds(pl.multiple_of((1 - shard) * rows, rows), rows)

    place_blk = lax.axis_index("blk")
    chips = wd_send.shape[0]
    chip = place_blk // 2
    core = place_blk % 2
    chunk_rows = wx.shape[0] // (2 * chips * CHUNKS)
    above = jnp.minimum(chip + 1, chips - 1) * 2 + core
    below = jnp.maximum(chip - 1, 0) * 2 + core
    beside = chip * 2 + 1 - core
    has_above = chip < chips - 1
    has_below = chip > 0

    def remote(source, target, send, recv, device):
        return pltpu.make_async_remote_copy(
            src_ref=source,
            dst_ref=target,
            send_sem=send,
            recv_sem=recv,
            device_id=device,
            device_id_type=MESH,
        )

    barrier = pltpu.get_barrier_semaphore()
    for peer in (across, along, corner):
        pl.semaphore_signal(barrier, inc=1, device_id={"section": peer}, device_id_type=MESH)

    @pl.when(has_above)
    def _():
        pl.semaphore_signal(barrier, inc=1, device_id={"blk": above}, device_id_type=MESH)

    @pl.when(has_below)
    def _():
        pl.semaphore_signal(barrier, inc=1, device_id={"blk": below}, device_id_type=MESH)

    pl.semaphore_signal(barrier, inc=1, device_id={"blk": beside}, device_id_type=MESH)

    def own_copy(i):
        return pltpu.make_async_copy(
            hidden.at[pl.ds(i * BLOCK, BLOCK)], stage.at[i], own_sem.at[i]
        )

    def rest_copy(i):
        return pltpu.make_async_copy(
            hidden.at[pl.ds(i * BLOCK, BLOCK), pl.ds(low, wide)],
            stage.at[half + i, :, pl.ds(low, wide)],
            own_sem.at[i],
        )

    load_wq = pltpu.make_async_copy(wq_hbm, wq, load_sem.at[0])
    load_cache = pltpu.make_async_copy(cache_hbm, cache, load_sem.at[1])
    load_wo = pltpu.make_async_copy(wo_hbm, wo, load_sem.at[2])

    @pl.when(seg == 0)
    def _():
        own_copy(0).start()

    load_wq.start()
    load_cache.start()

    lane = lax.broadcasted_iota(jnp.int32, (128, 128), 1)
    line = lax.broadcasted_iota(jnp.int32, (128, 128), 0)
    for start in range(0, MICRO * BLOCK, 128):
        cols = pl.ds(start, 128)
        depth = jnp.sum(jnp.where(lane == line, exits[:, cols], 0), axis=1, keepdims=True)
        limit = jnp.sum(jnp.where(lane == line, lens[:, cols], 0), axis=1, keepdims=True)
        table[cols, :] = jnp.where(lane == 0, depth, limit)

    def place(i):
        return jnp.where(i < half, 2 * i, 2 * (i - half) + 1)

    def token_rows(i):
        return pl.ds(pl.multiple_of(place(i) * BLOCK, BLOCK), BLOCK)

    def depths(i):
        return table[token_rows(i), :][:, 0:1]

    def chunk_at(owner, chunk):
        first = pl.multiple_of(owner * (CHUNKS * chunk_rows) + chunk * chunk_rows, chunk_rows)
        return pl.ds(first, chunk_rows)

    def weight_out(layer, chunk):
        at = chunk_at(place_blk, chunk)
        first, size = (low, wide) if layer == 0 else (0, span)
        return remote(
            wo_hbm.at[at, pl.ds(first, size)],
            wx.at[at, pl.ds(0, size)],
            wy_send.at[chunk],
            wy_recv.at[chunk],
            {"section": along},
        )

    def held_size(layer):
        return pl.ds(0, wide if layer == 1 else span)

    def weight_in(layer, chunk):
        part = wx.at[chunk_at(place_blk, chunk), held_size(layer)]
        return remote(part, part, wy_send.at[chunk], wy_recv.at[chunk], {"section": along})

    def upward(layer, owner, chunk):
        part = wx.at[chunk_at(owner * 2 + core, chunk), held_size(layer)]
        return remote(
            part, part, up_send.at[owner, chunk], up_recv.at[owner, chunk], {"blk": above}
        )

    def downward(layer, owner, chunk):
        part = wx.at[chunk_at(owner * 2 + core, chunk), held_size(layer)]
        return remote(
            part, part, dn_send.at[owner, chunk], dn_recv.at[owner, chunk], {"blk": below}
        )

    def sideways(layer, owner, chunk, holder):
        part = wx.at[chunk_at(owner * 2 + holder, chunk), held_size(layer)]
        return remote(
            part, part, wd_send.at[owner, chunk], wd_recv.at[owner, chunk], {"blk": beside}
        )

    def spread(layer, chunk):
        weight_in(layer, chunk).wait_recv()

        @pl.when(has_above)
        def _():
            upward(layer, chip, chunk).start()

        @pl.when(has_below)
        def _():
            downward(layer, chip, chunk).start()

        sideways(layer, chip, chunk, core).start()

    def pass_on(layer, distance, chunk):
        @pl.when(chip >= distance)
        def _():
            upward(layer, chip - distance, chunk).wait_recv()

            @pl.when(has_above)
            def _():
                upward(layer, chip - distance, chunk).start()

            sideways(layer, chip - distance, chunk, core).start()

        @pl.when(chip + distance < chips)
        def _():
            downward(layer, chip + distance, chunk).wait_recv()

            @pl.when(has_below)
            def _():
                downward(layer, chip + distance, chunk).start()

            sideways(layer, chip + distance, chunk, core).start()

    def gathered(layer):
        for owner in range(chips):
            for chunk in range(CHUNKS):
                sideways(layer, owner, chunk, 1 - core).wait_recv()

    def settle_weights(layer):
        for chunk in range(CHUNKS):
            weight_out(layer, chunk).wait_send()
            for owner in range(chips):
                sideways(layer, owner, chunk, core).wait_send()

                @pl.when(has_above & (owner <= chip))
                def _():
                    upward(layer, owner, chunk).wait_send()

                @pl.when(has_below & (owner >= chip))
                def _():
                    downward(layer, owner, chunk).wait_send()

    def hidden_copy(i):
        return remote(
            hidden.at[pl.ds(i * BLOCK, BLOCK)],
            stage.at[half + i],
            h_send.at[i],
            h_recv.at[i],
            {"section": along},
        )

    def low_copy(i, size):
        return remote(
            ready.at[i, :, pl.ds(0, size)],
            stage.at[i, :, pl.ds(0, size)],
            lo_send.at[i],
            lo_recv.at[i],
            {"section": along},
        )

    def high_copy(i):
        cols = pl.ds(span, span)
        return remote(
            ready.at[i, :, cols],
            stage.at[i, :, cols],
            hi_send.at[i],
            hi_recv.at[i],
            {"section": along},
        )

    def branch_copy(i, sent_rows):
        return remote(
            att.at[i, sent_rows],
            att_in.at[i, sent_rows],
            r_send.at[i],
            r_recv.at[i],
            {"section": along},
        )

    def corner_copy(i, sent_rows):
        return remote(
            att.at[i, sent_rows],
            att_in.at[i, sent_rows],
            d_send.at[i],
            d_recv.at[i],
            {"section": corner},
        )

    def relay_copy(i, sent_rows):
        return remote(
            att_in.at[i, sent_rows],
            att_in.at[i, sent_rows],
            x_send.at[i],
            x_recv.at[i],
            {"section": across},
        )

    def partial_copy(i):
        return remote(
            psend.at[i], precv.at[i], p_send.at[i], p_recv.at[i], {"section": across}
        )

    def attended_copy(i, sent_rows):
        return remote(
            att.at[i, sent_rows],
            att.at[i, sent_rows],
            a_send.at[i],
            a_recv.at[i],
            {"section": across},
        )

    def scale(i, first, last):
        total = jnp.zeros((BLOCK, 1), jnp.float32)
        size = min(last - first, 512)
        for start in range(first, last, size):
            cols = pl.ds(start, size)
            piece = stage[i, :, cols].astype(jnp.float32)
            total = total + jnp.sum(piece * piece, axis=1, keepdims=True)
            scaled[:, cols] = (piece * gain[:, cols].astype(jnp.float32)).astype(jnp.bfloat16)
        return total

    def multiply(first, last, more):
        step = 512
        for start in range(0, columns, step):
            cols = pl.ds(start, min(step, columns - start))
            product = jnp.dot(
                scaled[:, pl.ds(first, last - first)],
                wq[pl.ds(first, last - first), cols],
                preferred_element_type=jnp.float32,
            )
            partial[:, cols] = partial[:, cols] + product if more else product

    def send_partial(i):
        psend[i, :, pl.ds(0, columns)] = partial[other_rows, :].astype(jnp.bfloat16)
        theirs = squares[other_rows, :]
        coarse = theirs.astype(jnp.bfloat16)
        fine = (theirs - coarse.astype(jnp.float32)).astype(jnp.bfloat16)
        psend[i, :, pl.ds(columns, 128)] = coarse
        psend[i, :, pl.ds(columns + 128, 128)] = fine
        partial_copy(i).start()

    def project(i):
        squares[...] = jnp.broadcast_to(scale(i, 0, width), squares.shape)
        multiply(0, width, False)
        send_partial(i)

    def attend_rows(i):
        partial_copy(i).wait_recv()
        coarse = precv[i, :, pl.ds(columns, 128)].astype(jnp.float32)
        fine = precv[i, :, pl.ds(columns + 128, 128)].astype(jnp.float32)
        total_squares = squares[own_rows, :] + coarse + fine
        factor = lax.rsqrt(total_squares / (width * shards) + EPSILON)[:, :1]
        fitted = (
            partial[own_rows, :] + precv[i, :, pl.ds(0, columns)].astype(jnp.float32)
        ) * factor
        scale = 1.0 / math.sqrt(head_size)
        query = jnp.concatenate(
            [fitted[:, h * head_size : (h + 1) * head_size] for h in range(heads)], axis=0
        )
        query = (query * scale).astype(jnp.bfloat16)
        key_new = fitted[:, query_width : query_width + head_size].astype(jnp.bfloat16)
        value_new = fitted[:, query_width + head_size :].astype(jnp.bfloat16)
        key_new = jnp.concatenate([key_new.astype(jnp.float32)] * heads, axis=0)
        value_new = jnp.concatenate([value_new.astype(jnp.float32)] * heads, axis=0)
        start = pl.multiple_of(place(i) * rows, rows)
        held = cache[pl.ds(start, rows)].reshape(rows * context, 2 * head_size)
        scores = lax.dot_general(
            query,
            held[:, :head_size],
            (((1,), (1,)), ((), ())),
            preferred_element_type=jnp.float32,
        )
        own = jnp.sum(query.astype(jnp.float32) * key_new, axis=1, keepdims=True)
        limits = table[pl.ds(pl.multiple_of(place(i) * BLOCK + shard * rows, rows), rows), :][:, 1:2]
        row = lax.broadcasted_iota(jnp.int32, (rows, 1), 0) * context
        first = jnp.concatenate([row] * heads, axis=0)
        last = jnp.concatenate([row + limits] * heads, axis=0)
        column = lax.broadcasted_iota(jnp.int32, scores.shape, 1)
        usable = (column >= first) & (column < last)
        scores = jnp.where(usable, scores, NEGATIVE)
        row_top = jnp.maximum(jnp.max(scores, axis=1, keepdims=True), own)
        raw = jnp.where(usable, jnp.exp(scores - row_top), 0.0)
        raw_own = jnp.exp(own - row_top)
        total = jnp.sum(raw, axis=1, keepdims=True) + raw_own
        weights = (raw / total).astype(jnp.bfloat16)
        own_weight = (raw_own / total).astype(jnp.bfloat16).astype(jnp.float32)
        attended = jnp.dot(
            weights, held[:, head_size:], preferred_element_type=jnp.float32
        )
        attended = (attended + own_weight * value_new).astype(jnp.bfloat16)
        att[i, own_rows, :] = jnp.concatenate(
            [attended[h * rows : (h + 1) * rows] for h in range(heads)], axis=1
        )

    def added(source, weight, before, chosen, target, first, last, shift_weight, shift):
        size = min(last - first, 512)
        for start in range(first, last, size):
            branch = jnp.dot(
                source,
                weight[:, pl.ds(start + shift_weight, size)],
                preferred_element_type=jnp.float32,
            )
            kept = before[:, pl.ds(start, size)].astype(jnp.float32)
            target[:, pl.ds(start + shift, size)] = jnp.where(
                chosen, kept + branch, kept
            ).astype(jnp.bfloat16)

    pl.semaphore_wait(
        barrier, 4 + has_above.astype(jnp.int32) + has_below.astype(jnp.int32)
    )

    def first_layer():
        for chunk in range(CHUNKS):
            weight_out(0, chunk).start()
        for i in range(1, half):
            own_copy(i).start()
        load_wo.start()

        def update(i):
            attended_copy(i, other_rows).wait_recv()
            active = depths(i) > 0
            fill = functools.partial(added, att[i], wo, stage.at[i], active, ready.at[i])
            fill(0, span, 0, 0)

            @pl.when(i < half)
            def _():
                low_copy(i, span).start()
                fill(span, width, 0, 0)
                high_copy(i).start()

            if low:

                @pl.when(i >= half)
                def _():
                    low_copy(i, low).start()

        def step(i, carry):
            @pl.when(i < MICRO)
            def _():
                @pl.when(i < half)
                def _():
                    own_copy(i).wait()

                @pl.when(i == half)
                def _():
                    for chunk in range(CHUNKS):
                        spread(0, chunk)

                @pl.when(i >= half)
                def _():
                    hidden_copy(i - half).wait_recv()

                for distance in range(1, chips - 1):

                    @pl.when(i == half + 1 + distance)
                    def _():
                        for chunk in range(CHUNKS):
                            pass_on(0, distance, chunk)

                @pl.when(i == 0)
                def _():
                    load_wq.wait()

                project(i)

            @pl.when(i == 1)
            def _():
                load_wo.wait()

            @pl.when(i > 0)
            def _():
                update(i - 1)

            @pl.when(i == 0)
            def _():
                load_cache.wait()

            @pl.when(i < MICRO)
            def _():
                attend_rows(i)
                attended_copy(i, own_rows).start()

                @pl.when(i >= half)
                def _():
                    branch_copy(i, own_rows).start()

            return carry

        lax.fori_loop(0, MICRO + 1, step, 0)
        for chunk in range(CHUNKS):
            pass_on(0, chips - 1, chunk)
        gathered(0)

        def finish(i, carry):
            branch_copy(i, own_rows).wait_recv()
            corner_copy(i, other_rows).wait_recv()
            added(
                att_in[i],
                wx,
                ready.at[i],
                depths(i) > 1,
                out.at[token_rows(i)],
                0,
                span,
                0,
                0,
            )
            return carry

        lax.fori_loop(0, MICRO, finish, 0)

        def drain(i, carry):
            partial_copy(i).wait_send()
            attended_copy(i, own_rows).wait_send()

            @pl.when(i < half)
            def _():
                low_copy(i, span).wait_send()
                high_copy(i).wait_send()

            @pl.when(i >= half)
            def _():
                branch_copy(i, own_rows).wait_send()
                if low:
                    low_copy(i, low).wait_send()

            return carry

        lax.fori_loop(0, MICRO, drain, 0)
        settle_weights(0)

    def second_layer():
        hidden_copy(0).start()
        for chunk in range(CHUNKS):
            weight_out(1, chunk).start()
        for i in range(1, half):
            hidden_copy(i).start()
        for i in range(half):
            rest_copy(i).start()
        load_wo.start()
        load_wq.wait()
        load_cache.wait()
        for chunk in range(CHUNKS):
            spread(1, chunk)

        def relay(i):
            branch_copy(i, own_rows).wait_recv()
            relay_copy(i, own_rows).start()

        def early(i):
            high_copy(i).wait_recv()
            low_copy(i, span).wait_recv()
            project(i)

        def late(i):
            rest_copy(i - half).wait()
            relay_copy(i, other_rows).wait_recv()
            added(
                att_in[i],
                wx,
                stage.at[i],
                depths(i) > 0,
                stage.at[i],
                low,
                width,
                -low,
                0,
            )
            total = scale(i, low, width)
            multiply(low, width, False)
            if low:
                low_copy(i, low).wait_recv()
                total = total + scale(i, 0, low)
                multiply(0, low, True)
            squares[...] = jnp.broadcast_to(total, squares.shape)
            send_partial(i)

        def update(i):
            attended_copy(i, other_rows).wait_recv()
            added(
                att[i],
                wo,
                stage.at[i],
                depths(i) > 1,
                out.at[token_rows(i)],
                span,
                width,
                0,
                -span,
            )

        def step(i, carry):
            for distance in range(1, chips):

                @pl.when(i == min(distance - 1, half - 1))
                def _():
                    for chunk in range(CHUNKS):
                        pass_on(1, distance, chunk)

            @pl.when(i < half)
            def _():
                early(i)

            @pl.when(i == half)
            def _():
                gathered(1)
                relay(half)

            @pl.when((i >= half) & (i < MICRO))
            def _():
                late(i)

            @pl.when((i >= half) & (i < MICRO - 1))
            def _():
                relay(i + 1)

            @pl.when(i == 1)
            def _():
                load_wo.wait()

            @pl.when(i > 0)
            def _():
                update(i - 1)

            @pl.when(i < MICRO)
            def _():
                attend_rows(i)
                corner_copy(i, own_rows).start()
                branch_copy(i, own_rows).start()
                attended_copy(i, own_rows).start()

            return carry

        lax.fori_loop(0, MICRO + 1, step, 0)

        def drain(i, carry):
            partial_copy(i).wait_send()
            attended_copy(i, own_rows).wait_send()
            branch_copy(i, own_rows).wait_send()
            corner_copy(i, own_rows).wait_send()

            @pl.when(i < half)
            def _():
                hidden_copy(i).wait_send()

            @pl.when(i >= half)
            def _():
                relay_copy(i, own_rows).wait_send()

            return carry

        lax.fori_loop(0, MICRO, drain, 0)
        settle_weights(1)

    @pl.when(seg == 0)
    def _():
        first_layer()

    @pl.when(seg == 1)
    def _():
        second_layer()


def cycle_of_two(chips, hidden, exit_layer, lengths, kv_cache, norm_gain, w_qkv, w_out):
    shards = 2
    width = w_qkv.shape[1]
    columns = w_qkv.shape[2]
    query_width = w_out.shape[1]
    head_size = (columns - query_width) // 2
    heads = query_width // head_size
    rows = BLOCK // shards
    span = width // 2
    wide = span + span // 2
    tokens = exit_layer.shape[0]
    hbm = pl.BlockSpec(memory_space=pltpu.HBM)
    vmem = pl.BlockSpec(memory_space=pltpu.VMEM)
    dma = pltpu.SemaphoreType.DMA((MICRO,))
    pieces = pltpu.SemaphoreType.DMA((chips, CHUNKS))
    bf16 = jnp.bfloat16
    return pl.pallas_call(
        functools.partial(cycle_kernel, (shards, head_size, heads)),
        out_shape=pltpu.VMEM((MICRO * BLOCK, span), bf16),
        in_specs=[hbm, vmem, vmem, hbm, vmem, hbm, hbm],
        out_specs=vmem,
        scratch_shapes=[
            pltpu.VMEM(w_qkv.shape[1:], bf16),
            pltpu.VMEM(w_out.shape[1:], bf16),
            pltpu.VMEM(kv_cache.shape[1:], bf16),
            pltpu.VMEM((MICRO, BLOCK, width), bf16),
            pltpu.VMEM((MICRO, BLOCK, width), bf16),
            pltpu.VMEM((MICRO * BLOCK, 128), jnp.int32),
            pltpu.VMEM((BLOCK, width), bf16),
            pltpu.VMEM((BLOCK, columns), jnp.float32),
            pltpu.VMEM((BLOCK, 128), jnp.float32),
            pltpu.VMEM((MICRO, rows, columns + 256), bf16),
            pltpu.VMEM((MICRO, rows, columns + 256), bf16),
            pltpu.VMEM((MICRO, BLOCK, query_width), bf16),
            pltpu.VMEM((query_width, wide), bf16),
            pltpu.VMEM((MICRO, BLOCK, query_width), bf16),
            pltpu.SemaphoreType.DMA((3,)),
            dma,
            pltpu.SemaphoreType.DMA((CHUNKS,)),
            pltpu.SemaphoreType.DMA((CHUNKS,)),
        ]
        + [pieces] * 6
        + [dma] * 16,
        compiler_params=pltpu.CompilerParams(
            collective_id=0, has_side_effects=True, vmem_limit_bytes=VMEM_LIMIT
        ),
        name="cycle",
    )(
        hidden[0],
        exit_layer.reshape(1, tokens),
        lengths.reshape(1, tokens),
        kv_cache[0],
        norm_gain,
        w_qkv[0],
        w_out[0],
    )


def chosen(batches, devices, *arguments):
    shards = max(2, devices // 4)
    if shards == 2 and devices // shards == 2:
        return cycle_of_two(batches // 2, *arguments)
    return body(*arguments)


def solution(mesh):
    return jax.shard_map(
        functools.partial(chosen, mesh.shape["blk"], mesh.shape["section"]),
        mesh=mesh,
        in_specs=(
            P("section", "blk", None),
            P("blk"),
            P("blk"),
            P("section", "blk", None, None),
            P("section", None),
            P("section", None, None),
            P("section", None, None),
        ),
        out_specs=P("blk", "section"),
        check_vma=False,
    )
```

```python
import functools
import math

import jax
import jax.numpy as jnp
from jax import lax
from jax.experimental import pallas as pl
from jax.experimental.pallas import tpu as pltpu
from jax.sharding import PartitionSpec as P

BLOCK = 64
MICRO = 8


EPSILON = 1e-05
NEGATIVE = -1e30
VMEM_LIMIT = 60 << 20


def partner(value, axis, distance):
    return lax.ppermute(value, axis, [(i, i ^ 1 << distance) for i in range(lax.axis_size(axis))])


def shifted(value, axis, steps):
    count = lax.axis_size(axis)
    pairs = [(source, (source + steps) % count) for source in range(count)]
    return lax.ppermute(value, axis, pairs)


def body(hidden, exit_layer, lengths, kv_cache, norm_gain, w_qkv, w_out):
    devices = lax.axis_size("section")
    index = lax.axis_index("section")
    shards = max(2, devices // 4)
    cycle_size = devices // shards
    segment_bits = cycle_size.bit_length() - 1
    shard_bits = shards.bit_length() - 1
    segment_index = index // shards
    shard_index = index % shards
    own_blocks = hidden[0]
    gain_row = norm_gain[0].astype(jnp.float32)
    proj_weight = w_qkv[0]
    out_weight = w_out[0]
    cache_all = kv_cache[0]
    query_width = out_weight.shape[0]
    head_size = (proj_weight.shape[1] - query_width) // 2
    heads = query_width // head_size
    quarter = proj_weight.shape[0]
    total_width = quarter * shards
    group_rows = BLOCK // shards
    rounds = MICRO // cycle_size
    context = cache_all.shape[1]
    positions = jnp.arange(context, dtype=jnp.int32)
    blank_block = jnp.zeros((BLOCK, quarter), jnp.bfloat16)

    def advance(carry, microstep):
        incoming, arriving, records = carry
        micro_index = microstep - segment_index
        in_range = (micro_index >= 0) & (micro_index < MICRO)
        slot = jnp.clip(micro_index, 0, MICRO - 1)
        on_turn = microstep % cycle_size == 0
        local_slot = jnp.minimum(microstep // cycle_size, rounds - 1)
        own_block = lax.dynamic_slice_in_dim(own_blocks, local_slot * BLOCK, BLOCK, 0)
        exit_rows = lax.dynamic_slice_in_dim(exit_layer, slot * BLOCK, BLOCK)
        own_lengths = lax.dynamic_slice_in_dim(
            lengths, slot * BLOCK + shard_index * group_rows, group_rows
        )
        own_cache = lax.dynamic_slice_in_dim(cache_all, slot * group_rows, group_rows, 0)
        first_input = jnp.where(on_turn, own_block, arriving)
        entering = jnp.where(segment_index == 0, first_input, incoming)
        active = exit_rows > segment_index
        gate = in_range & (jnp.sum(active.astype(jnp.int32)) > 0)

        def local_partials():
            widened = entering.astype(jnp.float32)
            scaled = (widened * gain_row).astype(jnp.bfloat16)
            return (
                jnp.dot(scaled, proj_weight, preferred_element_type=jnp.float32),
                jnp.sum(widened * widened, axis=1),
            )

        def no_partials():
            return (
                jnp.zeros((BLOCK, proj_weight.shape[1]), jnp.float32),
                jnp.zeros((BLOCK,), jnp.float32),
            )

        partial_proj, partial_squares = lax.cond(gate, local_partials, no_partials)
        kept = (partial_proj, partial_squares)
        for level in range(shard_bits):
            bit = shard_bits - 1 - level
            upper = index >> bit & 1
            halves = tuple(
                (piece.reshape((2, piece.shape[0] // 2) + piece.shape[1:]) for piece in kept)
            )
            keep = tuple((jnp.where(upper == 1, half[1], half[0]) for half in halves))
            send = tuple((jnp.where(upper == 1, half[0], half[1]) for half in halves))
            received = partner(send, "section", bit)
            kept = tuple((first + second for first, second in zip(keep, received)))
        own_proj, own_squares = kept

        def local_attention():
            fitted = own_proj * lax.rsqrt(own_squares / total_width + EPSILON)[:, None]
            query = (fitted[:, :query_width] * (1.0 / math.sqrt(head_size))).astype(jnp.bfloat16)
            query = query.reshape(group_rows, heads, head_size)
            key_new = fitted[:, query_width : query_width + head_size].astype(jnp.bfloat16)
            value_new = fitted[:, query_width + head_size :].astype(jnp.bfloat16)
            scores = jnp.einsum(
                "rhd,rcd->rhc",
                query,
                own_cache[:, :, :head_size],
                preferred_element_type=jnp.float32,
            )
            own = jnp.einsum("rhd,rd->rh", query, key_new, preferred_element_type=jnp.float32)
            usable = (positions[None, :] < own_lengths[:, None])[:, None, :]
            scores = jnp.where(usable, scores, NEGATIVE)
            row_top = jnp.maximum(jnp.max(scores, axis=-1), own)
            raw = jnp.where(usable, jnp.exp(scores - row_top[:, :, None]), jnp.float32(0.0))
            raw_own = jnp.exp(own - row_top)
            total = jnp.sum(raw, axis=-1) + raw_own
            weights = (raw / total[:, :, None]).astype(jnp.bfloat16)
            own_weight = (raw_own / total).astype(jnp.bfloat16)
            attended = jnp.einsum(
                "rhc,rcd->rhd",
                weights,
                own_cache[:, :, head_size:],
                preferred_element_type=jnp.float32,
            )
            attended = (
                attended
                + own_weight.astype(jnp.float32)[:, :, None]
                * value_new.astype(jnp.float32)[:, None, :]
            )
            return attended.astype(jnp.bfloat16).reshape(group_rows, query_width)

        def no_attention():
            return jnp.zeros((group_rows, query_width), jnp.bfloat16)

        collected = lax.cond(gate, local_attention, no_attention)
        for level in range(shard_bits):
            bit = level
            other = partner(collected, "section", bit)
            upper = index >> bit & 1
            collected = jnp.where(
                upper == 1,
                jnp.concatenate([other, collected], 0),
                jnp.concatenate([collected, other], 0),
            )

        def local_update():
            branch_out = jnp.dot(collected, out_weight, preferred_element_type=jnp.float32)
            updated = (entering.astype(jnp.float32) + branch_out).astype(jnp.bfloat16)
            return jnp.where(active[:, None], updated, entering)

        def keep_state():
            return entering

        outgoing = lax.cond(gate, local_update, keep_state)
        leaving = in_range & (exit_rows == segment_index + 1)
        previous = lax.dynamic_slice_in_dim(records, slot * BLOCK, BLOCK, 0)
        records = lax.dynamic_update_slice_in_dim(
            records, jnp.where(leaving[:, None], outgoing, previous), slot * BLOCK, 0
        )
        relayed = jnp.where(on_turn & (segment_index > 0), own_block, arriving)
        incoming, arriving = shifted((outgoing, relayed), "section", shards)
        return ((incoming, arriving, records), None)

    start = (blank_block, blank_block, jnp.zeros((MICRO * BLOCK, quarter), jnp.bfloat16))
    carry, _ = lax.scan(advance, start, jnp.arange(MICRO + cycle_size - 1, dtype=jnp.int32))
    kept = carry[2]
    for level in range(segment_bits):
        bit = shard_bits + segment_bits - 1 - level
        upper = index >> bit & 1
        halves = kept.reshape(kept.shape[0], 2, kept.shape[1] // 2)
        keep = jnp.where(upper == 1, halves[:, 1], halves[:, 0])
        send = jnp.where(upper == 1, halves[:, 0], halves[:, 1])
        received = partner(send, "section", bit)
        kept = (keep.astype(jnp.float32) + received.astype(jnp.float32)).astype(jnp.bfloat16)
    return kept


MESH = pl.DeviceIdType.MESH
CHUNKS = 2


def cycle_kernel(
    sizes,
    hidden,
    exits,
    lens,
    cache_hbm,
    gain,
    wq_hbm,
    wo_hbm,
    out,
    wq,
    wo,
    cache,
    stage,
    ready,
    table,
    scaled,
    partial,
    squares,
    psend,
    precv,
    att,
    wx,
    att_in,
    load_sem,
    own_sem,
    wy_send,
    wy_recv,
    up_send,
    up_recv,
    dn_send,
    dn_recv,
    wd_send,
    wd_recv,
    h_send,
    h_recv,
    lo_send,
    lo_recv,
    hi_send,
    hi_recv,
    p_send,
    p_recv,
    a_send,
    a_recv,
    r_send,
    r_recv,
    d_send,
    d_recv,
    x_send,
    x_recv,
):
    shards, head_size, heads = sizes
    index = lax.axis_index("section")
    seg = index // shards
    shard = index % shards
    across = seg * shards + (1 - shard)
    along = (1 - seg) * shards + shard
    corner = (1 - seg) * shards + (1 - shard)
    width = stage.shape[2]
    columns = wq.shape[1]
    query_width = heads * head_size
    half = MICRO // 2
    rows = BLOCK // shards
    span = out.shape[1]
    wide = wx.shape[1]
    low = width - wide
    context = cache.shape[1]
    own_rows = pl.ds(pl.multiple_of(shard * rows, rows), rows)
    other_rows = pl.ds(pl.multiple_of((1 - shard) * rows, rows), rows)

    place_blk = lax.axis_index("blk")
    chips = wd_send.shape[0]
    chip = place_blk // 2
    core = place_blk % 2
    chunk_rows = wx.shape[0] // (2 * chips * CHUNKS)
    above = jnp.minimum(chip + 1, chips - 1) * 2 + core
    below = jnp.maximum(chip - 1, 0) * 2 + core
    beside = chip * 2 + 1 - core
    has_above = chip < chips - 1
    has_below = chip > 0

    def remote(source, target, send, recv, device):
        return pltpu.make_async_remote_copy(
            src_ref=source,
            dst_ref=target,
            send_sem=send,
            recv_sem=recv,
            device_id=device,
            device_id_type=MESH,
        )

    barrier = pltpu.get_barrier_semaphore()
    for peer in (across, along, corner):
        pl.semaphore_signal(barrier, inc=1, device_id={"section": peer}, device_id_type=MESH)

    @pl.when(has_above)
    def _():
        pl.semaphore_signal(barrier, inc=1, device_id={"blk": above}, device_id_type=MESH)

    @pl.when(has_below)
    def _():
        pl.semaphore_signal(barrier, inc=1, device_id={"blk": below}, device_id_type=MESH)

    pl.semaphore_signal(barrier, inc=1, device_id={"blk": beside}, device_id_type=MESH)

    def own_copy(i):
        return pltpu.make_async_copy(
            hidden.at[pl.ds(i * BLOCK, BLOCK)], stage.at[i], own_sem.at[i]
        )

    def rest_copy(i):
        return pltpu.make_async_copy(
            hidden.at[pl.ds(i * BLOCK, BLOCK), pl.ds(low, wide)],
            stage.at[half + i, :, pl.ds(low, wide)],
            own_sem.at[i],
        )

    load_wq = pltpu.make_async_copy(wq_hbm, wq, load_sem.at[0])
    load_cache = pltpu.make_async_copy(cache_hbm, cache, load_sem.at[1])
    load_wo = pltpu.make_async_copy(wo_hbm, wo, load_sem.at[2])

    @pl.when(seg == 0)
    def _():
        own_copy(0).start()

    load_wq.start()
    load_cache.start()

    lane = lax.broadcasted_iota(jnp.int32, (128, 128), 1)
    line = lax.broadcasted_iota(jnp.int32, (128, 128), 0)
    for start in range(0, MICRO * BLOCK, 128):
        cols = pl.ds(start, 128)
        depth = jnp.sum(jnp.where(lane == line, exits[:, cols], 0), axis=1, keepdims=True)
        limit = jnp.sum(jnp.where(lane == line, lens[:, cols], 0), axis=1, keepdims=True)
        table[cols, :] = jnp.where(lane == 0, depth, limit)

    def place(i):
        return jnp.where(i < half, 2 * i, 2 * (i - half) + 1)

    def token_rows(i):
        return pl.ds(pl.multiple_of(place(i) * BLOCK, BLOCK), BLOCK)

    def depths(i):
        return table[token_rows(i), :][:, 0:1]

    def chunk_at(owner, chunk):
        first = pl.multiple_of(owner * (CHUNKS * chunk_rows) + chunk * chunk_rows, chunk_rows)
        return pl.ds(first, chunk_rows)

    def weight_out(layer, chunk):
        at = chunk_at(place_blk, chunk)
        first, size = (low, wide) if layer == 0 else (0, span)
        return remote(
            wo_hbm.at[at, pl.ds(first, size)],
            wx.at[at, pl.ds(0, size)],
            wy_send.at[chunk],
            wy_recv.at[chunk],
            {"section": along},
        )

    def held_size(layer):
        return pl.ds(0, wide if layer == 1 else span)

    def weight_in(layer, chunk):
        part = wx.at[chunk_at(place_blk, chunk), held_size(layer)]
        return remote(part, part, wy_send.at[chunk], wy_recv.at[chunk], {"section": along})

    def upward(layer, owner, chunk):
        part = wx.at[chunk_at(owner * 2 + core, chunk), held_size(layer)]
        return remote(
            part, part, up_send.at[owner, chunk], up_recv.at[owner, chunk], {"blk": above}
        )

    def downward(layer, owner, chunk):
        part = wx.at[chunk_at(owner * 2 + core, chunk), held_size(layer)]
        return remote(
            part, part, dn_send.at[owner, chunk], dn_recv.at[owner, chunk], {"blk": below}
        )

    def sideways(layer, owner, chunk, holder):
        part = wx.at[chunk_at(owner * 2 + holder, chunk), held_size(layer)]
        return remote(
            part, part, wd_send.at[owner, chunk], wd_recv.at[owner, chunk], {"blk": beside}
        )

    def spread(layer, chunk):
        weight_in(layer, chunk).wait_recv()

        @pl.when(has_above)
        def _():
            upward(layer, chip, chunk).start()

        @pl.when(has_below)
        def _():
            downward(layer, chip, chunk).start()

        sideways(layer, chip, chunk, core).start()

    def from_below(layer, distance, chunk):
        owner = chip - distance

        @pl.when(owner >= 0)
        def _():
            upward(layer, owner, chunk).wait_recv()

            @pl.when(has_above)
            def _():
                upward(layer, owner, chunk).start()

            sideways(layer, owner, chunk, core).start()

    def from_above(layer, distance, chunk):
        owner = chip + distance

        @pl.when(owner < chips)
        def _():
            downward(layer, owner, chunk).wait_recv()

            @pl.when(has_below)
            def _():
                downward(layer, owner, chunk).start()

            sideways(layer, owner, chunk, core).start()

    def pass_on(layer, distance, chunk):
        @pl.when(has_above)
        def _():
            from_below(layer, distance, chunk)

        @pl.when(has_below)
        def _():
            from_above(layer, distance, chunk)

    def collect(layer, chunk):
        for distance in range(1, chips):

            @pl.when(jnp.logical_not(has_above))
            def _():
                from_below(layer, distance, chunk)

            @pl.when(jnp.logical_not(has_below))
            def _():
                from_above(layer, distance, chunk)

    def gathered(layer):
        for owner in range(chips):
            for chunk in range(CHUNKS):
                sideways(layer, owner, chunk, 1 - core).wait_recv()

    def settle_weights(layer):
        for chunk in range(CHUNKS):
            weight_out(layer, chunk).wait_send()
            for owner in range(chips):
                sideways(layer, owner, chunk, core).wait_send()

                @pl.when(has_above & (owner <= chip))
                def _():
                    upward(layer, owner, chunk).wait_send()

                @pl.when(has_below & (owner >= chip))
                def _():
                    downward(layer, owner, chunk).wait_send()

    def hidden_copy(i):
        return remote(
            hidden.at[pl.ds(i * BLOCK, BLOCK)],
            stage.at[half + i],
            h_send.at[i],
            h_recv.at[i],
            {"section": along},
        )

    def low_copy(i, size):
        return remote(
            ready.at[i, :, pl.ds(0, size)],
            stage.at[i, :, pl.ds(0, size)],
            lo_send.at[i],
            lo_recv.at[i],
            {"section": along},
        )

    def high_copy(i):
        cols = pl.ds(span, span)
        return remote(
            ready.at[i, :, cols],
            stage.at[i, :, cols],
            hi_send.at[i],
            hi_recv.at[i],
            {"section": along},
        )

    def branch_copy(i, sent_rows):
        return remote(
            att.at[i, sent_rows],
            att_in.at[i, sent_rows],
            r_send.at[i],
            r_recv.at[i],
            {"section": along},
        )

    def corner_copy(i, sent_rows):
        return remote(
            att.at[i, sent_rows],
            att_in.at[i, sent_rows],
            d_send.at[i],
            d_recv.at[i],
            {"section": corner},
        )

    def relay_copy(i, sent_rows):
        return remote(
            att_in.at[i, sent_rows],
            att_in.at[i, sent_rows],
            x_send.at[i],
            x_recv.at[i],
            {"section": across},
        )

    def partial_copy(i):
        return remote(
            psend.at[i], precv.at[i], p_send.at[i], p_recv.at[i], {"section": across}
        )

    def attended_copy(i, sent_rows):
        return remote(
            att.at[i, sent_rows],
            att.at[i, sent_rows],
            a_send.at[i],
            a_recv.at[i],
            {"section": across},
        )

    def turn(layer, t):
        last = half if layer == 0 else MICRO - 1
        moved = jnp.where((t >= half - 1) & (t < last), t + 1, t)
        return jnp.where(t == last, half - 1, moved)

    def scale(i, first, last):
        total = jnp.zeros((BLOCK, 1), jnp.float32)
        size = min(last - first, 512)
        for start in range(first, last, size):
            cols = pl.ds(start, size)
            piece = stage[i, :, cols].astype(jnp.float32)
            total = total + jnp.sum(piece * piece, axis=1, keepdims=True)
            scaled[:, cols] = (piece * gain[:, cols].astype(jnp.float32)).astype(jnp.bfloat16)
        return total

    def multiply(slot, first, last, more):
        step = 512
        for start in range(0, columns, step):
            cols = pl.ds(start, min(step, columns - start))
            product = jnp.dot(
                scaled[:, pl.ds(first, last - first)],
                wq[pl.ds(first, last - first), cols],
                preferred_element_type=jnp.float32,
            )
            if more:
                product = partial[slot, :, cols] + product
            partial[slot, :, cols] = product

    def send_partial(i, slot):
        psend[i, :, pl.ds(0, columns)] = partial[slot, other_rows, :].astype(jnp.bfloat16)
        theirs = squares[slot, other_rows, :]
        coarse = theirs.astype(jnp.bfloat16)
        fine = (theirs - coarse.astype(jnp.float32)).astype(jnp.bfloat16)
        psend[i, :, pl.ds(columns, 128)] = coarse
        psend[i, :, pl.ds(columns + 128, 128)] = fine
        partial_copy(i).start()

    def keep_squares(slot, total):
        squares[slot] = jnp.broadcast_to(total, squares.shape[1:])

    def project(i, slot):
        keep_squares(slot, scale(i, 0, width))
        multiply(slot, 0, width, False)
        send_partial(i, slot)

    def attend_rows(i, slot):
        partial_copy(i).wait_recv()
        coarse = precv[i, :, pl.ds(columns, 128)].astype(jnp.float32)
        fine = precv[i, :, pl.ds(columns + 128, 128)].astype(jnp.float32)
        total_squares = squares[slot, own_rows, :] + coarse + fine
        factor = lax.rsqrt(total_squares / (width * shards) + EPSILON)[:, :1]
        fitted = (
            partial[slot, own_rows, :] + precv[i, :, pl.ds(0, columns)].astype(jnp.float32)
        ) * factor
        scale = 1.0 / math.sqrt(head_size)
        query = jnp.concatenate(
            [fitted[:, h * head_size : (h + 1) * head_size] for h in range(heads)], axis=0
        )
        query = (query * scale).astype(jnp.bfloat16)
        key_new = fitted[:, query_width : query_width + head_size].astype(jnp.bfloat16)
        value_new = fitted[:, query_width + head_size :].astype(jnp.bfloat16)
        key_new = jnp.concatenate([key_new.astype(jnp.float32)] * heads, axis=0)
        value_new = jnp.concatenate([value_new.astype(jnp.float32)] * heads, axis=0)
        start = pl.multiple_of(place(i) * rows, rows)
        held = cache[pl.ds(start, rows)].reshape(rows * context, 2 * head_size)
        scores = lax.dot_general(
            query,
            held[:, :head_size],
            (((1,), (1,)), ((), ())),
            preferred_element_type=jnp.float32,
        )
        own = jnp.sum(query.astype(jnp.float32) * key_new, axis=1, keepdims=True)
        limits = table[pl.ds(pl.multiple_of(place(i) * BLOCK + shard * rows, rows), rows), :][:, 1:2]
        row = lax.broadcasted_iota(jnp.int32, (rows, 1), 0) * context
        first = jnp.concatenate([row] * heads, axis=0)
        last = jnp.concatenate([row + limits] * heads, axis=0)
        column = lax.broadcasted_iota(jnp.int32, scores.shape, 1)
        usable = (column >= first) & (column < last)
        scores = jnp.where(usable, scores, NEGATIVE)
        row_top = jnp.maximum(jnp.max(scores, axis=1, keepdims=True), own)
        raw = jnp.where(usable, jnp.exp(scores - row_top), 0.0)
        raw_own = jnp.exp(own - row_top)
        total = jnp.sum(raw, axis=1, keepdims=True) + raw_own
        weights = (raw / total).astype(jnp.bfloat16)
        own_weight = (raw_own / total).astype(jnp.bfloat16).astype(jnp.float32)
        attended = jnp.dot(
            weights, held[:, head_size:], preferred_element_type=jnp.float32
        )
        attended = (attended + own_weight * value_new).astype(jnp.bfloat16)
        att[i, own_rows, :] = jnp.concatenate(
            [attended[h * rows : (h + 1) * rows] for h in range(heads)], axis=1
        )

    def added(source, weight, before, chosen, target, first, last, shift_weight, shift):
        size = min(last - first, 512)
        for start in range(first, last, size):
            branch = jnp.dot(
                source,
                weight[:, pl.ds(start + shift_weight, size)],
                preferred_element_type=jnp.float32,
            )
            kept = before[:, pl.ds(start, size)].astype(jnp.float32)
            target[:, pl.ds(start + shift, size)] = jnp.where(
                chosen, kept + branch, kept
            ).astype(jnp.bfloat16)

    neighbours = has_above.astype(jnp.int32) + has_below.astype(jnp.int32)
    pl.semaphore_wait(barrier, 4 + neighbours)

    def first_layer():
        for chunk in range(CHUNKS):
            weight_out(0, chunk).start()
        for i in range(1, half):
            own_copy(i).start()
        load_wo.start()

        def update(i):
            attended_copy(i, other_rows).wait_recv()
            active = depths(i) > 0
            fill = functools.partial(added, att[i], wo, stage.at[i], active, ready.at[i])
            fill(0, span, 0, 0)

            @pl.when(i < half - 1)
            def _():
                low_copy(i, span).start()

            @pl.when(i < half)
            def _():
                fill(span, width, 0, 0)

            @pl.when(i < half - 1)
            def _():
                high_copy(i).start()

            if low:

                @pl.when(i >= half)
                def _():
                    low_copy(i, low).start()

            @pl.when(i == MICRO - 1)
            def _():
                low_copy(half - 1, span).start()
                high_copy(half - 1).start()

        def step(t, carry):
            i = turn(0, t)

            @pl.when(i < half)
            def _():
                own_copy(i).wait()

            @pl.when(i >= half)
            def _():
                hidden_copy(i - half).wait_recv()

            @pl.when(t == half - 1)
            def _():
                spread(0, 0)

            for distance in range(1, chips - 1):

                @pl.when(t == min(half + distance, MICRO - 1))
                def _():
                    pass_on(0, distance, 0)

            @pl.when(t == 0)
            def _():
                load_wq.wait()

            project(i, 0)

            @pl.when(t == 1)
            def _():
                load_wo.wait()

            @pl.when((t > 0) & (t < MICRO - 1))
            def _():
                update(turn(0, t - 1))

            @pl.when(t == 0)
            def _():
                load_cache.wait()

            attend_rows(i, 0)

            @pl.when(i >= half)
            def _():
                branch_copy(i, own_rows).start()

            attended_copy(i, own_rows).start()

            @pl.when(t >= MICRO - 2)
            def _():
                update(i)

            return carry

        lax.fori_loop(0, MICRO, step, 0)
        pass_on(0, chips - 1, 0)
        collect(0, 0)
        for chunk in range(1, CHUNKS):
            spread(0, chunk)
        for distance in range(1, chips):
            for chunk in range(1, CHUNKS):
                pass_on(0, distance, chunk)
        for chunk in range(1, CHUNKS):
            collect(0, chunk)
        gathered(0)

        def finish(t, carry):
            i = turn(1, t)
            branch_copy(i, own_rows).wait_recv()
            corner_copy(i, other_rows).wait_recv()
            added(
                att_in[i],
                wx,
                ready.at[i],
                depths(i) > 1,
                out.at[token_rows(i)],
                0,
                span,
                0,
                0,
            )
            return carry

        lax.fori_loop(0, MICRO, finish, 0)

        def drain(i, carry):
            partial_copy(i).wait_send()
            attended_copy(i, own_rows).wait_send()

            @pl.when(i < half)
            def _():
                low_copy(i, span).wait_send()
                high_copy(i).wait_send()

            @pl.when(i >= half)
            def _():
                branch_copy(i, own_rows).wait_send()
                if low:
                    low_copy(i, low).wait_send()

            return carry

        lax.fori_loop(0, MICRO, drain, 0)
        settle_weights(0)

    def second_layer():
        hidden_copy(0).start()
        weight_out(1, 0).start()
        for i in range(1, half):
            hidden_copy(i).start()
        for chunk in range(1, CHUNKS):
            weight_out(1, chunk).start()
        for i in range(half):
            rest_copy(i).start()
        load_wo.start()
        load_wq.wait()
        load_cache.wait()
        for chunk in range(CHUNKS):
            spread(1, chunk)

        def relay(i):
            branch_copy(i, own_rows).wait_recv()
            relay_copy(i, own_rows).start()

        def early(i, slot):
            low_copy(i, span).wait_recv()
            total = scale(i, 0, span)
            multiply(slot, 0, span, False)
            high_copy(i).wait_recv()
            total = total + scale(i, span, width)
            multiply(slot, span, width, True)

            @pl.when(i == half - 2)
            def _():
                relay(half)

            keep_squares(slot, total)
            send_partial(i, slot)

        def late(i, slot):
            relay_copy(i, other_rows).wait_recv()
            added(
                att_in[i],
                wx,
                stage.at[i],
                depths(i) > 0,
                stage.at[i],
                low,
                width,
                -low,
                0,
            )

            @pl.when(i < MICRO - 1)
            def _():
                relay(i + 1)

            total = scale(i, low, width)
            multiply(slot, low, width, False)
            if low:
                low_copy(i, low).wait_recv()
                total = total + scale(i, 0, low)
                multiply(slot, 0, low, True)
            keep_squares(slot, total)
            send_partial(i, slot)

        def update(i):
            attended_copy(i, other_rows).wait_recv()
            added(
                att[i],
                wo,
                stage.at[i],
                depths(i) > 1,
                out.at[token_rows(i)],
                span,
                width,
                0,
                -span,
            )

        def step(t, carry):
            i = turn(1, t)

            for distance in range(1, chips):

                @pl.when(t == min(distance - 1, half - 1))
                def _():
                    for chunk in range(CHUNKS):
                        pass_on(1, distance, chunk)

            @pl.when(i < half)
            def _():
                early(i, t % 2)

            @pl.when(t == half - 1)
            def _():
                for chunk in range(CHUNKS):
                    collect(1, chunk)
                gathered(1)
                for j in range(half):
                    rest_copy(j).wait()

            @pl.when((i >= half) & (t < MICRO))
            def _():
                late(i, t % 2)

            @pl.when(t == MICRO)
            def _():
                update(half)
                update(half + 1)
                update(half + 2)

            @pl.when(t > 0)
            def _():
                j = turn(1, t - 1)
                attend_rows(j, (t - 1) % 2)
                corner_copy(j, own_rows).start()
                branch_copy(j, own_rows).start()
                attended_copy(j, own_rows).start()

            @pl.when(t == 1)
            def _():
                load_wo.wait()

            @pl.when((t > 1) & (t < half + 1))
            def _():
                update(turn(1, t - 2))

            return carry

        lax.fori_loop(0, MICRO + 1, step, 0)
        update(MICRO - 1)
        update(half - 1)

        def drain(i, carry):
            partial_copy(i).wait_send()
            attended_copy(i, own_rows).wait_send()
            branch_copy(i, own_rows).wait_send()
            corner_copy(i, own_rows).wait_send()

            @pl.when(i < half)
            def _():
                hidden_copy(i).wait_send()

            @pl.when(i >= half)
            def _():
                relay_copy(i, own_rows).wait_send()

            return carry

        lax.fori_loop(0, MICRO, drain, 0)
        settle_weights(1)

    @pl.when(seg == 0)
    def _():
        first_layer()

    @pl.when(seg == 1)
    def _():
        second_layer()


def cycle_of_two(chips, hidden, exit_layer, lengths, kv_cache, norm_gain, w_qkv, w_out):
    shards = 2
    width = w_qkv.shape[1]
    columns = w_qkv.shape[2]
    query_width = w_out.shape[1]
    head_size = (columns - query_width) // 2
    heads = query_width // head_size
    rows = BLOCK // shards
    span = width // 2
    wide = span + span // 2
    tokens = exit_layer.shape[0]
    hbm = pl.BlockSpec(memory_space=pltpu.HBM)
    vmem = pl.BlockSpec(memory_space=pltpu.VMEM)
    dma = pltpu.SemaphoreType.DMA((MICRO,))
    pieces = pltpu.SemaphoreType.DMA((chips, CHUNKS))
    bf16 = jnp.bfloat16
    return pl.pallas_call(
        functools.partial(cycle_kernel, (shards, head_size, heads)),
        out_shape=pltpu.VMEM((MICRO * BLOCK, span), bf16),
        in_specs=[hbm, vmem, vmem, hbm, vmem, hbm, hbm],
        out_specs=vmem,
        scratch_shapes=[
            pltpu.VMEM(w_qkv.shape[1:], bf16),
            pltpu.VMEM(w_out.shape[1:], bf16),
            pltpu.VMEM(kv_cache.shape[1:], bf16),
            pltpu.VMEM((MICRO, BLOCK, width), bf16),
            pltpu.VMEM((MICRO, BLOCK, width), bf16),
            pltpu.VMEM((MICRO * BLOCK, 128), jnp.int32),
            pltpu.VMEM((BLOCK, width), bf16),
            pltpu.VMEM((2, BLOCK, columns), jnp.float32),
            pltpu.VMEM((2, BLOCK, 128), jnp.float32),
            pltpu.VMEM((MICRO, rows, columns + 256), bf16),
            pltpu.VMEM((MICRO, rows, columns + 256), bf16),
            pltpu.VMEM((MICRO, BLOCK, query_width), bf16),
            pltpu.VMEM((query_width, wide), bf16),
            pltpu.VMEM((MICRO, BLOCK, query_width), bf16),
            pltpu.SemaphoreType.DMA((3,)),
            dma,
            pltpu.SemaphoreType.DMA((CHUNKS,)),
            pltpu.SemaphoreType.DMA((CHUNKS,)),
        ]
        + [pieces] * 6
        + [dma] * 16,
        compiler_params=pltpu.CompilerParams(
            collective_id=0, has_side_effects=True, vmem_limit_bytes=VMEM_LIMIT
        ),
        name="cycle",
    )(
        hidden[0],
        exit_layer.reshape(1, tokens),
        lengths.reshape(1, tokens),
        kv_cache[0],
        norm_gain,
        w_qkv[0],
        w_out[0],
    )


def chosen(batches, devices, *arguments):
    shards = max(2, devices // 4)
    if shards == 2 and devices // shards == 2:
        return cycle_of_two(batches // 2, *arguments)
    return body(*arguments)


def solution(mesh):
    return jax.shard_map(
        functools.partial(chosen, mesh.shape["blk"], mesh.shape["section"]),
        mesh=mesh,
        in_specs=(
            P("section", "blk", None),
            P("blk"),
            P("blk"),
            P("section", "blk", None, None),
            P("section", None),
            P("section", None, None),
            P("section", None, None),
        ),
        out_specs=P("blk", "section"),
        check_vma=False,
    )
```

```python
import functools
import math

import jax
import jax.numpy as jnp
from jax import lax
from jax.experimental import pallas as pl
from jax.experimental.pallas import tpu as pltpu
from jax.sharding import PartitionSpec as P

BLOCK = 64
MICRO = 8


EPSILON = 1e-05
NEGATIVE = -1e30
VMEM_LIMIT = 60 << 20


def partner(value, axis, distance):
    return lax.ppermute(value, axis, [(i, i ^ 1 << distance) for i in range(lax.axis_size(axis))])


def shifted(value, axis, steps):
    count = lax.axis_size(axis)
    pairs = [(source, (source + steps) % count) for source in range(count)]
    return lax.ppermute(value, axis, pairs)


def body(hidden, exit_layer, lengths, kv_cache, norm_gain, w_qkv, w_out):
    devices = lax.axis_size("section")
    index = lax.axis_index("section")
    shards = max(2, devices // 4)
    cycle_size = devices // shards
    segment_bits = cycle_size.bit_length() - 1
    shard_bits = shards.bit_length() - 1
    segment_index = index // shards
    shard_index = index % shards
    own_blocks = hidden[0]
    gain_row = norm_gain[0].astype(jnp.float32)
    proj_weight = w_qkv[0]
    out_weight = w_out[0]
    cache_all = kv_cache[0]
    query_width = out_weight.shape[0]
    head_size = (proj_weight.shape[1] - query_width) // 2
    heads = query_width // head_size
    quarter = proj_weight.shape[0]
    total_width = quarter * shards
    group_rows = BLOCK // shards
    rounds = MICRO // cycle_size
    context = cache_all.shape[1]
    positions = jnp.arange(context, dtype=jnp.int32)
    blank_block = jnp.zeros((BLOCK, quarter), jnp.bfloat16)

    def advance(carry, microstep):
        incoming, arriving, records = carry
        micro_index = microstep - segment_index
        in_range = (micro_index >= 0) & (micro_index < MICRO)
        slot = jnp.clip(micro_index, 0, MICRO - 1)
        on_turn = microstep % cycle_size == 0
        local_slot = jnp.minimum(microstep // cycle_size, rounds - 1)
        own_block = lax.dynamic_slice_in_dim(own_blocks, local_slot * BLOCK, BLOCK, 0)
        exit_rows = lax.dynamic_slice_in_dim(exit_layer, slot * BLOCK, BLOCK)
        own_lengths = lax.dynamic_slice_in_dim(
            lengths, slot * BLOCK + shard_index * group_rows, group_rows
        )
        own_cache = lax.dynamic_slice_in_dim(cache_all, slot * group_rows, group_rows, 0)
        first_input = jnp.where(on_turn, own_block, arriving)
        entering = jnp.where(segment_index == 0, first_input, incoming)
        active = exit_rows > segment_index
        gate = in_range & (jnp.sum(active.astype(jnp.int32)) > 0)

        def local_partials():
            widened = entering.astype(jnp.float32)
            scaled = (widened * gain_row).astype(jnp.bfloat16)
            return (
                jnp.dot(scaled, proj_weight, preferred_element_type=jnp.float32),
                jnp.sum(widened * widened, axis=1),
            )

        def no_partials():
            return (
                jnp.zeros((BLOCK, proj_weight.shape[1]), jnp.float32),
                jnp.zeros((BLOCK,), jnp.float32),
            )

        partial_proj, partial_squares = lax.cond(gate, local_partials, no_partials)
        kept = (partial_proj, partial_squares)
        for level in range(shard_bits):
            bit = shard_bits - 1 - level
            upper = index >> bit & 1
            halves = tuple(
                (piece.reshape((2, piece.shape[0] // 2) + piece.shape[1:]) for piece in kept)
            )
            keep = tuple((jnp.where(upper == 1, half[1], half[0]) for half in halves))
            send = tuple((jnp.where(upper == 1, half[0], half[1]) for half in halves))
            received = partner(send, "section", bit)
            kept = tuple((first + second for first, second in zip(keep, received)))
        own_proj, own_squares = kept

        def local_attention():
            fitted = own_proj * lax.rsqrt(own_squares / total_width + EPSILON)[:, None]
            query = (fitted[:, :query_width] * (1.0 / math.sqrt(head_size))).astype(jnp.bfloat16)
            query = query.reshape(group_rows, heads, head_size)
            key_new = fitted[:, query_width : query_width + head_size].astype(jnp.bfloat16)
            value_new = fitted[:, query_width + head_size :].astype(jnp.bfloat16)
            scores = jnp.einsum(
                "rhd,rcd->rhc",
                query,
                own_cache[:, :, :head_size],
                preferred_element_type=jnp.float32,
            )
            own = jnp.einsum("rhd,rd->rh", query, key_new, preferred_element_type=jnp.float32)
            usable = (positions[None, :] < own_lengths[:, None])[:, None, :]
            scores = jnp.where(usable, scores, NEGATIVE)
            row_top = jnp.maximum(jnp.max(scores, axis=-1), own)
            raw = jnp.where(usable, jnp.exp(scores - row_top[:, :, None]), jnp.float32(0.0))
            raw_own = jnp.exp(own - row_top)
            total = jnp.sum(raw, axis=-1) + raw_own
            weights = (raw / total[:, :, None]).astype(jnp.bfloat16)
            own_weight = (raw_own / total).astype(jnp.bfloat16)
            attended = jnp.einsum(
                "rhc,rcd->rhd",
                weights,
                own_cache[:, :, head_size:],
                preferred_element_type=jnp.float32,
            )
            attended = (
                attended
                + own_weight.astype(jnp.float32)[:, :, None]
                * value_new.astype(jnp.float32)[:, None, :]
            )
            return attended.astype(jnp.bfloat16).reshape(group_rows, query_width)

        def no_attention():
            return jnp.zeros((group_rows, query_width), jnp.bfloat16)

        collected = lax.cond(gate, local_attention, no_attention)
        for level in range(shard_bits):
            bit = level
            other = partner(collected, "section", bit)
            upper = index >> bit & 1
            collected = jnp.where(
                upper == 1,
                jnp.concatenate([other, collected], 0),
                jnp.concatenate([collected, other], 0),
            )

        def local_update():
            branch_out = jnp.dot(collected, out_weight, preferred_element_type=jnp.float32)
            updated = (entering.astype(jnp.float32) + branch_out).astype(jnp.bfloat16)
            return jnp.where(active[:, None], updated, entering)

        def keep_state():
            return entering

        outgoing = lax.cond(gate, local_update, keep_state)
        leaving = in_range & (exit_rows == segment_index + 1)
        previous = lax.dynamic_slice_in_dim(records, slot * BLOCK, BLOCK, 0)
        records = lax.dynamic_update_slice_in_dim(
            records, jnp.where(leaving[:, None], outgoing, previous), slot * BLOCK, 0
        )
        relayed = jnp.where(on_turn & (segment_index > 0), own_block, arriving)
        incoming, arriving = shifted((outgoing, relayed), "section", shards)
        return ((incoming, arriving, records), None)

    start = (blank_block, blank_block, jnp.zeros((MICRO * BLOCK, quarter), jnp.bfloat16))
    carry, _ = lax.scan(advance, start, jnp.arange(MICRO + cycle_size - 1, dtype=jnp.int32))
    kept = carry[2]
    for level in range(segment_bits):
        bit = shard_bits + segment_bits - 1 - level
        upper = index >> bit & 1
        halves = kept.reshape(kept.shape[0], 2, kept.shape[1] // 2)
        keep = jnp.where(upper == 1, halves[:, 1], halves[:, 0])
        send = jnp.where(upper == 1, halves[:, 0], halves[:, 1])
        received = partner(send, "section", bit)
        kept = (keep.astype(jnp.float32) + received.astype(jnp.float32)).astype(jnp.bfloat16)
    return kept


MESH = pl.DeviceIdType.MESH
CHUNKS = 4
EARLY = 3


def cycle_kernel(
    sizes,
    hidden,
    exits,
    lens,
    cache_hbm,
    gain,
    wq_hbm,
    wo_hbm,
    out,
    wq,
    wo,
    cache,
    stage,
    ready,
    table,
    scaled,
    partial,
    squares,
    psend,
    precv,
    att,
    wx,
    att_in,
    load_sem,
    own_sem,
    wy_send,
    wy_recv,
    up_send,
    up_recv,
    dn_send,
    dn_recv,
    wd_send,
    wd_recv,
    h_send,
    h_recv,
    lo_send,
    lo_recv,
    hi_send,
    hi_recv,
    p_send,
    p_recv,
    a_send,
    a_recv,
    r_send,
    r_recv,
    d_send,
    d_recv,
    x_send,
    x_recv,
):
    shards, head_size, heads = sizes
    index = lax.axis_index("section")
    seg = index // shards
    shard = index % shards
    across = seg * shards + (1 - shard)
    along = (1 - seg) * shards + shard
    corner = (1 - seg) * shards + (1 - shard)
    width = stage.shape[2]
    columns = wq.shape[1]
    query_width = heads * head_size
    half = MICRO // 2
    rows = BLOCK // shards
    span = out.shape[1]
    wide = wx.shape[1]
    low = width - wide
    context = cache.shape[1]
    own_rows = pl.ds(pl.multiple_of(shard * rows, rows), rows)
    other_rows = pl.ds(pl.multiple_of((1 - shard) * rows, rows), rows)

    place_blk = lax.axis_index("blk")
    chips = wd_send.shape[0]
    chip = place_blk // 2
    core = place_blk % 2
    chunk_rows = wx.shape[0] // (2 * chips * CHUNKS)
    above = jnp.minimum(chip + 1, chips - 1) * 2 + core
    below = jnp.maximum(chip - 1, 0) * 2 + core
    beside = chip * 2 + 1 - core
    has_above = chip < chips - 1
    has_below = chip > 0

    def remote(source, target, send, recv, device):
        return pltpu.make_async_remote_copy(
            src_ref=source,
            dst_ref=target,
            send_sem=send,
            recv_sem=recv,
            device_id=device,
            device_id_type=MESH,
        )

    barrier = pltpu.get_barrier_semaphore()
    for peer in (across, along, corner):
        pl.semaphore_signal(barrier, inc=1, device_id={"section": peer}, device_id_type=MESH)

    @pl.when(has_above)
    def _():
        pl.semaphore_signal(barrier, inc=1, device_id={"blk": above}, device_id_type=MESH)

    @pl.when(has_below)
    def _():
        pl.semaphore_signal(barrier, inc=1, device_id={"blk": below}, device_id_type=MESH)

    pl.semaphore_signal(barrier, inc=1, device_id={"blk": beside}, device_id_type=MESH)

    def own_copy(i):
        return pltpu.make_async_copy(
            hidden.at[pl.ds(i * BLOCK, BLOCK)], stage.at[i], own_sem.at[i]
        )

    def rest_copy(i):
        return pltpu.make_async_copy(
            hidden.at[pl.ds(i * BLOCK, BLOCK), pl.ds(low, wide)],
            stage.at[half + i, :, pl.ds(low, wide)],
            own_sem.at[i],
        )

    load_wq = pltpu.make_async_copy(wq_hbm, wq, load_sem.at[0])
    load_cache = pltpu.make_async_copy(cache_hbm, cache, load_sem.at[1])
    load_wo = pltpu.make_async_copy(wo_hbm, wo, load_sem.at[2])

    @pl.when(seg == 0)
    def _():
        own_copy(0).start()

    load_wq.start()
    load_cache.start()

    lane = lax.broadcasted_iota(jnp.int32, (128, 128), 1)
    line = lax.broadcasted_iota(jnp.int32, (128, 128), 0)
    for start in range(0, MICRO * BLOCK, 128):
        cols = pl.ds(start, 128)
        depth = jnp.sum(jnp.where(lane == line, exits[:, cols], 0), axis=1, keepdims=True)
        limit = jnp.sum(jnp.where(lane == line, lens[:, cols], 0), axis=1, keepdims=True)
        table[cols, :] = jnp.where(lane == 0, depth, limit)

    def place(i):
        if isinstance(i, int):
            return 2 * i if i < half else 2 * (i - half) + 1
        return jnp.where(i < half, 2 * i, 2 * (i - half) + 1)

    def token_rows(i):
        return pl.ds(pl.multiple_of(place(i) * BLOCK, BLOCK), BLOCK)

    def depths(i):
        return table[token_rows(i), :][:, 0:1]

    def chunk_at(owner, chunk):
        first = pl.multiple_of(owner * (CHUNKS * chunk_rows) + chunk * chunk_rows, chunk_rows)
        return pl.ds(first, chunk_rows)

    def weight_out(layer, chunk):
        at = chunk_at(place_blk, chunk)
        first, size = (low, wide) if layer == 0 else (0, span)
        return remote(
            wo_hbm.at[at, pl.ds(first, size)],
            wx.at[at, pl.ds(0, size)],
            wy_send.at[chunk],
            wy_recv.at[chunk],
            {"section": along},
        )

    def held_size(layer):
        return pl.ds(0, wide if layer == 1 else span)

    def weight_in(layer, chunk):
        part = wx.at[chunk_at(place_blk, chunk), held_size(layer)]
        return remote(part, part, wy_send.at[chunk], wy_recv.at[chunk], {"section": along})

    def upward(layer, owner, chunk):
        part = wx.at[chunk_at(owner * 2 + core, chunk), held_size(layer)]
        return remote(
            part, part, up_send.at[owner, chunk], up_recv.at[owner, chunk], {"blk": above}
        )

    def downward(layer, owner, chunk):
        part = wx.at[chunk_at(owner * 2 + core, chunk), held_size(layer)]
        return remote(
            part, part, dn_send.at[owner, chunk], dn_recv.at[owner, chunk], {"blk": below}
        )

    def sideways(layer, owner, chunk, holder):
        part = wx.at[chunk_at(owner * 2 + holder, chunk), held_size(layer)]
        return remote(
            part, part, wd_send.at[owner, chunk], wd_recv.at[owner, chunk], {"blk": beside}
        )

    def spread(layer, chunk):
        weight_in(layer, chunk).wait_recv()

        @pl.when(has_above)
        def _():
            upward(layer, chip, chunk).start()

        @pl.when(has_below)
        def _():
            downward(layer, chip, chunk).start()

        sideways(layer, chip, chunk, core).start()

    def from_below(layer, distance, chunk):
        owner = chip - distance

        @pl.when(owner >= 0)
        def _():
            upward(layer, owner, chunk).wait_recv()

            @pl.when(has_above)
            def _():
                upward(layer, owner, chunk).start()

            sideways(layer, owner, chunk, core).start()

    def from_above(layer, distance, chunk):
        owner = chip + distance

        @pl.when(owner < chips)
        def _():
            downward(layer, owner, chunk).wait_recv()

            @pl.when(has_below)
            def _():
                downward(layer, owner, chunk).start()

            sideways(layer, owner, chunk, core).start()

    def pass_on(layer, distance, chunk):
        @pl.when(has_above)
        def _():
            from_below(layer, distance, chunk)

        @pl.when(has_below)
        def _():
            from_above(layer, distance, chunk)

    def collect(layer, chunk):
        for distance in range(1, chips):

            @pl.when(jnp.logical_not(has_above))
            def _():
                from_below(layer, distance, chunk)

            @pl.when(jnp.logical_not(has_below))
            def _():
                from_above(layer, distance, chunk)

    def gathered(layer):
        for owner in range(chips):
            for chunk in range(CHUNKS):
                sideways(layer, owner, chunk, 1 - core).wait_recv()

    def settle_weights(layer):
        for chunk in range(CHUNKS):
            weight_out(layer, chunk).wait_send()
            for owner in range(chips):
                sideways(layer, owner, chunk, core).wait_send()

                @pl.when(has_above & (owner <= chip))
                def _():
                    upward(layer, owner, chunk).wait_send()

                @pl.when(has_below & (owner >= chip))
                def _():
                    downward(layer, owner, chunk).wait_send()

    def hidden_copy(i):
        return remote(
            hidden.at[pl.ds(i * BLOCK, BLOCK)],
            stage.at[half + i],
            h_send.at[i],
            h_recv.at[i],
            {"section": along},
        )

    def low_copy(i, size):
        return remote(
            ready.at[i, :, pl.ds(0, size)],
            stage.at[i, :, pl.ds(0, size)],
            lo_send.at[i],
            lo_recv.at[i],
            {"section": along},
        )

    def high_copy(i):
        cols = pl.ds(span, span)
        return remote(
            ready.at[i, :, cols],
            stage.at[i, :, cols],
            hi_send.at[i],
            hi_recv.at[i],
            {"section": along},
        )

    def branch_copy(i, sent_rows):
        return remote(
            att.at[i, sent_rows],
            att_in.at[i, sent_rows],
            r_send.at[i],
            r_recv.at[i],
            {"section": along},
        )

    def corner_copy(i, sent_rows):
        return remote(
            att.at[i, sent_rows],
            att_in.at[i, sent_rows],
            d_send.at[i],
            d_recv.at[i],
            {"section": corner},
        )

    def relay_copy(i, sent_rows):
        return remote(
            att_in.at[i, sent_rows],
            att_in.at[i, sent_rows],
            x_send.at[i],
            x_recv.at[i],
            {"section": across},
        )

    def relay(i):
        branch_copy(i, own_rows).wait_recv()
        relay_copy(i, own_rows).start()

    def partial_copy(i):
        return remote(
            psend.at[i], precv.at[i], p_send.at[i], p_recv.at[i], {"section": across}
        )

    def attended_copy(i, sent_rows):
        return remote(
            att.at[i, sent_rows],
            att.at[i, sent_rows],
            a_send.at[i],
            a_recv.at[i],
            {"section": across},
        )

    def turn(layer, t):
        last = half if layer == 0 else MICRO - 1
        moved = jnp.where((t >= half - 1) & (t < last), t + 1, t)
        return jnp.where(t == last, half - 1, moved)

    def blocks_at(ref, i, count, cols):
        return ref[pl.ds(i, count), :, cols].reshape(count * BLOCK, cols.size)

    def scale(i, count, first, last):
        total = jnp.zeros((count * BLOCK, 1), jnp.float32)
        for start in range(first, last, 512):
            cols = pl.ds(start, min(512, last - start))
            piece = blocks_at(stage, i, count, cols).astype(jnp.float32)
            total = total + jnp.sum(piece * piece, axis=1, keepdims=True)
            scaled[pl.ds(0, count * BLOCK), cols] = (
                piece * gain[:, cols].astype(jnp.float32)
            ).astype(jnp.bfloat16)
        return total

    def multiply(slot, count, first, last, more):
        step = 512
        for start in range(0, columns, step):
            cols = pl.ds(start, min(step, columns - start))
            product = jnp.dot(
                scaled[pl.ds(0, count * BLOCK), pl.ds(first, last - first)],
                wq[pl.ds(first, last - first), cols],
                preferred_element_type=jnp.float32,
            )
            if more:
                product = blocks_at(partial, slot, count, cols) + product
            partial[pl.ds(slot, count), :, cols] = product.reshape(count, BLOCK, cols.size)

    def send_partial(i, slot):
        psend[i, :, pl.ds(0, columns)] = partial[slot, other_rows, :].astype(jnp.bfloat16)
        theirs = squares[slot, other_rows, :]
        coarse = theirs.astype(jnp.bfloat16)
        fine = (theirs - coarse.astype(jnp.float32)).astype(jnp.bfloat16)
        first = lax.broadcasted_iota(jnp.int32, theirs.shape, 1) == 0
        psend[i, :, pl.ds(columns, 128)] = jnp.where(
            first, coarse.astype(jnp.float32), fine.astype(jnp.float32)
        ).astype(jnp.bfloat16)
        partial_copy(i).start()

    def keep_squares(slot, count, total):
        spread_out = jnp.broadcast_to(total, (count * BLOCK, 128))
        squares[pl.ds(slot, count)] = spread_out.reshape(count, BLOCK, 128)

    def project(i, slot):
        keep_squares(slot, 1, scale(i, 1, 0, width))
        multiply(slot, 1, 0, width, False)
        send_partial(i, slot)

    def attend_rows(i, slot):
        partial_copy(i).wait_recv()
        theirs = precv[i, :, pl.ds(columns, 128)].astype(jnp.float32)
        total_squares = squares[slot, own_rows, :][:, :1] + (theirs[:, :1] + theirs[:, 1:2])
        factor = lax.rsqrt(total_squares / (width * shards) + EPSILON)
        fitted = (
            partial[slot, own_rows, :] + precv[i, :, pl.ds(0, columns)].astype(jnp.float32)
        ) * factor
        scale = 1.0 / math.sqrt(head_size)
        query = jnp.concatenate(
            [fitted[:, h * head_size : (h + 1) * head_size] for h in range(heads)], axis=0
        )
        query = (query * scale).astype(jnp.bfloat16)
        key_new = fitted[:, query_width : query_width + head_size].astype(jnp.bfloat16)
        value_new = fitted[:, query_width + head_size :].astype(jnp.bfloat16)
        key_new = jnp.concatenate([key_new.astype(jnp.float32)] * heads, axis=0)
        value_new = jnp.concatenate([value_new.astype(jnp.float32)] * heads, axis=0)
        start = pl.multiple_of(place(i) * rows, rows)
        held = cache[pl.ds(start, rows)].reshape(rows * context, 2 * head_size)
        scores = lax.dot_general(
            query,
            held[:, :head_size],
            (((1,), (1,)), ((), ())),
            preferred_element_type=jnp.float32,
        )
        own = jnp.sum(query.astype(jnp.float32) * key_new, axis=1, keepdims=True)
        limits = table[pl.ds(pl.multiple_of(place(i) * BLOCK + shard * rows, rows), rows), :][:, 1:2]
        row = lax.broadcasted_iota(jnp.int32, (rows, 1), 0) * context
        first = jnp.concatenate([row] * heads, axis=0)
        last = jnp.concatenate([row + limits] * heads, axis=0)
        column = lax.broadcasted_iota(jnp.int32, scores.shape, 1)
        usable = (column >= first) & (column < last)
        scores = jnp.where(usable, scores, NEGATIVE)
        row_top = jnp.maximum(jnp.max(scores, axis=1, keepdims=True), own)
        raw = jnp.where(usable, jnp.exp(scores - row_top), 0.0)
        raw_own = jnp.exp(own - row_top)
        total = jnp.sum(raw, axis=1, keepdims=True) + raw_own
        weights = (raw / total).astype(jnp.bfloat16)
        own_weight = (raw_own / total).astype(jnp.bfloat16).astype(jnp.float32)
        attended = jnp.dot(
            weights, held[:, head_size:], preferred_element_type=jnp.float32
        )
        attended = (attended + own_weight * value_new).astype(jnp.bfloat16)
        att[i, own_rows, :] = jnp.concatenate(
            [attended[h * rows : (h + 1) * rows] for h in range(heads)], axis=1
        )

    def added(source, weight, before, chosen, target, first, last, shift_weight, shift):
        for start in range(first, last, 512):
            size = min(512, last - start)
            branch = jnp.dot(
                source,
                weight[:, pl.ds(start + shift_weight, size)],
                preferred_element_type=jnp.float32,
            )
            kept = before[:, pl.ds(start, size)].astype(jnp.float32)
            target[:, pl.ds(start + shift, size)] = jnp.where(
                chosen, kept + branch, kept
            ).astype(jnp.bfloat16)

    neighbours = has_above.astype(jnp.int32) + has_below.astype(jnp.int32)
    pl.semaphore_wait(barrier, 4 + neighbours)

    def first_layer():
        for chunk in range(CHUNKS):
            weight_out(0, chunk).start()
        for i in range(1, half):
            own_copy(i).start()
        load_wo.start()

        def update(i):
            attended_copy(i, other_rows).wait_recv()
            active = depths(i) > 0
            fill = functools.partial(added, att[i], wo, stage.at[i], active, ready.at[i])
            fill(0, span, 0, 0)

            @pl.when(i < half - 2)
            def _():
                low_copy(i, span).start()

            @pl.when(i < half)
            def _():
                fill(span, width, 0, 0)

            @pl.when(i < half - 2)
            def _():
                high_copy(i).start()

            if low:

                @pl.when(i >= half)
                def _():
                    low_copy(i, low).start()

            @pl.when(i == MICRO - 1)
            def _():
                low_copy(half - 1, span).start()
                high_copy(half - 1).start()

        def step(t, carry):
            i = turn(0, t)

            @pl.when(i < half)
            def _():
                own_copy(i).wait()

            @pl.when(i >= half)
            def _():
                hidden_copy(i - half).wait_recv()

            @pl.when(t == half - 1)
            def _():
                for chunk in range(EARLY):
                    spread(0, chunk)

            for distance in range(1, chips - 1):

                @pl.when(t == min(half + distance, MICRO - 1))
                def _():
                    for chunk in range(EARLY):
                        pass_on(0, distance, chunk)

            @pl.when(t == 0)
            def _():
                load_wq.wait()

            project(i, 0)

            @pl.when(t == MICRO - 1)
            def _():
                for chunk in range(EARLY, CHUNKS):
                    spread(0, chunk)

            @pl.when(t == 1)
            def _():
                load_wo.wait()

            @pl.when((t > 0) & (t < MICRO - 1))
            def _():
                update(turn(0, t - 1))

            @pl.when(t == 0)
            def _():
                load_cache.wait()

            attend_rows(i, 0)

            @pl.when(i >= half)
            def _():
                branch_copy(i, own_rows).start()

            @pl.when(i == half + 1)
            def _():
                low_copy(half - 2, span).start()

            @pl.when(i == half + 2)
            def _():
                high_copy(half - 2).start()

            attended_copy(i, own_rows).start()

            @pl.when(t == MICRO - 1)
            def _():
                for chunk in range(EARLY, CHUNKS):
                    pass_on(0, 1, chunk)

            @pl.when(t >= MICRO - 2)
            def _():
                update(i)

            return carry

        lax.fori_loop(0, MICRO, step, 0)
        relay(0)
        for chunk in range(EARLY):
            pass_on(0, chips - 1, chunk)
            collect(0, chunk)
        relay(1)
        for distance in range(2, chips):
            for chunk in range(EARLY, CHUNKS):
                pass_on(0, distance, chunk)
        for chunk in range(EARLY, CHUNKS):
            collect(0, chunk)
        for i in range(2, half - 1):
            relay(i)
        gathered(0)

        def finish(i, count):
            for j in range(i, i + count):
                if j == half - 1:
                    branch_copy(j, own_rows).wait_recv()
                    corner_copy(j, other_rows).wait_recv()
                else:
                    relay_copy(j, other_rows).wait_recv()
            source = att_in[pl.ds(i, count)].reshape(count * BLOCK, query_width)
            deep = jnp.concatenate([depths(j) for j in range(i, i + count)], axis=0) > 1
            for start in range(0, span, 512):
                cols = pl.ds(start, min(512, span - start))
                branch = jnp.dot(source, wx[:, cols], preferred_element_type=jnp.float32)
                kept = blocks_at(ready, i, count, cols).astype(jnp.float32)
                now = jnp.where(deep, kept + branch, kept).astype(jnp.bfloat16)
                for j in range(count):
                    out[token_rows(i + j), cols] = now[j * BLOCK : (j + 1) * BLOCK]

        def drain(i, carry):
            partial_copy(i).wait_send()
            attended_copy(i, own_rows).wait_send()

            @pl.when(i < half)
            def _():
                low_copy(i, span).wait_send()
                high_copy(i).wait_send()

            @pl.when(i >= half)
            def _():
                branch_copy(i, own_rows).wait_send()
                if low:
                    low_copy(i, low).wait_send()

            return carry

        def unrelay(i, carry):
            @pl.when(i != half - 1)
            def _():
                relay_copy(i, own_rows).wait_send()

            return carry

        finish(0, 2)
        settle_weights(0)
        lax.fori_loop(0, MICRO, drain, 0)
        relay(half)
        relay(half + 1)
        finish(2, 1)
        relay(half + 2)
        finish(half, 2)
        relay(half + 3)
        lax.fori_loop(0, half + 2, unrelay, 0)
        finish(half + 2, 2)
        finish(half - 1, 1)

        lax.fori_loop(half + 2, MICRO, unrelay, 0)

    def second_layer():
        hidden_copy(0).start()
        for chunk in range(EARLY):
            weight_out(1, chunk).start()
        for i in range(1, half):
            hidden_copy(i).start()
        for chunk in range(EARLY, CHUNKS):
            weight_out(1, chunk).start()
        for i in range(half):
            rest_copy(i).start()
        load_wo.start()
        load_wq.wait()
        load_cache.wait()
        for chunk in range(CHUNKS):
            spread(1, chunk)

        def first_half(i, slot):
            low_copy(i, span).wait_recv()
            total = scale(i, 1, 0, span)
            multiply(slot, 1, 0, span, False)
            return total

        def second_half(i, slot, total):
            high_copy(i).wait_recv()
            total = total + scale(i, 1, span, width)
            multiply(slot, 1, span, width, True)
            keep_squares(slot, 1, total)
            send_partial(i, slot)

        def late(i, slot):
            for j in range(2):
                relay_copy(i + j, other_rows).wait_recv()
            source = att_in[pl.ds(i, 2)].reshape(2 * BLOCK, query_width)
            active = jnp.concatenate([depths(i), depths(i + 1)], axis=0) > 0
            for start in range(low, width, 512):
                size = min(512, width - start)
                cols = pl.ds(start, size)
                branch = jnp.dot(
                    source, wx[:, pl.ds(start - low, size)], preferred_element_type=jnp.float32
                )
                kept = blocks_at(stage, i, 2, cols).astype(jnp.float32)
                now = jnp.where(active, kept + branch, kept).astype(jnp.bfloat16)
                stage[pl.ds(i, 2), :, cols] = now.reshape(2, BLOCK, size)

            @pl.when(i == half)
            def _():
                relay(half + 3)

            total = scale(i, 2, low, width)
            multiply(slot, 2, low, width, False)
            if low:
                for j in range(2):
                    low_copy(i + j, low).wait_recv()
                total = total + scale(i, 2, 0, low)
                multiply(slot, 2, 0, low, True)
            keep_squares(slot, 2, total)
            for j in range(2):
                send_partial(i + j, slot + j)

        def update(i):
            attended_copy(i, other_rows).wait_recv()
            added(
                att[i],
                wo,
                stage.at[i],
                depths(i) > 1,
                out.at[token_rows(i)],
                span,
                width,
                0,
                -span,
            )

        def attend(i, slot):
            attend_rows(i, slot)
            branch_copy(i, own_rows).start()
            attended_copy(i, own_rows).start()

        def early(t, carry):
            for distance in range(1, chips):

                @pl.when(t == min(distance - 1, half - 2))
                def _():
                    for chunk in range(CHUNKS):
                        pass_on(1, distance, chunk)

            @pl.when(t == half - 2)
            def _():
                for j in range(2):
                    relay(half + j)

            total = first_half(t, t % 2)

            @pl.when(t == half - 2)
            def _():
                relay(half + 2)
                for chunk in range(CHUNKS):
                    collect(1, chunk)

            second_half(t, t % 2, total)

            @pl.when(t > 0)
            def _():
                attend(t - 1, (t - 1) % 2)

            return carry

        lax.fori_loop(0, half - 1, early, 0)
        load_wo.wait()
        update(0)
        gathered(1)
        for i in range(half):
            rest_copy(i).wait()

        def pair(t, carry):
            late(half + 2 * t, 2 - 2 * t)

            @pl.when(t == 0)
            def _():
                attend(half - 2, (half - 2) % 2)
                update(1)

            return carry

        lax.fori_loop(0, half // 2, pair, 0)
        total = first_half(half - 1, 4)

        def last(t, carry):
            i = jnp.where(t < half, half + t, half - 1)

            @pl.when(t == 2)
            def _():
                second_half(half - 1, 4, total)
                for j in range(half, half + 2):
                    attended_copy(j, own_rows).start()

            attend_rows(i, jnp.where(t < half, (t + 2) % 4, 4))

            @pl.when(t == half)
            def _():
                corner_copy(i, own_rows).start()

            branch_copy(i, own_rows).start()

            @pl.when(t == half - 1)
            def _():
                update(half - 2)

            return carry

        lax.fori_loop(0, half + 1, last, 0)
        for j in (half + 2, half + 3, half - 1):
            attended_copy(j, own_rows).start()
        settle_weights(1)

        def drain(i, carry):
            partial_copy(i).wait_send()
            branch_copy(i, own_rows).wait_send()

            @pl.when(i < half)
            def _():
                hidden_copy(i).wait_send()

            @pl.when(i >= half)
            def _():
                relay_copy(i, own_rows).wait_send()

            return carry

        lax.fori_loop(0, MICRO, drain, 0)

        def settle(i, carry):
            update(i)
            attended_copy(i, own_rows).wait_send()
            return carry

        lax.fori_loop(half, MICRO, settle, 0)
        settle(half - 1, 0)
        for i in range(half - 1):
            attended_copy(i, own_rows).wait_send()
        corner_copy(half - 1, own_rows).wait_send()

    @pl.when(seg == 0)
    def _():
        first_layer()

    @pl.when(seg == 1)
    def _():
        second_layer()


def cycle_of_two(chips, hidden, exit_layer, lengths, kv_cache, norm_gain, w_qkv, w_out):
    shards = 2
    width = w_qkv.shape[1]
    columns = w_qkv.shape[2]
    query_width = w_out.shape[1]
    head_size = (columns - query_width) // 2
    heads = query_width // head_size
    rows = BLOCK // shards
    span = width // 2
    wide = span + span * 5 // 8
    tokens = exit_layer.shape[0]
    hbm = pl.BlockSpec(memory_space=pltpu.HBM)
    vmem = pl.BlockSpec(memory_space=pltpu.VMEM)
    dma = pltpu.SemaphoreType.DMA((MICRO,))
    pieces = pltpu.SemaphoreType.DMA((chips, CHUNKS))
    bf16 = jnp.bfloat16
    return pl.pallas_call(
        functools.partial(cycle_kernel, (shards, head_size, heads)),
        out_shape=pltpu.VMEM((MICRO * BLOCK, span), bf16),
        in_specs=[hbm, vmem, vmem, hbm, vmem, hbm, hbm],
        out_specs=vmem,
        scratch_shapes=[
            pltpu.VMEM(w_qkv.shape[1:], bf16),
            pltpu.VMEM(w_out.shape[1:], bf16),
            pltpu.VMEM(kv_cache.shape[1:], bf16),
            pltpu.VMEM((MICRO, BLOCK, width), bf16),
            pltpu.VMEM((MICRO, BLOCK, width), bf16),
            pltpu.VMEM((MICRO * BLOCK, 128), jnp.int32),
            pltpu.VMEM((2 * BLOCK, width), bf16),
            pltpu.VMEM((5, BLOCK, columns), jnp.float32),
            pltpu.VMEM((5, BLOCK, 128), jnp.float32),
            pltpu.VMEM((MICRO, rows, columns + 128), bf16),
            pltpu.VMEM((MICRO, rows, columns + 128), bf16),
            pltpu.VMEM((MICRO, BLOCK, query_width), bf16),
            pltpu.VMEM((query_width, wide), bf16),
            pltpu.VMEM((MICRO, BLOCK, query_width), bf16),
            pltpu.SemaphoreType.DMA((3,)),
            dma,
            pltpu.SemaphoreType.DMA((CHUNKS,)),
            pltpu.SemaphoreType.DMA((CHUNKS,)),
        ]
        + [pieces] * 6
        + [dma] * 16,
        compiler_params=pltpu.CompilerParams(
            collective_id=0, has_side_effects=True, vmem_limit_bytes=VMEM_LIMIT
        ),
        name="cycle",
    )(
        hidden[0],
        exit_layer.reshape(1, tokens),
        lengths.reshape(1, tokens),
        kv_cache[0],
        norm_gain,
        w_qkv[0],
        w_out[0],
    )


def chosen(batches, devices, *arguments):
    shards = max(2, devices // 4)
    if shards == 2 and devices // shards == 2:
        return cycle_of_two(batches // 2, *arguments)
    return body(*arguments)


def solution(mesh):
    return jax.shard_map(
        functools.partial(chosen, mesh.shape["blk"], mesh.shape["section"]),
        mesh=mesh,
        in_specs=(
            P("section", "blk", None),
            P("blk"),
            P("blk"),
            P("section", "blk", None, None),
            P("section", None),
            P("section", None, None),
            P("section", None, None),
        ),
        out_specs=P("blk", "section"),
        check_vma=False,
    )
```

```python
import functools
import math

import jax
import jax.numpy as jnp
from jax import lax
from jax.experimental import pallas as pl
from jax.experimental.pallas import tpu as pltpu
from jax.sharding import PartitionSpec as P

BLOCK = 64
MICRO = 8


EPSILON = 1e-05
NEGATIVE = -1e30
VMEM_LIMIT = 60 << 20


def partner(value, axis, distance):
    return lax.ppermute(value, axis, [(i, i ^ 1 << distance) for i in range(lax.axis_size(axis))])


def shifted(value, axis, steps):
    count = lax.axis_size(axis)
    pairs = [(source, (source + steps) % count) for source in range(count)]
    return lax.ppermute(value, axis, pairs)


def body(hidden, exit_layer, lengths, kv_cache, norm_gain, w_qkv, w_out):
    devices = lax.axis_size("section")
    index = lax.axis_index("section")
    shards = max(2, devices // 4)
    cycle_size = devices // shards
    segment_bits = cycle_size.bit_length() - 1
    shard_bits = shards.bit_length() - 1
    segment_index = index // shards
    shard_index = index % shards
    own_blocks = hidden[0]
    gain_row = norm_gain[0].astype(jnp.float32)
    proj_weight = w_qkv[0]
    out_weight = w_out[0]
    cache_all = kv_cache[0]
    query_width = out_weight.shape[0]
    head_size = (proj_weight.shape[1] - query_width) // 2
    heads = query_width // head_size
    quarter = proj_weight.shape[0]
    total_width = quarter * shards
    group_rows = BLOCK // shards
    rounds = MICRO // cycle_size
    context = cache_all.shape[1]
    positions = jnp.arange(context, dtype=jnp.int32)
    blank_block = jnp.zeros((BLOCK, quarter), jnp.bfloat16)

    def advance(carry, microstep):
        incoming, arriving, records = carry
        micro_index = microstep - segment_index
        in_range = (micro_index >= 0) & (micro_index < MICRO)
        slot = jnp.clip(micro_index, 0, MICRO - 1)
        on_turn = microstep % cycle_size == 0
        local_slot = jnp.minimum(microstep // cycle_size, rounds - 1)
        own_block = lax.dynamic_slice_in_dim(own_blocks, local_slot * BLOCK, BLOCK, 0)
        exit_rows = lax.dynamic_slice_in_dim(exit_layer, slot * BLOCK, BLOCK)
        own_lengths = lax.dynamic_slice_in_dim(
            lengths, slot * BLOCK + shard_index * group_rows, group_rows
        )
        own_cache = lax.dynamic_slice_in_dim(cache_all, slot * group_rows, group_rows, 0)
        first_input = jnp.where(on_turn, own_block, arriving)
        entering = jnp.where(segment_index == 0, first_input, incoming)
        active = exit_rows > segment_index
        gate = in_range & (jnp.sum(active.astype(jnp.int32)) > 0)

        def local_partials():
            widened = entering.astype(jnp.float32)
            scaled = (widened * gain_row).astype(jnp.bfloat16)
            return (
                jnp.dot(scaled, proj_weight, preferred_element_type=jnp.float32),
                jnp.sum(widened * widened, axis=1),
            )

        def no_partials():
            return (
                jnp.zeros((BLOCK, proj_weight.shape[1]), jnp.float32),
                jnp.zeros((BLOCK,), jnp.float32),
            )

        partial_proj, partial_squares = lax.cond(gate, local_partials, no_partials)
        kept = (partial_proj, partial_squares)
        for level in range(shard_bits):
            bit = shard_bits - 1 - level
            upper = index >> bit & 1
            halves = tuple(
                (piece.reshape((2, piece.shape[0] // 2) + piece.shape[1:]) for piece in kept)
            )
            keep = tuple((jnp.where(upper == 1, half[1], half[0]) for half in halves))
            send = tuple((jnp.where(upper == 1, half[0], half[1]) for half in halves))
            received = partner(send, "section", bit)
            kept = tuple((first + second for first, second in zip(keep, received)))
        own_proj, own_squares = kept

        def local_attention():
            fitted = own_proj * lax.rsqrt(own_squares / total_width + EPSILON)[:, None]
            query = (fitted[:, :query_width] * (1.0 / math.sqrt(head_size))).astype(jnp.bfloat16)
            query = query.reshape(group_rows, heads, head_size)
            key_new = fitted[:, query_width : query_width + head_size].astype(jnp.bfloat16)
            value_new = fitted[:, query_width + head_size :].astype(jnp.bfloat16)
            scores = jnp.einsum(
                "rhd,rcd->rhc",
                query,
                own_cache[:, :, :head_size],
                preferred_element_type=jnp.float32,
            )
            own = jnp.einsum("rhd,rd->rh", query, key_new, preferred_element_type=jnp.float32)
            usable = (positions[None, :] < own_lengths[:, None])[:, None, :]
            scores = jnp.where(usable, scores, NEGATIVE)
            row_top = jnp.maximum(jnp.max(scores, axis=-1), own)
            raw = jnp.where(usable, jnp.exp(scores - row_top[:, :, None]), jnp.float32(0.0))
            raw_own = jnp.exp(own - row_top)
            total = jnp.sum(raw, axis=-1) + raw_own
            weights = (raw / total[:, :, None]).astype(jnp.bfloat16)
            own_weight = (raw_own / total).astype(jnp.bfloat16)
            attended = jnp.einsum(
                "rhc,rcd->rhd",
                weights,
                own_cache[:, :, head_size:],
                preferred_element_type=jnp.float32,
            )
            attended = (
                attended
                + own_weight.astype(jnp.float32)[:, :, None]
                * value_new.astype(jnp.float32)[:, None, :]
            )
            return attended.astype(jnp.bfloat16).reshape(group_rows, query_width)

        def no_attention():
            return jnp.zeros((group_rows, query_width), jnp.bfloat16)

        collected = lax.cond(gate, local_attention, no_attention)
        for level in range(shard_bits):
            bit = level
            other = partner(collected, "section", bit)
            upper = index >> bit & 1
            collected = jnp.where(
                upper == 1,
                jnp.concatenate([other, collected], 0),
                jnp.concatenate([collected, other], 0),
            )

        def local_update():
            branch_out = jnp.dot(collected, out_weight, preferred_element_type=jnp.float32)
            updated = (entering.astype(jnp.float32) + branch_out).astype(jnp.bfloat16)
            return jnp.where(active[:, None], updated, entering)

        def keep_state():
            return entering

        outgoing = lax.cond(gate, local_update, keep_state)
        leaving = in_range & (exit_rows == segment_index + 1)
        previous = lax.dynamic_slice_in_dim(records, slot * BLOCK, BLOCK, 0)
        records = lax.dynamic_update_slice_in_dim(
            records, jnp.where(leaving[:, None], outgoing, previous), slot * BLOCK, 0
        )
        relayed = jnp.where(on_turn & (segment_index > 0), own_block, arriving)
        incoming, arriving = shifted((outgoing, relayed), "section", shards)
        return ((incoming, arriving, records), None)

    start = (blank_block, blank_block, jnp.zeros((MICRO * BLOCK, quarter), jnp.bfloat16))
    carry, _ = lax.scan(advance, start, jnp.arange(MICRO + cycle_size - 1, dtype=jnp.int32))
    kept = carry[2]
    for level in range(segment_bits):
        bit = shard_bits + segment_bits - 1 - level
        upper = index >> bit & 1
        halves = kept.reshape(kept.shape[0], 2, kept.shape[1] // 2)
        keep = jnp.where(upper == 1, halves[:, 1], halves[:, 0])
        send = jnp.where(upper == 1, halves[:, 0], halves[:, 1])
        received = partner(send, "section", bit)
        kept = (keep.astype(jnp.float32) + received.astype(jnp.float32)).astype(jnp.bfloat16)
    return kept


MESH = pl.DeviceIdType.MESH
CHUNKS = 4
EARLY = 3


def cycle_kernel(
    sizes,
    hidden,
    exits,
    lens,
    cache_hbm,
    gain,
    wq_hbm,
    wo_hbm,
    out,
    wq,
    wo,
    cache,
    stage,
    ready,
    table,
    scaled,
    partial,
    squares,
    psend,
    precv,
    att,
    wx,
    att_in,
    load_sem,
    own_sem,
    wy_send,
    wy_recv,
    up_send,
    up_recv,
    dn_send,
    dn_recv,
    wd_send,
    wd_recv,
    h_send,
    h_recv,
    lo_send,
    lo_recv,
    hi_send,
    hi_recv,
    p_send,
    p_recv,
    a_send,
    a_recv,
    r_send,
    r_recv,
    d_send,
    d_recv,
    x_send,
    x_recv,
):
    shards, head_size, heads = sizes
    index = lax.axis_index("section")
    seg = index // shards
    shard = index % shards
    across = seg * shards + (1 - shard)
    along = (1 - seg) * shards + shard
    corner = (1 - seg) * shards + (1 - shard)
    width = stage.shape[2]
    columns = wq.shape[1]
    query_width = heads * head_size
    half = MICRO // 2
    rows = BLOCK // shards
    span = out.shape[1]
    wide = wx.shape[1]
    low = width - wide
    context = cache.shape[1]
    own_rows = pl.ds(pl.multiple_of(shard * rows, rows), rows)
    other_rows = pl.ds(pl.multiple_of((1 - shard) * rows, rows), rows)

    place_blk = lax.axis_index("blk")
    chips = up_send.shape[0]
    chip = place_blk // 2
    core = place_blk % 2
    chunk_rows = wx.shape[0] // (2 * chips * CHUNKS)
    above = jnp.minimum(chip + 1, chips - 1) * 2 + core
    below = jnp.maximum(chip - 1, 0) * 2 + core
    beside = chip * 2 + 1 - core
    has_above = chip < chips - 1
    has_below = chip > 0

    def remote(source, target, send, recv, device):
        return pltpu.make_async_remote_copy(
            src_ref=source,
            dst_ref=target,
            send_sem=send,
            recv_sem=recv,
            device_id=device,
            device_id_type=MESH,
        )

    barrier = pltpu.get_barrier_semaphore()
    for peer in (across, along, corner):
        pl.semaphore_signal(barrier, inc=1, device_id={"section": peer}, device_id_type=MESH)

    @pl.when(has_above)
    def _():
        pl.semaphore_signal(barrier, inc=1, device_id={"blk": above}, device_id_type=MESH)

    @pl.when(has_below)
    def _():
        pl.semaphore_signal(barrier, inc=1, device_id={"blk": below}, device_id_type=MESH)

    pl.semaphore_signal(barrier, inc=1, device_id={"blk": beside}, device_id_type=MESH)

    def own_copy(i):
        return pltpu.make_async_copy(
            hidden.at[pl.ds(i * BLOCK, BLOCK)], stage.at[i], own_sem.at[i]
        )

    def rest_copy(i):
        return pltpu.make_async_copy(
            hidden.at[pl.ds(i * BLOCK, BLOCK), pl.ds(low, wide)],
            stage.at[half + i, :, pl.ds(low, wide)],
            own_sem.at[i],
        )

    load_wq = pltpu.make_async_copy(wq_hbm, wq, load_sem.at[0])
    load_cache = pltpu.make_async_copy(cache_hbm, cache, load_sem.at[1])
    load_wo = pltpu.make_async_copy(wo_hbm, wo, load_sem.at[2])

    @pl.when(seg == 0)
    def _():
        own_copy(0).start()

    load_wq.start()
    load_cache.start()

    lane = lax.broadcasted_iota(jnp.int32, (128, 128), 1)
    line = lax.broadcasted_iota(jnp.int32, (128, 128), 0)
    for start in range(0, MICRO * BLOCK, 128):
        cols = pl.ds(start, 128)
        depth = jnp.sum(jnp.where(lane == line, exits[:, cols], 0), axis=1, keepdims=True)
        limit = jnp.sum(jnp.where(lane == line, lens[:, cols], 0), axis=1, keepdims=True)
        table[cols, :] = jnp.where(lane == 0, depth, limit)

    def place(i):
        if isinstance(i, int):
            return 2 * i if i < half else 2 * (i - half) + 1
        return jnp.where(i < half, 2 * i, 2 * (i - half) + 1)

    def token_rows(i):
        return pl.ds(pl.multiple_of(place(i) * BLOCK, BLOCK), BLOCK)

    def depths(i):
        return table[token_rows(i), :][:, 0:1]

    def chunk_at(owner, chunk):
        first = pl.multiple_of(owner * (CHUNKS * chunk_rows) + chunk * chunk_rows, chunk_rows)
        return pl.ds(first, chunk_rows)

    def weight_out(layer, chunk):
        at = chunk_at(place_blk, chunk)
        first, size = (low, wide) if layer == 0 else (0, span)
        return remote(
            wo_hbm.at[at, pl.ds(first, size)],
            wx.at[at, pl.ds(0, size)],
            wy_send,
            wy_recv.at[chunk],
            {"section": along},
        )

    def held_size(layer):
        return pl.ds(0, wide if layer == 1 else span)

    def weight_in(layer, chunk):
        part = wx.at[chunk_at(place_blk, chunk), held_size(layer)]
        return remote(part, part, wy_send, wy_recv.at[chunk], {"section": along})

    def upward(layer, owner, chunk):
        part = wx.at[chunk_at(owner * 2 + core, chunk), held_size(layer)]
        return remote(
            part, part, up_send.at[owner], up_recv.at[owner, chunk], {"blk": above}
        )

    def downward(layer, owner, chunk):
        part = wx.at[chunk_at(owner * 2 + core, chunk), held_size(layer)]
        return remote(
            part, part, dn_send.at[owner], dn_recv.at[owner, chunk], {"blk": below}
        )

    def sideways(layer, owner, chunk):
        part = wx.at[chunk_at(owner * 2 + core, chunk), held_size(layer)]
        return remote(part, part, wd_send, wd_recv, {"blk": beside})

    def all_sideways(layer):
        part = wx.at[pl.ds(0, wx.shape[0] // 2), held_size(layer)]
        return remote(part, part, wd_send, wd_recv, {"blk": beside})

    def owned(owner, size):
        rows_held = CHUNKS * chunk_rows
        first = pl.multiple_of((owner * 2 + core) * rows_held, rows_held)
        return wx.at[pl.ds(first, rows_held), pl.ds(0, size)]

    def spread(layer, chunk):
        weight_in(layer, chunk).wait_recv()

        @pl.when(has_above)
        def _():
            upward(layer, chip, chunk).start()

        @pl.when(has_below)
        def _():
            downward(layer, chip, chunk).start()

        sideways(layer, chip, chunk).start()

    def from_below(layer, distance, chunk):
        owner = chip - distance

        @pl.when(owner >= 0)
        def _():
            upward(layer, owner, chunk).wait_recv()

            @pl.when(has_above)
            def _():
                upward(layer, owner, chunk).start()

            sideways(layer, owner, chunk).start()

    def from_above(layer, distance, chunk):
        owner = chip + distance

        @pl.when(owner < chips)
        def _():
            downward(layer, owner, chunk).wait_recv()

            @pl.when(has_below)
            def _():
                downward(layer, owner, chunk).start()

            sideways(layer, owner, chunk).start()

    def pass_on(layer, distance, chunk):
        @pl.when(has_above)
        def _():
            from_below(layer, distance, chunk)

        @pl.when(has_below)
        def _():
            from_above(layer, distance, chunk)

    def collect(layer, chunk):
        for distance in range(1, chips):

            @pl.when(jnp.logical_not(has_above))
            def _():
                from_below(layer, distance, chunk)

            @pl.when(jnp.logical_not(has_below))
            def _():
                from_above(layer, distance, chunk)

    def gathered(layer):
        all_sideways(layer).wait_recv()

    def settle_weights(layer):
        held = wide if layer == 1 else span
        mine = owned(chip, wide if layer == 0 else span)
        remote(mine, mine, wy_send, wy_recv.at[0], {"section": along}).wait_send()
        all_sideways(layer).wait_send()
        for owner in range(chips):
            part = owned(owner, held)

            @pl.when(has_above & (owner <= chip))
            def _():
                remote(
                    part, part, up_send.at[owner], up_recv.at[owner, 0], {"blk": above}
                ).wait_send()

            @pl.when(has_below & (owner >= chip))
            def _():
                remote(
                    part, part, dn_send.at[owner], dn_recv.at[owner, 0], {"blk": below}
                ).wait_send()

    def sent(part, send, receive):
        remote(part, part, send, receive.at[0], {"section": along}).wait_send()

    def hidden_copy(i):
        return remote(
            hidden.at[pl.ds(i * BLOCK, BLOCK)],
            stage.at[half + i],
            h_send,
            h_recv.at[i],
            {"section": along},
        )

    def low_copy(i, size):
        return remote(
            ready.at[i, :, pl.ds(0, size)],
            stage.at[i, :, pl.ds(0, size)],
            lo_send.at[0 if size == span else 1],
            lo_recv.at[i],
            {"section": along},
        )

    def high_copy(i):
        cols = pl.ds(span, span)
        return remote(
            ready.at[i, :, cols],
            stage.at[i, :, cols],
            hi_send,
            hi_recv.at[i],
            {"section": along},
        )

    def branch_copy(i, sent_rows):
        return remote(
            att.at[i, sent_rows],
            att_in.at[i, sent_rows],
            r_send,
            r_recv.at[i],
            {"section": along},
        )

    def corner_copy(i, sent_rows):
        return remote(
            att.at[i, sent_rows],
            att_in.at[i, sent_rows],
            d_send,
            d_recv,
            {"section": corner},
        )

    def relay_copy(i, sent_rows):
        return remote(
            att_in.at[i, sent_rows],
            att_in.at[i, sent_rows],
            x_send,
            x_recv.at[i],
            {"section": across},
        )

    def relay(i):
        branch_copy(i, own_rows).wait_recv()
        relay_copy(i, own_rows).start()

    def partial_copy(i):
        return remote(
            psend.at[i], precv.at[i], p_send, p_recv.at[i], {"section": across}
        )

    def attended_copy(i, sent_rows):
        return remote(
            att.at[i, sent_rows],
            att.at[i, sent_rows],
            a_send,
            a_recv.at[i],
            {"section": across},
        )

    def turn(layer, t):
        last = half if layer == 0 else MICRO - 1
        moved = jnp.where((t >= half - 1) & (t < last), t + 1, t)
        return jnp.where(t == last, half - 1, moved)

    def blocks_at(ref, i, count, cols):
        return ref[pl.ds(i, count), :, cols].reshape(count * BLOCK, cols.size)

    def scale(i, count, first, last):
        total = jnp.zeros((count * BLOCK, 1), jnp.float32)
        for start in range(first, last, 512):
            cols = pl.ds(start, min(512, last - start))
            piece = blocks_at(stage, i, count, cols).astype(jnp.float32)
            total = total + jnp.sum(piece * piece, axis=1, keepdims=True)
            scaled[pl.ds(0, count * BLOCK), cols] = (
                piece * gain[:, cols].astype(jnp.float32)
            ).astype(jnp.bfloat16)
        return total

    def multiply(slot, count, first, last, more):
        step = 512
        for start in range(0, columns, step):
            cols = pl.ds(start, min(step, columns - start))
            product = jnp.dot(
                scaled[pl.ds(0, count * BLOCK), pl.ds(first, last - first)],
                wq[pl.ds(first, last - first), cols],
                preferred_element_type=jnp.float32,
            )
            if more:
                product = blocks_at(partial, slot, count, cols) + product
            partial[pl.ds(slot, count), :, cols] = product.reshape(count, BLOCK, cols.size)

    def send_partial(i, slot):
        psend[i, :, pl.ds(0, columns)] = partial[slot, other_rows, :].astype(jnp.bfloat16)
        theirs = squares[slot, other_rows, :]
        coarse = theirs.astype(jnp.bfloat16)
        fine = (theirs - coarse.astype(jnp.float32)).astype(jnp.bfloat16)
        first = lax.broadcasted_iota(jnp.int32, theirs.shape, 1) == 0
        psend[i, :, pl.ds(columns, 128)] = jnp.where(
            first, coarse.astype(jnp.float32), fine.astype(jnp.float32)
        ).astype(jnp.bfloat16)
        partial_copy(i).start()

    def keep_squares(slot, count, total):
        spread_out = jnp.broadcast_to(total, (count * BLOCK, 128))
        squares[pl.ds(slot, count)] = spread_out.reshape(count, BLOCK, 128)

    def project(i, slot):
        keep_squares(slot, 1, scale(i, 1, 0, width))
        multiply(slot, 1, 0, width, False)
        send_partial(i, slot)

    def attend_rows(i, slot):
        partial_copy(i).wait_recv()
        theirs = precv[i, :, pl.ds(columns, 128)].astype(jnp.float32)
        total_squares = squares[slot, own_rows, :][:, :1] + (theirs[:, :1] + theirs[:, 1:2])
        factor = lax.rsqrt(total_squares / (width * shards) + EPSILON)
        fitted = (
            partial[slot, own_rows, :] + precv[i, :, pl.ds(0, columns)].astype(jnp.float32)
        ) * factor
        scale = 1.0 / math.sqrt(head_size)
        query = jnp.concatenate(
            [fitted[:, h * head_size : (h + 1) * head_size] for h in range(heads)], axis=0
        )
        query = (query * scale).astype(jnp.bfloat16)
        key_new = fitted[:, query_width : query_width + head_size].astype(jnp.bfloat16)
        value_new = fitted[:, query_width + head_size :].astype(jnp.bfloat16)
        key_new = jnp.concatenate([key_new.astype(jnp.float32)] * heads, axis=0)
        value_new = jnp.concatenate([value_new.astype(jnp.float32)] * heads, axis=0)
        start = pl.multiple_of(place(i) * rows, rows)
        held = cache[pl.ds(start, rows)].reshape(rows * context, 2 * head_size)
        scores = lax.dot_general(
            query,
            held[:, :head_size],
            (((1,), (1,)), ((), ())),
            preferred_element_type=jnp.float32,
        )
        own = jnp.sum(query.astype(jnp.float32) * key_new, axis=1, keepdims=True)
        limits = table[pl.ds(pl.multiple_of(place(i) * BLOCK + shard * rows, rows), rows), :][:, 1:2]
        row = lax.broadcasted_iota(jnp.int32, (rows, 1), 0) * context
        first = jnp.concatenate([row] * heads, axis=0)
        last = jnp.concatenate([row + limits] * heads, axis=0)
        column = lax.broadcasted_iota(jnp.int32, scores.shape, 1)
        usable = (column >= first) & (column < last)
        scores = jnp.where(usable, scores, NEGATIVE)
        row_top = jnp.maximum(jnp.max(scores, axis=1, keepdims=True), own)
        raw = jnp.where(usable, jnp.exp(scores - row_top), 0.0)
        raw_own = jnp.exp(own - row_top)
        total = jnp.sum(raw, axis=1, keepdims=True) + raw_own
        weights = (raw / total).astype(jnp.bfloat16)
        own_weight = (raw_own / total).astype(jnp.bfloat16).astype(jnp.float32)
        attended = jnp.dot(
            weights, held[:, head_size:], preferred_element_type=jnp.float32
        )
        attended = (attended + own_weight * value_new).astype(jnp.bfloat16)
        att[i, own_rows, :] = jnp.concatenate(
            [attended[h * rows : (h + 1) * rows] for h in range(heads)], axis=1
        )

    def added(source, weight, before, chosen, target, first, last, shift_weight, shift):
        for start in range(first, last, 512):
            size = min(512, last - start)
            branch = jnp.dot(
                source,
                weight[:, pl.ds(start + shift_weight, size)],
                preferred_element_type=jnp.float32,
            )
            kept = before[:, pl.ds(start, size)].astype(jnp.float32)
            target[:, pl.ds(start + shift, size)] = jnp.where(
                chosen, kept + branch, kept
            ).astype(jnp.bfloat16)

    neighbours = has_above.astype(jnp.int32) + has_below.astype(jnp.int32)
    pl.semaphore_wait(barrier, 4 + neighbours)

    def first_layer():
        for chunk in range(CHUNKS):
            weight_out(0, chunk).start()
        for i in range(1, half):
            own_copy(i).start()
        load_wo.start()

        def update(i):
            attended_copy(i, other_rows).wait_recv()
            active = depths(i) > 0
            fill = functools.partial(added, att[i], wo, stage.at[i], active, ready.at[i])
            fill(0, span, 0, 0)

            @pl.when(i < half - 2)
            def _():
                low_copy(i, span).start()

            @pl.when(i < half)
            def _():
                fill(span, width, 0, 0)

            @pl.when(i < half - 2)
            def _():
                high_copy(i).start()

            if low:

                @pl.when(i >= half)
                def _():
                    low_copy(i, low).start()

            @pl.when(i == MICRO - 1)
            def _():
                low_copy(half - 1, span).start()
                high_copy(half - 1).start()

        def step(t, carry):
            i = turn(0, t)

            @pl.when(i < half)
            def _():
                own_copy(i).wait()

            @pl.when(i >= half)
            def _():
                hidden_copy(i - half).wait_recv()

            @pl.when(t == half - 1)
            def _():
                for chunk in range(EARLY):
                    spread(0, chunk)

            for distance in range(1, chips - 1):

                @pl.when(t == min(half + distance, MICRO - 1))
                def _():
                    for chunk in range(EARLY):
                        pass_on(0, distance, chunk)

            @pl.when(t == 0)
            def _():
                load_wq.wait()

            project(i, 0)

            @pl.when(t == MICRO - 1)
            def _():
                for chunk in range(EARLY, CHUNKS):
                    spread(0, chunk)

            @pl.when(t == 1)
            def _():
                load_wo.wait()

            @pl.when((t > 0) & (t < MICRO - 1))
            def _():
                update(turn(0, t - 1))

            @pl.when(t == 0)
            def _():
                load_cache.wait()

            attend_rows(i, 0)

            @pl.when(i >= half)
            def _():
                branch_copy(i, own_rows).start()

            @pl.when(i == half + 1)
            def _():
                low_copy(half - 2, span).start()

            @pl.when(i == half + 2)
            def _():
                high_copy(half - 2).start()

            attended_copy(i, own_rows).start()

            @pl.when(t == MICRO - 1)
            def _():
                for chunk in range(EARLY, CHUNKS):
                    pass_on(0, 1, chunk)

            @pl.when(t >= MICRO - 2)
            def _():
                update(i)

            return carry

        lax.fori_loop(0, MICRO, step, 0)
        relay(0)
        for chunk in range(EARLY):
            pass_on(0, chips - 1, chunk)
            collect(0, chunk)
        relay(1)
        for distance in range(2, chips):
            for chunk in range(EARLY, CHUNKS):
                pass_on(0, distance, chunk)
        for chunk in range(EARLY, CHUNKS):
            collect(0, chunk)
        for i in range(2, half - 1):
            relay(i)
        gathered(0)

        def finish(i, count):
            for j in range(i, i + count):
                if j == half - 1:
                    branch_copy(j, own_rows).wait_recv()
                    corner_copy(j, other_rows).wait_recv()
                else:
                    relay_copy(j, other_rows).wait_recv()
            source = att_in[pl.ds(i, count)].reshape(count * BLOCK, query_width)
            deep = jnp.concatenate([depths(j) for j in range(i, i + count)], axis=0) > 1
            for start in range(0, span, 512):
                cols = pl.ds(start, min(512, span - start))
                branch = jnp.dot(source, wx[:, cols], preferred_element_type=jnp.float32)
                kept = blocks_at(ready, i, count, cols).astype(jnp.float32)
                now = jnp.where(deep, kept + branch, kept).astype(jnp.bfloat16)
                for j in range(count):
                    out[token_rows(i + j), cols] = now[j * BLOCK : (j + 1) * BLOCK]

        finish(0, 2)
        settle_weights(0)
        relay(half)
        relay(half + 1)
        finish(2, 1)
        relay(half + 2)
        finish(half, 2)
        relay(half + 3)
        sent(psend, p_send, p_recv)
        sent(att.at[:, own_rows], a_send, a_recv)
        sent(att.at[pl.ds(half, half), own_rows], r_send, r_recv)
        early = pl.ds(0, half)
        sent(ready.at[early, :, pl.ds(0, span)], lo_send.at[0], lo_recv)
        sent(ready.at[early, :, pl.ds(span, span)], hi_send, hi_recv)
        if low:
            sent(ready.at[early, :, pl.ds(0, low)], lo_send.at[1], lo_recv)
        finish(half + 2, 2)
        finish(half - 1, 1)
        sent(att_in.at[pl.ds(0, MICRO - 1), own_rows], x_send, x_recv)

    def second_layer():
        hidden_copy(0).start()
        for chunk in range(EARLY):
            weight_out(1, chunk).start()
        for i in range(1, half):
            hidden_copy(i).start()
        for chunk in range(EARLY, CHUNKS):
            weight_out(1, chunk).start()
        for i in range(half):
            rest_copy(i).start()
        load_wo.start()
        load_wq.wait()
        load_cache.wait()
        for chunk in range(CHUNKS):
            spread(1, chunk)

        def first_half(i, slot):
            low_copy(i, span).wait_recv()
            total = scale(i, 1, 0, span)
            multiply(slot, 1, 0, span, False)
            return total

        def second_half(i, slot, total):
            high_copy(i).wait_recv()
            total = total + scale(i, 1, span, width)
            multiply(slot, 1, span, width, True)
            keep_squares(slot, 1, total)
            send_partial(i, slot)

        def late(i, slot):
            for j in range(2):
                relay_copy(i + j, other_rows).wait_recv()
            source = att_in[pl.ds(i, 2)].reshape(2 * BLOCK, query_width)
            active = jnp.concatenate([depths(i), depths(i + 1)], axis=0) > 0
            for start in range(low, width, 512):
                size = min(512, width - start)
                cols = pl.ds(start, size)
                branch = jnp.dot(
                    source, wx[:, pl.ds(start - low, size)], preferred_element_type=jnp.float32
                )
                kept = blocks_at(stage, i, 2, cols).astype(jnp.float32)
                now = jnp.where(active, kept + branch, kept).astype(jnp.bfloat16)
                stage[pl.ds(i, 2), :, cols] = now.reshape(2, BLOCK, size)

            @pl.when(i == half)
            def _():
                relay(half + 3)

            total = scale(i, 2, low, width)
            multiply(slot, 2, low, width, False)
            if low:
                for j in range(2):
                    low_copy(i + j, low).wait_recv()
                total = total + scale(i, 2, 0, low)
                multiply(slot, 2, 0, low, True)
            keep_squares(slot, 2, total)
            for j in range(2):
                send_partial(i + j, slot + j)

        def update(i):
            attended_copy(i, other_rows).wait_recv()
            added(
                att[i],
                wo,
                stage.at[i],
                depths(i) > 1,
                out.at[token_rows(i)],
                span,
                width,
                0,
                -span,
            )

        def attend(i, slot):
            attend_rows(i, slot)
            branch_copy(i, own_rows).start()
            attended_copy(i, own_rows).start()

        def early(t, carry):
            for distance in range(1, chips):

                @pl.when(t == min(distance - 1, half - 2))
                def _():
                    for chunk in range(CHUNKS):
                        pass_on(1, distance, chunk)

            @pl.when(t == half - 2)
            def _():
                for j in range(2):
                    relay(half + j)

            total = first_half(t, t % 2)

            @pl.when(t == half - 2)
            def _():
                relay(half + 2)
                for chunk in range(CHUNKS):
                    collect(1, chunk)

            second_half(t, t % 2, total)

            @pl.when(t > 0)
            def _():
                attend(t - 1, (t - 1) % 2)

            return carry

        lax.fori_loop(0, half - 1, early, 0)
        load_wo.wait()
        update(0)
        gathered(1)
        for i in range(half):
            rest_copy(i).wait()

        def pair(t, carry):
            late(half + 2 * t, 2 - 2 * t)

            @pl.when(t == 0)
            def _():
                attend(half - 2, (half - 2) % 2)
                update(1)

            return carry

        lax.fori_loop(0, half // 2, pair, 0)
        def last(t, carry):
            i = jnp.where(t < half, half + t, half - 1)

            @pl.when(t == 2)
            def _():
                second_half(half - 1, 4, first_half(half - 1, 4))
                for j in range(half, half + 2):
                    attended_copy(j, own_rows).start()

            attend_rows(i, jnp.where(t < half, (t + 2) % 4, 4))

            @pl.when(t == half)
            def _():
                corner_copy(i, own_rows).start()

            branch_copy(i, own_rows).start()

            @pl.when(t == half - 1)
            def _():
                update(half - 2)

            return carry

        lax.fori_loop(0, half + 1, last, 0)
        for j in (half + 2, half + 3, half - 1):
            attended_copy(j, own_rows).start()
        settle_weights(1)
        sent(psend, p_send, p_recv)
        sent(stage.at[pl.ds(half, half)], h_send, h_recv)
        sent(att_in.at[pl.ds(half, half), own_rows], x_send, x_recv)
        lax.fori_loop(half, MICRO, lambda i, carry: update(i), None)
        update(half - 1)
        sent(att.at[:, own_rows], r_send, r_recv)
        sent(att.at[:, own_rows], a_send, a_recv)
        corner_copy(half - 1, own_rows).wait_send()

    @pl.when(seg == 0)
    def _():
        first_layer()

    @pl.when(seg == 1)
    def _():
        second_layer()


def cycle_of_two(chips, hidden, exit_layer, lengths, kv_cache, norm_gain, w_qkv, w_out):
    shards = 2
    width = w_qkv.shape[1]
    columns = w_qkv.shape[2]
    query_width = w_out.shape[1]
    head_size = (columns - query_width) // 2
    heads = query_width // head_size
    rows = BLOCK // shards
    span = width // 2
    wide = span + span * 5 // 8
    tokens = exit_layer.shape[0]
    hbm = pl.BlockSpec(memory_space=pltpu.HBM)
    vmem = pl.BlockSpec(memory_space=pltpu.VMEM)
    one = pltpu.SemaphoreType.DMA
    few = pltpu.SemaphoreType.DMA((MICRO // 2,))
    dma = pltpu.SemaphoreType.DMA((MICRO,))
    pieces = pltpu.SemaphoreType.DMA((chips, CHUNKS))
    bf16 = jnp.bfloat16
    return pl.pallas_call(
        functools.partial(cycle_kernel, (shards, head_size, heads)),
        out_shape=pltpu.VMEM((MICRO * BLOCK, span), bf16),
        in_specs=[hbm, vmem, vmem, hbm, vmem, hbm, hbm],
        out_specs=vmem,
        scratch_shapes=[
            pltpu.VMEM(w_qkv.shape[1:], bf16),
            pltpu.VMEM(w_out.shape[1:], bf16),
            pltpu.VMEM(kv_cache.shape[1:], bf16),
            pltpu.VMEM((MICRO, BLOCK, width), bf16),
            pltpu.VMEM((MICRO, BLOCK, width), bf16),
            pltpu.VMEM((MICRO * BLOCK, 128), jnp.int32),
            pltpu.VMEM((2 * BLOCK, width), bf16),
            pltpu.VMEM((5, BLOCK, columns), jnp.float32),
            pltpu.VMEM((5, BLOCK, 128), jnp.float32),
            pltpu.VMEM((MICRO, rows, columns + 128), bf16),
            pltpu.VMEM((MICRO, rows, columns + 128), bf16),
            pltpu.VMEM((MICRO, BLOCK, query_width), bf16),
            pltpu.VMEM((query_width, wide), bf16),
            pltpu.VMEM((MICRO, BLOCK, query_width), bf16),
            pltpu.SemaphoreType.DMA((3,)),
            few,
            one,
            pltpu.SemaphoreType.DMA((CHUNKS,)),
            pltpu.SemaphoreType.DMA((chips,)),
            pieces,
            pltpu.SemaphoreType.DMA((chips,)),
            pieces,
            one,
            one,
            one,
            few,
            pltpu.SemaphoreType.DMA((2,)),
            dma,
            one,
            few,
            one,
            dma,
            one,
            dma,
            one,
            dma,
            one,
            one,
            one,
            dma,
        ],
        compiler_params=pltpu.CompilerParams(
            collective_id=0, has_side_effects=True, vmem_limit_bytes=VMEM_LIMIT
        ),
        name="cycle",
    )(
        hidden[0],
        exit_layer.reshape(1, tokens),
        lengths.reshape(1, tokens),
        kv_cache[0],
        norm_gain,
        w_qkv[0],
        w_out[0],
    )


def chosen(batches, devices, *arguments):
    shards = max(2, devices // 4)
    if shards == 2 and devices // shards == 2:
        return cycle_of_two(batches // 2, *arguments)
    return body(*arguments)


def solution(mesh):
    return jax.shard_map(
        functools.partial(chosen, mesh.shape["blk"], mesh.shape["section"]),
        mesh=mesh,
        in_specs=(
            P("section", "blk", None),
            P("blk"),
            P("blk"),
            P("section", "blk", None, None),
            P("section", None),
            P("section", None, None),
            P("section", None, None),
        ),
        out_specs=P("blk", "section"),
        check_vma=False,
    )
```

```python
import functools
import math

import jax
import jax.numpy as jnp
from jax import lax
from jax.experimental import pallas as pl
from jax.experimental.pallas import tpu as pltpu
from jax.sharding import PartitionSpec as P

BLOCK = 64
MICRO = 8


EPSILON = 1e-05
NEGATIVE = -1e30
VMEM_LIMIT = 60 << 20


def partner(value, axis, distance):
    return lax.ppermute(value, axis, [(i, i ^ 1 << distance) for i in range(lax.axis_size(axis))])


def shifted(value, axis, steps):
    count = lax.axis_size(axis)
    pairs = [(source, (source + steps) % count) for source in range(count)]
    return lax.ppermute(value, axis, pairs)


def body(hidden, exit_layer, lengths, kv_cache, norm_gain, w_qkv, w_out):
    devices = lax.axis_size("section")
    index = lax.axis_index("section")
    shards = max(2, devices // 4)
    cycle_size = devices // shards
    segment_bits = cycle_size.bit_length() - 1
    shard_bits = shards.bit_length() - 1
    segment_index = index // shards
    shard_index = index % shards
    own_blocks = hidden[0]
    gain_row = norm_gain[0].astype(jnp.float32)
    proj_weight = w_qkv[0]
    out_weight = w_out[0]
    cache_all = kv_cache[0]
    query_width = out_weight.shape[0]
    head_size = (proj_weight.shape[1] - query_width) // 2
    heads = query_width // head_size
    quarter = proj_weight.shape[0]
    total_width = quarter * shards
    group_rows = BLOCK // shards
    rounds = MICRO // cycle_size
    context = cache_all.shape[1]
    positions = jnp.arange(context, dtype=jnp.int32)
    blank_block = jnp.zeros((BLOCK, quarter), jnp.bfloat16)

    def advance(carry, microstep):
        incoming, arriving, records = carry
        micro_index = microstep - segment_index
        in_range = (micro_index >= 0) & (micro_index < MICRO)
        slot = jnp.clip(micro_index, 0, MICRO - 1)
        on_turn = microstep % cycle_size == 0
        local_slot = jnp.minimum(microstep // cycle_size, rounds - 1)
        own_block = lax.dynamic_slice_in_dim(own_blocks, local_slot * BLOCK, BLOCK, 0)
        exit_rows = lax.dynamic_slice_in_dim(exit_layer, slot * BLOCK, BLOCK)
        own_lengths = lax.dynamic_slice_in_dim(
            lengths, slot * BLOCK + shard_index * group_rows, group_rows
        )
        own_cache = lax.dynamic_slice_in_dim(cache_all, slot * group_rows, group_rows, 0)
        first_input = jnp.where(on_turn, own_block, arriving)
        entering = jnp.where(segment_index == 0, first_input, incoming)
        active = exit_rows > segment_index
        gate = in_range & (jnp.sum(active.astype(jnp.int32)) > 0)

        def local_partials():
            widened = entering.astype(jnp.float32)
            scaled = (widened * gain_row).astype(jnp.bfloat16)
            return (
                jnp.dot(scaled, proj_weight, preferred_element_type=jnp.float32),
                jnp.sum(widened * widened, axis=1),
            )

        def no_partials():
            return (
                jnp.zeros((BLOCK, proj_weight.shape[1]), jnp.float32),
                jnp.zeros((BLOCK,), jnp.float32),
            )

        partial_proj, partial_squares = lax.cond(gate, local_partials, no_partials)
        kept = (partial_proj, partial_squares)
        for level in range(shard_bits):
            bit = shard_bits - 1 - level
            upper = index >> bit & 1
            halves = tuple(
                (piece.reshape((2, piece.shape[0] // 2) + piece.shape[1:]) for piece in kept)
            )
            keep = tuple((jnp.where(upper == 1, half[1], half[0]) for half in halves))
            send = tuple((jnp.where(upper == 1, half[0], half[1]) for half in halves))
            received = partner(send, "section", bit)
            kept = tuple((first + second for first, second in zip(keep, received)))
        own_proj, own_squares = kept

        def local_attention():
            fitted = own_proj * lax.rsqrt(own_squares / total_width + EPSILON)[:, None]
            query = (fitted[:, :query_width] * (1.0 / math.sqrt(head_size))).astype(jnp.bfloat16)
            query = query.reshape(group_rows, heads, head_size)
            key_new = fitted[:, query_width : query_width + head_size].astype(jnp.bfloat16)
            value_new = fitted[:, query_width + head_size :].astype(jnp.bfloat16)
            scores = jnp.einsum(
                "rhd,rcd->rhc",
                query,
                own_cache[:, :, :head_size],
                preferred_element_type=jnp.float32,
            )
            own = jnp.einsum("rhd,rd->rh", query, key_new, preferred_element_type=jnp.float32)
            usable = (positions[None, :] < own_lengths[:, None])[:, None, :]
            scores = jnp.where(usable, scores, NEGATIVE)
            row_top = jnp.maximum(jnp.max(scores, axis=-1), own)
            raw = jnp.where(usable, jnp.exp(scores - row_top[:, :, None]), jnp.float32(0.0))
            raw_own = jnp.exp(own - row_top)
            total = jnp.sum(raw, axis=-1) + raw_own
            weights = (raw / total[:, :, None]).astype(jnp.bfloat16)
            own_weight = (raw_own / total).astype(jnp.bfloat16)
            attended = jnp.einsum(
                "rhc,rcd->rhd",
                weights,
                own_cache[:, :, head_size:],
                preferred_element_type=jnp.float32,
            )
            attended = (
                attended
                + own_weight.astype(jnp.float32)[:, :, None]
                * value_new.astype(jnp.float32)[:, None, :]
            )
            return attended.astype(jnp.bfloat16).reshape(group_rows, query_width)

        def no_attention():
            return jnp.zeros((group_rows, query_width), jnp.bfloat16)

        collected = lax.cond(gate, local_attention, no_attention)
        for level in range(shard_bits):
            bit = level
            other = partner(collected, "section", bit)
            upper = index >> bit & 1
            collected = jnp.where(
                upper == 1,
                jnp.concatenate([other, collected], 0),
                jnp.concatenate([collected, other], 0),
            )

        def local_update():
            branch_out = jnp.dot(collected, out_weight, preferred_element_type=jnp.float32)
            updated = (entering.astype(jnp.float32) + branch_out).astype(jnp.bfloat16)
            return jnp.where(active[:, None], updated, entering)

        def keep_state():
            return entering

        outgoing = lax.cond(gate, local_update, keep_state)
        leaving = in_range & (exit_rows == segment_index + 1)
        previous = lax.dynamic_slice_in_dim(records, slot * BLOCK, BLOCK, 0)
        records = lax.dynamic_update_slice_in_dim(
            records, jnp.where(leaving[:, None], outgoing, previous), slot * BLOCK, 0
        )
        relayed = jnp.where(on_turn & (segment_index > 0), own_block, arriving)
        incoming, arriving = shifted((outgoing, relayed), "section", shards)
        return ((incoming, arriving, records), None)

    start = (blank_block, blank_block, jnp.zeros((MICRO * BLOCK, quarter), jnp.bfloat16))
    carry, _ = lax.scan(advance, start, jnp.arange(MICRO + cycle_size - 1, dtype=jnp.int32))
    kept = carry[2]
    for level in range(segment_bits):
        bit = shard_bits + segment_bits - 1 - level
        upper = index >> bit & 1
        halves = kept.reshape(kept.shape[0], 2, kept.shape[1] // 2)
        keep = jnp.where(upper == 1, halves[:, 1], halves[:, 0])
        send = jnp.where(upper == 1, halves[:, 0], halves[:, 1])
        received = partner(send, "section", bit)
        kept = (keep.astype(jnp.float32) + received.astype(jnp.float32)).astype(jnp.bfloat16)
    return kept


MESH = pl.DeviceIdType.MESH
CHUNKS = 4
LIGHT = 4
EARLY = 3


def cycle_kernel(
    sizes,
    hidden,
    exits,
    lens,
    cache_hbm,
    gain,
    wq_hbm,
    wo_hbm,
    out,
    wq,
    wo,
    cache,
    stage,
    ready,
    table,
    scaled,
    partial,
    squares,
    psend,
    precv,
    att,
    wx,
    att_in,
    load_sem,
    own_sem,
    wy_send,
    wy_recv,
    up_send,
    up_recv,
    dn_send,
    dn_recv,
    wd_send,
    wd_recv,
    h_send,
    h_recv,
    lo_send,
    lo_recv,
    hi_send,
    hi_recv,
    p_send,
    p_recv,
    a_send,
    a_recv,
    r_send,
    r_recv,
    d_send,
    d_recv,
    x_send,
    x_recv,
    e_send,
):
    shards, head_size, heads = sizes
    index = lax.axis_index("section")
    seg = index // shards
    shard = index % shards
    across = seg * shards + (1 - shard)
    along = (1 - seg) * shards + shard
    corner = (1 - seg) * shards + (1 - shard)
    width = stage.shape[2]
    columns = wq.shape[1]
    query_width = heads * head_size
    half = MICRO // 2
    rows = BLOCK // shards
    span = out.shape[1]
    wide = wx.shape[1]
    low = width - wide
    context = cache.shape[1]
    own_rows = pl.ds(pl.multiple_of(shard * rows, rows), rows)
    other_rows = pl.ds(pl.multiple_of((1 - shard) * rows, rows), rows)

    place_blk = lax.axis_index("blk")
    chips = up_send.shape[0]
    chip = place_blk // 2
    core = place_blk % 2
    units = CHUNKS + LIGHT
    chunk_rows = wx.shape[0] // (chips * units)
    above = jnp.minimum(chip + 1, chips - 1) * 2 + core
    below = jnp.maximum(chip - 1, 0) * 2 + core
    beside = chip * 2 + 1 - core
    has_above = chip < chips - 1
    has_below = chip > 0

    def remote(source, target, send, recv, device):
        return pltpu.make_async_remote_copy(
            src_ref=source,
            dst_ref=target,
            send_sem=send,
            recv_sem=recv,
            device_id=device,
            device_id_type=MESH,
        )

    barrier = pltpu.get_barrier_semaphore()
    for peer in (across, along, corner):
        pl.semaphore_signal(barrier, inc=1, device_id={"section": peer}, device_id_type=MESH)

    @pl.when(has_above)
    def _():
        pl.semaphore_signal(barrier, inc=1, device_id={"blk": above}, device_id_type=MESH)

    @pl.when(has_below)
    def _():
        pl.semaphore_signal(barrier, inc=1, device_id={"blk": below}, device_id_type=MESH)

    pl.semaphore_signal(barrier, inc=1, device_id={"blk": beside}, device_id_type=MESH)

    def own_copy(i):
        return pltpu.make_async_copy(
            hidden.at[pl.ds(i * BLOCK, BLOCK)], stage.at[i], own_sem.at[i]
        )

    def rest_copy(i):
        return pltpu.make_async_copy(
            hidden.at[pl.ds(i * BLOCK, BLOCK), pl.ds(low, wide)],
            stage.at[half + i, :, pl.ds(low, wide)],
            own_sem.at[i],
        )

    load_wq = pltpu.make_async_copy(wq_hbm, wq, load_sem.at[0])
    load_cache = pltpu.make_async_copy(cache_hbm, cache, load_sem.at[1])
    load_wo = pltpu.make_async_copy(wo_hbm, wo, load_sem.at[2])

    @pl.when(seg == 0)
    def _():
        own_copy(0).start()

    load_wq.start()
    load_cache.start()

    lane = lax.broadcasted_iota(jnp.int32, (128, 128), 1)
    line = lax.broadcasted_iota(jnp.int32, (128, 128), 0)
    for start in range(0, MICRO * BLOCK, 128):
        cols = pl.ds(start, 128)
        depth = jnp.sum(jnp.where(lane == line, exits[:, cols], 0), axis=1, keepdims=True)
        limit = jnp.sum(jnp.where(lane == line, lens[:, cols], 0), axis=1, keepdims=True)
        table[cols, :] = jnp.where(lane == 0, depth, limit)

    def place(i):
        if isinstance(i, int):
            return 2 * i if i < half else 2 * (i - half) + 1
        return jnp.where(i < half, 2 * i, 2 * (i - half) + 1)

    def token_rows(i):
        return pl.ds(pl.multiple_of(place(i) * BLOCK, BLOCK), BLOCK)

    def depths(i):
        return table[token_rows(i), :][:, 0:1]

    def chunk_at(owner, chunk):
        first = (owner * units + core * LIGHT + chunk) * chunk_rows
        return pl.ds(pl.multiple_of(first, chunk_rows), chunk_rows)

    def carried(chunk, action):
        if chunk < LIGHT:
            action()
        else:
            pl.when(core == 1)(action)

    def by_core(action):
        pl.when(core == 0)(functools.partial(action, LIGHT))
        pl.when(core == 1)(functools.partial(action, CHUNKS))

    def weight_out(layer, chunk):
        at = chunk_at(chip, chunk)
        first, size = (low, wide) if layer == 0 else (0, span)
        return remote(
            wo_hbm.at[at, pl.ds(first, size)],
            wx.at[at, pl.ds(0, size)],
            wy_send,
            wy_recv.at[chunk],
            {"section": along},
        )

    def held_size(layer):
        return pl.ds(0, wide if layer == 1 else span)

    def weight_in(layer, chunk):
        part = wx.at[chunk_at(chip, chunk), held_size(layer)]
        return remote(part, part, wy_send, wy_recv.at[chunk], {"section": along})

    def upward(layer, owner, chunk):
        part = wx.at[chunk_at(owner, chunk), held_size(layer)]
        return remote(
            part, part, up_send.at[owner], up_recv.at[owner, chunk], {"blk": above}
        )

    def downward(layer, owner, chunk):
        part = wx.at[chunk_at(owner, chunk), held_size(layer)]
        return remote(
            part, part, dn_send.at[owner], dn_recv.at[owner, chunk], {"blk": below}
        )

    def sideways(layer, owner, chunk):
        part = wx.at[chunk_at(owner, chunk), held_size(layer)]
        return remote(part, part, wd_send, wd_recv, {"blk": beside})

    def all_sideways(layer, count):
        part = wx.at[pl.ds(0, chips * count * chunk_rows), held_size(layer)]
        return remote(part, part, wd_send, wd_recv, {"blk": beside})

    def owned(owner, count, size):
        first = (owner * units + core * LIGHT) * chunk_rows
        rows_held = pl.ds(pl.multiple_of(first, chunk_rows), count * chunk_rows)
        return wx.at[rows_held, pl.ds(0, size)]

    def send_weights(layer, chunk):
        carried(chunk, lambda: weight_out(layer, chunk).start())

    def spread_held(layer, chunk):
        weight_in(layer, chunk).wait_recv()

        @pl.when(has_above)
        def _():
            upward(layer, chip, chunk).start()

        @pl.when(has_below)
        def _():
            downward(layer, chip, chunk).start()

        sideways(layer, chip, chunk).start()

    def from_below(layer, distance, chunk):
        owner = chip - distance

        @pl.when(owner >= 0)
        def _():
            upward(layer, owner, chunk).wait_recv()

            @pl.when(has_above)
            def _():
                upward(layer, owner, chunk).start()

            sideways(layer, owner, chunk).start()

    def from_above(layer, distance, chunk):
        owner = chip + distance

        @pl.when(owner < chips)
        def _():
            downward(layer, owner, chunk).wait_recv()

            @pl.when(has_below)
            def _():
                downward(layer, owner, chunk).start()

            sideways(layer, owner, chunk).start()

    def pass_held(layer, distance, chunk):
        @pl.when(has_above)
        def _():
            from_below(layer, distance, chunk)

        @pl.when(has_below)
        def _():
            from_above(layer, distance, chunk)

    def collect_held(layer, chunk):
        for distance in range(1, chips):

            @pl.when(jnp.logical_not(has_above))
            def _():
                from_below(layer, distance, chunk)

            @pl.when(jnp.logical_not(has_below))
            def _():
                from_above(layer, distance, chunk)

    def spread(layer, chunk):
        carried(chunk, functools.partial(spread_held, layer, chunk))

    def pass_on(layer, distance, chunk):
        carried(chunk, functools.partial(pass_held, layer, distance, chunk))

    def collect(layer, chunk):
        carried(chunk, functools.partial(collect_held, layer, chunk))

    def gathered(layer):
        by_core(lambda count: all_sideways(layer, units - count).wait_recv())

    def settle_weights(layer):
        by_core(functools.partial(settle_held, layer))

    def settle_held(layer, count):
        held = wide if layer == 1 else span
        mine = owned(chip, count, wide if layer == 0 else span)
        remote(mine, mine, wy_send, wy_recv.at[0], {"section": along}).wait_send()
        all_sideways(layer, count).wait_send()
        for owner in range(chips):
            part = owned(owner, count, held)

            @pl.when(has_above & (owner <= chip))
            def _():
                remote(
                    part, part, up_send.at[owner], up_recv.at[owner, 0], {"blk": above}
                ).wait_send()

            @pl.when(has_below & (owner >= chip))
            def _():
                remote(
                    part, part, dn_send.at[owner], dn_recv.at[owner, 0], {"blk": below}
                ).wait_send()

    def sent(part, send, receive):
        remote(part, part, send, receive.at[0], {"section": along}).wait_send()

    def hidden_copy(i):
        return remote(
            hidden.at[pl.ds(i * BLOCK, BLOCK)],
            stage.at[half + i],
            h_send,
            h_recv.at[i],
            {"section": along},
        )

    def low_copy(i, size):
        return remote(
            ready.at[i, :, pl.ds(0, size)],
            stage.at[i, :, pl.ds(0, size)],
            lo_send.at[0 if size == span else 1],
            lo_recv.at[i],
            {"section": along},
        )

    def high_copy(i):
        cols = pl.ds(span, span)
        return remote(
            ready.at[i, :, cols],
            stage.at[i, :, cols],
            hi_send,
            hi_recv.at[i],
            {"section": along},
        )

    def high_part(part):
        cols = pl.ds(span + part * (span // 2), span // 2)
        return remote(
            ready.at[half - 1, :, cols],
            stage.at[half - 1, :, cols],
            hi_send,
            hi_recv.at[half - 1 + part],
            {"section": along},
        )

    def echo_copy(i):
        return remote(
            att_in.at[i, other_rows],
            att.at[i, other_rows],
            e_send,
            a_recv.at[i],
            {"section": along},
        )

    def branch_copy(i, sent_rows):
        return remote(
            att.at[i, sent_rows],
            att_in.at[i, sent_rows],
            r_send,
            r_recv.at[i],
            {"section": along},
        )

    def corner_copy(i, sent_rows):
        return remote(
            att.at[i, sent_rows],
            att_in.at[i, sent_rows],
            d_send,
            d_recv,
            {"section": corner},
        )

    def relay_copy(i, sent_rows):
        return remote(
            att_in.at[i, sent_rows],
            att_in.at[i, sent_rows],
            x_send,
            x_recv.at[i],
            {"section": across},
        )

    def relay(i):
        branch_copy(i, own_rows).wait_recv()
        relay_copy(i, own_rows).start()

    def partial_copy(i):
        return remote(
            psend.at[i], precv.at[i], p_send, p_recv.at[i], {"section": across}
        )

    def attended_copy(i, sent_rows):
        return remote(
            att.at[i, sent_rows],
            att.at[i, sent_rows],
            a_send,
            a_recv.at[i],
            {"section": across},
        )

    def turn(layer, t):
        last = half if layer == 0 else MICRO - 1
        moved = jnp.where((t >= half - 1) & (t < last), t + 1, t)
        return jnp.where(t == last, half - 1, moved)

    def blocks_at(ref, i, count, cols):
        return ref[pl.ds(i, count), :, cols].reshape(count * BLOCK, cols.size)

    def scale(i, count, first, last):
        total = jnp.zeros((count * BLOCK, 1), jnp.float32)
        for start in range(first, last, 512):
            cols = pl.ds(start, min(512, last - start))
            piece = blocks_at(stage, i, count, cols).astype(jnp.float32)
            total = total + jnp.sum(piece * piece, axis=1, keepdims=True)
            scaled[pl.ds(0, count * BLOCK), cols] = (
                piece * gain[:, cols].astype(jnp.float32)
            ).astype(jnp.bfloat16)
        return total

    def multiply(slot, count, first, last, more):
        step = 512
        for start in range(0, columns, step):
            cols = pl.ds(start, min(step, columns - start))
            product = jnp.dot(
                scaled[pl.ds(0, count * BLOCK), pl.ds(first, last - first)],
                wq[pl.ds(first, last - first), cols],
                preferred_element_type=jnp.float32,
            )
            if more:
                product = blocks_at(partial, slot, count, cols) + product
            partial[pl.ds(slot, count), :, cols] = product.reshape(count, BLOCK, cols.size)

    def send_partial(i, slot):
        psend[i, :, pl.ds(0, columns)] = partial[slot, other_rows, :].astype(jnp.bfloat16)
        theirs = squares[slot, other_rows, :]
        coarse = theirs.astype(jnp.bfloat16)
        fine = (theirs - coarse.astype(jnp.float32)).astype(jnp.bfloat16)
        first = lax.broadcasted_iota(jnp.int32, theirs.shape, 1) == 0
        psend[i, :, pl.ds(columns, 128)] = jnp.where(
            first, coarse.astype(jnp.float32), fine.astype(jnp.float32)
        ).astype(jnp.bfloat16)
        partial_copy(i).start()

    def keep_squares(slot, count, total):
        spread_out = jnp.broadcast_to(total, (count * BLOCK, 128))
        squares[pl.ds(slot, count)] = spread_out.reshape(count, BLOCK, 128)

    def project(i, slot):
        keep_squares(slot, 1, scale(i, 1, 0, width))
        multiply(slot, 1, 0, width, False)
        send_partial(i, slot)

    def attend_rows(i, slot):
        partial_copy(i).wait_recv()
        theirs = precv[i, :, pl.ds(columns, 128)].astype(jnp.float32)
        total_squares = squares[slot, own_rows, :][:, :1] + (theirs[:, :1] + theirs[:, 1:2])
        factor = lax.rsqrt(total_squares / (width * shards) + EPSILON)
        fitted = (
            partial[slot, own_rows, :] + precv[i, :, pl.ds(0, columns)].astype(jnp.float32)
        ) * factor
        scale = 1.0 / math.sqrt(head_size)
        query = jnp.concatenate(
            [fitted[:, h * head_size : (h + 1) * head_size] for h in range(heads)], axis=0
        )
        query = (query * scale).astype(jnp.bfloat16)
        key_new = fitted[:, query_width : query_width + head_size].astype(jnp.bfloat16)
        value_new = fitted[:, query_width + head_size :].astype(jnp.bfloat16)
        key_new = jnp.concatenate([key_new.astype(jnp.float32)] * heads, axis=0)
        value_new = jnp.concatenate([value_new.astype(jnp.float32)] * heads, axis=0)
        start = pl.multiple_of(place(i) * rows, rows)
        held = cache[pl.ds(start, rows)].reshape(rows * context, 2 * head_size)
        scores = lax.dot_general(
            query,
            held[:, :head_size],
            (((1,), (1,)), ((), ())),
            preferred_element_type=jnp.float32,
        )
        own = jnp.sum(query.astype(jnp.float32) * key_new, axis=1, keepdims=True)
        limits = table[pl.ds(pl.multiple_of(place(i) * BLOCK + shard * rows, rows), rows), :][:, 1:2]
        row = lax.broadcasted_iota(jnp.int32, (rows, 1), 0) * context
        first = jnp.concatenate([row] * heads, axis=0)
        last = jnp.concatenate([row + limits] * heads, axis=0)
        column = lax.broadcasted_iota(jnp.int32, scores.shape, 1)
        usable = (column >= first) & (column < last)
        scores = jnp.where(usable, scores, NEGATIVE)
        row_top = jnp.maximum(jnp.max(scores, axis=1, keepdims=True), own)
        raw = jnp.where(usable, jnp.exp(scores - row_top), 0.0)
        raw_own = jnp.exp(own - row_top)
        total = jnp.sum(raw, axis=1, keepdims=True) + raw_own
        weights = (raw / total).astype(jnp.bfloat16)
        own_weight = (raw_own / total).astype(jnp.bfloat16).astype(jnp.float32)
        attended = jnp.dot(
            weights, held[:, head_size:], preferred_element_type=jnp.float32
        )
        attended = (attended + own_weight * value_new).astype(jnp.bfloat16)
        att[i, own_rows, :] = jnp.concatenate(
            [attended[h * rows : (h + 1) * rows] for h in range(heads)], axis=1
        )

    def added(source, weight, before, chosen, target, first, last, shift_weight, shift):
        for start in range(first, last, 512):
            size = min(512, last - start)
            branch = jnp.dot(
                source,
                weight[:, pl.ds(start + shift_weight, size)],
                preferred_element_type=jnp.float32,
            )
            kept = before[:, pl.ds(start, size)].astype(jnp.float32)
            target[:, pl.ds(start + shift, size)] = jnp.where(
                chosen, kept + branch, kept
            ).astype(jnp.bfloat16)

    neighbours = has_above.astype(jnp.int32) + has_below.astype(jnp.int32)
    pl.semaphore_wait(barrier, 4 + neighbours)

    def first_layer():
        for chunk in range(CHUNKS):
            send_weights(0, chunk)
        for i in range(1, half):
            own_copy(i).start()
        load_wo.start()

        def update(i):
            attended_copy(i, other_rows).wait_recv()
            active = depths(i) > 0
            fill = functools.partial(added, att[i], wo, stage.at[i], active, ready.at[i])
            fill(0, span, 0, 0)

            @pl.when(i < half - 2)
            def _():
                low_copy(i, span).start()

            @pl.when(i < half)
            def _():
                fill(span, width, 0, 0)

            @pl.when(i < half - 2)
            def _():
                high_copy(i).start()

            if low:

                @pl.when(i >= half)
                def _():
                    low_copy(i, low).start()

            @pl.when(i == MICRO - 1)
            def _():
                low_copy(half - 1, span).start()
                for part in range(2):
                    high_part(part).start()

        def step(t, carry):
            i = turn(0, t)

            @pl.when(i < half)
            def _():
                own_copy(i).wait()

            @pl.when(i >= half)
            def _():
                hidden_copy(i - half).wait_recv()

            @pl.when(t == half - 1)
            def _():
                for chunk in range(EARLY):
                    spread(0, chunk)

            for distance in range(1, chips - 1):

                @pl.when(t == min(half + distance, MICRO - 1))
                def _():
                    for chunk in range(EARLY):
                        pass_on(0, distance, chunk)

            @pl.when(t == 0)
            def _():
                load_wq.wait()

            project(i, 0)

            @pl.when(t == MICRO - 1)
            def _():
                for chunk in range(EARLY, CHUNKS):
                    spread(0, chunk)

            @pl.when(t == 1)
            def _():
                load_wo.wait()

            @pl.when((t > 0) & (t < MICRO - 1))
            def _():
                update(turn(0, t - 1))

            @pl.when(t == 0)
            def _():
                load_cache.wait()

            attend_rows(i, 0)

            @pl.when(i >= half)
            def _():
                branch_copy(i, own_rows).start()

            @pl.when(i == half + 1)
            def _():
                low_copy(half - 2, span).start()

            @pl.when(i == half + 2)
            def _():
                high_copy(half - 2).start()

            attended_copy(i, own_rows).start()

            @pl.when(t == MICRO - 1)
            def _():
                for chunk in range(EARLY, CHUNKS):
                    pass_on(0, 1, chunk)

            @pl.when(t >= MICRO - 2)
            def _():
                update(i)

            return carry

        lax.fori_loop(0, MICRO, step, 0)
        relay(0)
        for chunk in range(EARLY):
            pass_on(0, chips - 1, chunk)
            collect(0, chunk)
        relay(1)
        for distance in range(2, chips):
            for chunk in range(EARLY, CHUNKS):
                pass_on(0, distance, chunk)
        for chunk in range(EARLY, CHUNKS):
            collect(0, chunk)
        for i in range(2, half - 1):
            relay(i)
        gathered(0)

        def finish(i, count):
            for j in range(i, i + count):
                if j == half - 1:
                    branch_copy(j, own_rows).wait_recv()
                    corner_copy(j, other_rows).wait_recv()
                elif j not in (half, half + 1):
                    relay_copy(j, other_rows).wait_recv()
            source = att_in[pl.ds(i, count)].reshape(count * BLOCK, query_width)
            deep = jnp.concatenate([depths(j) for j in range(i, i + count)], axis=0) > 1
            for start in range(0, span, 512):
                cols = pl.ds(start, min(512, span - start))
                branch = jnp.dot(source, wx[:, cols], preferred_element_type=jnp.float32)
                kept = blocks_at(ready, i, count, cols).astype(jnp.float32)
                now = jnp.where(deep, kept + branch, kept).astype(jnp.bfloat16)
                for j in range(count):
                    out[token_rows(i + j), cols] = now[j * BLOCK : (j + 1) * BLOCK]

        finish(0, 2)
        settle_weights(0)
        relay(half)
        relay(half + 1)
        finish(2, 1)
        for j in (half, half + 1):
            relay_copy(j, other_rows).wait_recv()
            echo_copy(j).start()
        relay(half + 2)
        finish(half, 2)
        relay(half + 3)
        sent(psend, p_send, p_recv)
        sent(att.at[:, own_rows], a_send, a_recv)
        sent(att.at[pl.ds(half, half), own_rows], r_send, r_recv)
        early = pl.ds(0, half)
        sent(ready.at[early, :, pl.ds(0, span)], lo_send.at[0], lo_recv)
        sent(ready.at[early, :, pl.ds(span, span)], hi_send, hi_recv)
        if low:
            sent(ready.at[early, :, pl.ds(0, low)], lo_send.at[1], lo_recv)
        finish(half + 2, 2)
        finish(half - 1, 1)
        sent(att_in.at[pl.ds(0, MICRO - 1), own_rows], x_send, x_recv)
        sent(att_in.at[pl.ds(half, 2), other_rows], e_send, a_recv)

    def second_layer():
        hidden_copy(0).start()
        for chunk in range(EARLY):
            send_weights(1, chunk)
        for i in range(1, half):
            hidden_copy(i).start()
        for chunk in range(EARLY, CHUNKS):
            send_weights(1, chunk)
        for i in range(half):
            rest_copy(i).start()
        load_wo.start()
        load_wq.wait()
        load_cache.wait()
        for chunk in range(CHUNKS):
            spread(1, chunk)

        def first_half(i, slot):
            low_copy(i, span).wait_recv()
            keep_squares(slot, 1, scale(i, 1, 0, span))
            multiply(slot, 1, 0, span, False)

        def second_half(i, slot):
            high_copy(i).wait_recv()
            total = squares[slot][:, :1] + scale(i, 1, span, width)
            multiply(slot, 1, span, width, True)
            keep_squares(slot, 1, total)
            send_partial(i, slot)

        def late(i, slot):
            for j in range(2):
                relay_copy(i + j, other_rows).wait_recv()
            source = att_in[pl.ds(i, 2)].reshape(2 * BLOCK, query_width)
            active = jnp.concatenate([depths(i), depths(i + 1)], axis=0) > 0
            for start in range(low, width, 512):
                size = min(512, width - start)
                cols = pl.ds(start, size)
                branch = jnp.dot(
                    source, wx[:, pl.ds(start - low, size)], preferred_element_type=jnp.float32
                )
                kept = blocks_at(stage, i, 2, cols).astype(jnp.float32)
                now = jnp.where(active, kept + branch, kept).astype(jnp.bfloat16)
                stage[pl.ds(i, 2), :, cols] = now.reshape(2, BLOCK, size)

            @pl.when(i == half)
            def _():
                relay(half + 3)

            total = scale(i, 2, low, width)
            multiply(slot, 2, low, width, False)
            if low:
                for j in range(2):
                    low_copy(i + j, low).wait_recv()
                total = total + scale(i, 2, 0, low)
                multiply(slot, 2, 0, low, True)
            keep_squares(slot, 2, total)
            for j in range(2):
                send_partial(i + j, slot + j)

        def update(i):
            attended_copy(i, other_rows).wait_recv()
            added(
                att[i],
                wo,
                stage.at[i],
                depths(i) > 1,
                out.at[token_rows(i)],
                span,
                width,
                0,
                -span,
            )

        def attend(i, slot):
            attend_rows(i, slot)
            branch_copy(i, own_rows).start()
            attended_copy(i, own_rows).start()

        def early(t, carry):
            for distance in range(1, chips):

                @pl.when(t == min(distance - 1, half - 2))
                def _():
                    for chunk in range(CHUNKS):
                        pass_on(1, distance, chunk)

            @pl.when(t == half - 2)
            def _():
                for j in range(2):
                    relay(half + j)

            first_half(t, t % 2)

            @pl.when(t == half - 2)
            def _():
                relay(half + 2)
                for chunk in range(CHUNKS):
                    collect(1, chunk)

            second_half(t, t % 2)

            @pl.when(t > 0)
            def _():
                attend(t - 1, (t - 1) % 2)

            return carry

        lax.fori_loop(0, half - 1, early, 0)
        load_wo.wait()
        update(0)
        gathered(1)
        for i in range(half):
            rest_copy(i).wait()

        def pair(t, carry):
            late(half + 2 * t, 2 - 2 * t)

            @pl.when(t == 0)
            def _():
                attend(half - 2, (half - 2) % 2)
                update(1)

            return carry

        lax.fori_loop(0, half // 2, pair, 0)
        def next_part(part):
            high_part(part).wait_recv()
            first = span + part * (span // 2)
            total = squares[4][:, :1] + scale(half - 1, 1, first, first + span // 2)
            multiply(4, 1, first, first + span // 2, True)
            keep_squares(4, 1, total)

        def last(t, carry):
            i = jnp.where(t < half, half + t, half - 1)

            @pl.when(t == 2)
            def _():
                first_half(half - 1, 4)
                next_part(0)

            attend_rows(i, jnp.where(t < half, (t + 2) % 4, 4))

            @pl.when(t == half)
            def _():
                corner_copy(i, own_rows).start()

            branch_copy(i, own_rows).start()

            @pl.when(t == 2)
            def _():
                next_part(1)
                send_partial(half - 1, 4)
                attended_copy(i, own_rows).start()

            @pl.when(t == half - 1)
            def _():
                update(half - 2)

            return carry

        lax.fori_loop(0, half + 1, last, 0)
        for j in (half + 3, half - 1):
            attended_copy(j, own_rows).start()
        settle_weights(1)
        sent(psend, p_send, p_recv)
        sent(stage.at[pl.ds(half, half)], h_send, h_recv)
        sent(att_in.at[pl.ds(half, half), own_rows], x_send, x_recv)
        lax.fori_loop(half, MICRO, lambda i, carry: update(i), None)
        update(half - 1)
        sent(att.at[:, own_rows], r_send, r_recv)
        sent(att.at[pl.ds(0, MICRO - 2), own_rows], a_send, a_recv)
        corner_copy(half - 1, own_rows).wait_send()

    @pl.when(seg == 0)
    def _():
        first_layer()

    @pl.when(seg == 1)
    def _():
        second_layer()


def cycle_of_two(chips, hidden, exit_layer, lengths, kv_cache, norm_gain, w_qkv, w_out):
    shards = 2
    width = w_qkv.shape[1]
    columns = w_qkv.shape[2]
    query_width = w_out.shape[1]
    head_size = (columns - query_width) // 2
    heads = query_width // head_size
    rows = BLOCK // shards
    span = width // 2
    wide = span + span * 5 // 8
    tokens = exit_layer.shape[0]
    hbm = pl.BlockSpec(memory_space=pltpu.HBM)
    vmem = pl.BlockSpec(memory_space=pltpu.VMEM)
    one = pltpu.SemaphoreType.DMA
    few = pltpu.SemaphoreType.DMA((MICRO // 2,))
    dma = pltpu.SemaphoreType.DMA((MICRO,))
    pieces = pltpu.SemaphoreType.DMA((chips, CHUNKS))
    bf16 = jnp.bfloat16
    return pl.pallas_call(
        functools.partial(cycle_kernel, (shards, head_size, heads)),
        out_shape=pltpu.VMEM((MICRO * BLOCK, span), bf16),
        in_specs=[hbm, vmem, vmem, hbm, vmem, hbm, hbm],
        out_specs=vmem,
        scratch_shapes=[
            pltpu.VMEM(w_qkv.shape[1:], bf16),
            pltpu.VMEM(w_out.shape[1:], bf16),
            pltpu.VMEM(kv_cache.shape[1:], bf16),
            pltpu.VMEM((MICRO, BLOCK, width), bf16),
            pltpu.VMEM((MICRO, BLOCK, width), bf16),
            pltpu.VMEM((MICRO * BLOCK, 128), jnp.int32),
            pltpu.VMEM((2 * BLOCK, width), bf16),
            pltpu.VMEM((5, BLOCK, columns), jnp.float32),
            pltpu.VMEM((5, BLOCK, 128), jnp.float32),
            pltpu.VMEM((MICRO, rows, columns + 128), bf16),
            pltpu.VMEM((MICRO, rows, columns + 128), bf16),
            pltpu.VMEM((MICRO, BLOCK, query_width), bf16),
            pltpu.VMEM((query_width, wide), bf16),
            pltpu.VMEM((MICRO, BLOCK, query_width), bf16),
            pltpu.SemaphoreType.DMA((3,)),
            few,
            one,
            pltpu.SemaphoreType.DMA((CHUNKS,)),
            pltpu.SemaphoreType.DMA((chips,)),
            pieces,
            pltpu.SemaphoreType.DMA((chips,)),
            pieces,
            one,
            one,
            one,
            few,
            pltpu.SemaphoreType.DMA((2,)),
            dma,
            one,
            pltpu.SemaphoreType.DMA((MICRO // 2 + 1,)),
            one,
            dma,
            one,
            dma,
            one,
            dma,
            one,
            one,
            one,
            dma,
            one,
        ],
        compiler_params=pltpu.CompilerParams(
            collective_id=0, has_side_effects=True, vmem_limit_bytes=VMEM_LIMIT
        ),
        name="cycle",
    )(
        hidden[0],
        exit_layer.reshape(1, tokens),
        lengths.reshape(1, tokens),
        kv_cache[0],
        norm_gain,
        w_qkv[0],
        w_out[0],
    )


def chosen(batches, devices, *arguments):
    shards = max(2, devices // 4)
    if shards == 2 and devices // shards == 2:
        return cycle_of_two(batches // 2, *arguments)
    return body(*arguments)


def solution(mesh):
    return jax.shard_map(
        functools.partial(chosen, mesh.shape["blk"], mesh.shape["section"]),
        mesh=mesh,
        in_specs=(
            P("section", "blk", None),
            P("blk"),
            P("blk"),
            P("section", "blk", None, None),
            P("section", None),
            P("section", None, None),
            P("section", None, None),
        ),
        out_specs=P("blk", "section"),
        check_vma=False,
    )
```

```python
import functools
import math

import jax
import jax.numpy as jnp
from jax import lax
from jax.experimental import pallas as pl
from jax.experimental.pallas import tpu as pltpu
from jax.sharding import PartitionSpec as P

BLOCK = 64
MICRO = 8


EPSILON = 1e-05
NEGATIVE = -1e30
VMEM_LIMIT = 60 << 20


def partner(value, axis, distance):
    return lax.ppermute(value, axis, [(i, i ^ 1 << distance) for i in range(lax.axis_size(axis))])


def shifted(value, axis, steps):
    count = lax.axis_size(axis)
    pairs = [(source, (source + steps) % count) for source in range(count)]
    return lax.ppermute(value, axis, pairs)


def body(hidden, exit_layer, lengths, kv_cache, norm_gain, w_qkv, w_out):
    devices = lax.axis_size("section")
    index = lax.axis_index("section")
    shards = max(2, devices // 4)
    cycle_size = devices // shards
    segment_bits = cycle_size.bit_length() - 1
    shard_bits = shards.bit_length() - 1
    segment_index = index // shards
    shard_index = index % shards
    own_blocks = hidden[0]
    gain_row = norm_gain[0].astype(jnp.float32)
    proj_weight = w_qkv[0]
    out_weight = w_out[0]
    cache_all = kv_cache[0]
    query_width = out_weight.shape[0]
    head_size = (proj_weight.shape[1] - query_width) // 2
    heads = query_width // head_size
    quarter = proj_weight.shape[0]
    total_width = quarter * shards
    group_rows = BLOCK // shards
    rounds = MICRO // cycle_size
    context = cache_all.shape[1]
    positions = jnp.arange(context, dtype=jnp.int32)
    blank_block = jnp.zeros((BLOCK, quarter), jnp.bfloat16)

    def advance(carry, microstep):
        incoming, arriving, records = carry
        micro_index = microstep - segment_index
        in_range = (micro_index >= 0) & (micro_index < MICRO)
        slot = jnp.clip(micro_index, 0, MICRO - 1)
        on_turn = microstep % cycle_size == 0
        local_slot = jnp.minimum(microstep // cycle_size, rounds - 1)
        own_block = lax.dynamic_slice_in_dim(own_blocks, local_slot * BLOCK, BLOCK, 0)
        exit_rows = lax.dynamic_slice_in_dim(exit_layer, slot * BLOCK, BLOCK)
        own_lengths = lax.dynamic_slice_in_dim(
            lengths, slot * BLOCK + shard_index * group_rows, group_rows
        )
        own_cache = lax.dynamic_slice_in_dim(cache_all, slot * group_rows, group_rows, 0)
        first_input = jnp.where(on_turn, own_block, arriving)
        entering = jnp.where(segment_index == 0, first_input, incoming)
        active = exit_rows > segment_index
        gate = in_range & (jnp.sum(active.astype(jnp.int32)) > 0)

        def local_partials():
            widened = entering.astype(jnp.float32)
            scaled = (widened * gain_row).astype(jnp.bfloat16)
            return (
                jnp.dot(scaled, proj_weight, preferred_element_type=jnp.float32),
                jnp.sum(widened * widened, axis=1),
            )

        def no_partials():
            return (
                jnp.zeros((BLOCK, proj_weight.shape[1]), jnp.float32),
                jnp.zeros((BLOCK,), jnp.float32),
            )

        partial_proj, partial_squares = lax.cond(gate, local_partials, no_partials)
        kept = (partial_proj, partial_squares)
        for level in range(shard_bits):
            bit = shard_bits - 1 - level
            upper = index >> bit & 1
            halves = tuple(
                (piece.reshape((2, piece.shape[0] // 2) + piece.shape[1:]) for piece in kept)
            )
            keep = tuple((jnp.where(upper == 1, half[1], half[0]) for half in halves))
            send = tuple((jnp.where(upper == 1, half[0], half[1]) for half in halves))
            received = partner(send, "section", bit)
            kept = tuple((first + second for first, second in zip(keep, received)))
        own_proj, own_squares = kept

        def local_attention():
            fitted = own_proj * lax.rsqrt(own_squares / total_width + EPSILON)[:, None]
            query = (fitted[:, :query_width] * (1.0 / math.sqrt(head_size))).astype(jnp.bfloat16)
            query = query.reshape(group_rows, heads, head_size)
            key_new = fitted[:, query_width : query_width + head_size].astype(jnp.bfloat16)
            value_new = fitted[:, query_width + head_size :].astype(jnp.bfloat16)
            scores = jnp.einsum(
                "rhd,rcd->rhc",
                query,
                own_cache[:, :, :head_size],
                preferred_element_type=jnp.float32,
            )
            own = jnp.einsum("rhd,rd->rh", query, key_new, preferred_element_type=jnp.float32)
            usable = (positions[None, :] < own_lengths[:, None])[:, None, :]
            scores = jnp.where(usable, scores, NEGATIVE)
            row_top = jnp.maximum(jnp.max(scores, axis=-1), own)
            raw = jnp.where(usable, jnp.exp(scores - row_top[:, :, None]), jnp.float32(0.0))
            raw_own = jnp.exp(own - row_top)
            total = jnp.sum(raw, axis=-1) + raw_own
            weights = (raw / total[:, :, None]).astype(jnp.bfloat16)
            own_weight = (raw_own / total).astype(jnp.bfloat16)
            attended = jnp.einsum(
                "rhc,rcd->rhd",
                weights,
                own_cache[:, :, head_size:],
                preferred_element_type=jnp.float32,
            )
            attended = (
                attended
                + own_weight.astype(jnp.float32)[:, :, None]
                * value_new.astype(jnp.float32)[:, None, :]
            )
            return attended.astype(jnp.bfloat16).reshape(group_rows, query_width)

        def no_attention():
            return jnp.zeros((group_rows, query_width), jnp.bfloat16)

        collected = lax.cond(gate, local_attention, no_attention)
        for level in range(shard_bits):
            bit = level
            other = partner(collected, "section", bit)
            upper = index >> bit & 1
            collected = jnp.where(
                upper == 1,
                jnp.concatenate([other, collected], 0),
                jnp.concatenate([collected, other], 0),
            )

        def local_update():
            branch_out = jnp.dot(collected, out_weight, preferred_element_type=jnp.float32)
            updated = (entering.astype(jnp.float32) + branch_out).astype(jnp.bfloat16)
            return jnp.where(active[:, None], updated, entering)

        def keep_state():
            return entering

        outgoing = lax.cond(gate, local_update, keep_state)
        leaving = in_range & (exit_rows == segment_index + 1)
        previous = lax.dynamic_slice_in_dim(records, slot * BLOCK, BLOCK, 0)
        records = lax.dynamic_update_slice_in_dim(
            records, jnp.where(leaving[:, None], outgoing, previous), slot * BLOCK, 0
        )
        relayed = jnp.where(on_turn & (segment_index > 0), own_block, arriving)
        incoming, arriving = shifted((outgoing, relayed), "section", shards)
        return ((incoming, arriving, records), None)

    start = (blank_block, blank_block, jnp.zeros((MICRO * BLOCK, quarter), jnp.bfloat16))
    carry, _ = lax.scan(advance, start, jnp.arange(MICRO + cycle_size - 1, dtype=jnp.int32))
    kept = carry[2]
    for level in range(segment_bits):
        bit = shard_bits + segment_bits - 1 - level
        upper = index >> bit & 1
        halves = kept.reshape(kept.shape[0], 2, kept.shape[1] // 2)
        keep = jnp.where(upper == 1, halves[:, 1], halves[:, 0])
        send = jnp.where(upper == 1, halves[:, 0], halves[:, 1])
        received = partner(send, "section", bit)
        kept = (keep.astype(jnp.float32) + received.astype(jnp.float32)).astype(jnp.bfloat16)
    return kept


MESH = pl.DeviceIdType.MESH
CHUNKS = 4
LIGHT = 4
EARLY = 3


def cycle_kernel(
    sizes,
    hidden,
    exits,
    lens,
    cache_hbm,
    gain,
    wq_hbm,
    wo_hbm,
    out,
    wq,
    wo,
    cache,
    stage,
    ready,
    table,
    scaled,
    partial,
    squares,
    psend,
    precv,
    att,
    wx,
    att_in,
    load_sem,
    own_sem,
    wy_send,
    wy_recv,
    up_send,
    up_recv,
    dn_send,
    dn_recv,
    wd_send,
    wd_recv,
    h_send,
    h_recv,
    lo_send,
    lo_recv,
    hi_send,
    hi_recv,
    p_send,
    p_recv,
    a_send,
    a_recv,
    r_send,
    r_recv,
    d_send,
    d_recv,
    x_send,
    x_recv,
    e_send,
):
    shards, head_size, heads = sizes
    index = lax.axis_index("section")
    seg = index // shards
    shard = index % shards
    across = seg * shards + (1 - shard)
    along = (1 - seg) * shards + shard
    corner = (1 - seg) * shards + (1 - shard)
    width = stage.shape[2]
    columns = wq.shape[1]
    query_width = heads * head_size
    half = MICRO // 2
    rows = BLOCK // shards
    span = out.shape[1]
    wide = wx.shape[1]
    low = width - wide
    context = cache.shape[1]
    own_rows = pl.ds(pl.multiple_of(shard * rows, rows), rows)
    other_rows = pl.ds(pl.multiple_of((1 - shard) * rows, rows), rows)

    place_blk = lax.axis_index("blk")
    chips = up_send.shape[0]
    chip = place_blk // 2
    core = place_blk % 2
    units = CHUNKS + LIGHT
    chunk_rows = wx.shape[0] // (chips * units)
    above = jnp.minimum(chip + 1, chips - 1) * 2 + core
    below = jnp.maximum(chip - 1, 0) * 2 + core
    beside = chip * 2 + 1 - core
    has_above = chip < chips - 1
    has_below = chip > 0

    def remote(source, target, send, recv, device):
        return pltpu.make_async_remote_copy(
            src_ref=source,
            dst_ref=target,
            send_sem=send,
            recv_sem=recv,
            device_id=device,
            device_id_type=MESH,
        )

    barrier = pltpu.get_barrier_semaphore()
    for peer in (across, along, corner):
        pl.semaphore_signal(barrier, inc=1, device_id={"section": peer}, device_id_type=MESH)

    @pl.when(has_above)
    def _():
        pl.semaphore_signal(barrier, inc=1, device_id={"blk": above}, device_id_type=MESH)

    @pl.when(has_below)
    def _():
        pl.semaphore_signal(barrier, inc=1, device_id={"blk": below}, device_id_type=MESH)

    pl.semaphore_signal(barrier, inc=1, device_id={"blk": beside}, device_id_type=MESH)

    def own_copy(i):
        return pltpu.make_async_copy(
            hidden.at[pl.ds(i * BLOCK, BLOCK)], stage.at[i], own_sem.at[i]
        )

    def rest_copy(i):
        return pltpu.make_async_copy(
            hidden.at[pl.ds(i * BLOCK, BLOCK), pl.ds(low, wide)],
            stage.at[half + i, :, pl.ds(low, wide)],
            own_sem.at[i],
        )

    load_wq = pltpu.make_async_copy(wq_hbm, wq, load_sem.at[0])
    load_cache = pltpu.make_async_copy(cache_hbm, cache, load_sem.at[1])
    load_wo = pltpu.make_async_copy(wo_hbm, wo, load_sem.at[2])

    @pl.when(seg == 0)
    def _():
        own_copy(0).start()

    load_wq.start()
    load_cache.start()

    lane = lax.broadcasted_iota(jnp.int32, (128, 128), 1)
    line = lax.broadcasted_iota(jnp.int32, (128, 128), 0)
    for start in range(0, MICRO * BLOCK, 128):
        cols = pl.ds(start, 128)
        depth = jnp.sum(jnp.where(lane == line, exits[:, cols], 0), axis=1, keepdims=True)
        limit = jnp.sum(jnp.where(lane == line, lens[:, cols], 0), axis=1, keepdims=True)
        table[cols, :] = jnp.where(lane == 0, depth, limit)

    def place(i):
        if isinstance(i, int):
            return 2 * i if i < half else 2 * (i - half) + 1
        return jnp.where(i < half, 2 * i, 2 * (i - half) + 1)

    def token_rows(i):
        return pl.ds(pl.multiple_of(place(i) * BLOCK, BLOCK), BLOCK)

    def depths(i):
        return table[token_rows(i), :][:, 0:1]

    def chunk_at(owner, chunk):
        first = (owner * units + core * LIGHT + chunk) * chunk_rows
        return pl.ds(pl.multiple_of(first, chunk_rows), chunk_rows)

    def carried(chunk, action):
        if chunk < LIGHT:
            action()
        else:
            pl.when(core == 1)(action)

    def by_core(action):
        pl.when(core == 0)(functools.partial(action, LIGHT))
        pl.when(core == 1)(functools.partial(action, CHUNKS))

    def weight_out(layer, chunk):
        at = chunk_at(chip, chunk)
        first, size = (low, wide) if layer == 0 else (0, span)
        return remote(
            wo_hbm.at[at, pl.ds(first, size)],
            wx.at[at, pl.ds(0, size)],
            wy_send,
            wy_recv.at[chunk],
            {"section": along},
        )

    def held_size(layer):
        return pl.ds(0, wide if layer == 1 else span)

    def weight_in(layer, chunk):
        part = wx.at[chunk_at(chip, chunk), held_size(layer)]
        return remote(part, part, wy_send, wy_recv.at[chunk], {"section": along})

    def upward(layer, owner, chunk):
        part = wx.at[chunk_at(owner, chunk), held_size(layer)]
        return remote(
            part, part, up_send.at[owner], up_recv.at[owner, chunk], {"blk": above}
        )

    def downward(layer, owner, chunk):
        part = wx.at[chunk_at(owner, chunk), held_size(layer)]
        return remote(
            part, part, dn_send.at[owner], dn_recv.at[owner, chunk], {"blk": below}
        )

    def sideways(layer, owner, chunk):
        part = wx.at[chunk_at(owner, chunk), held_size(layer)]
        return remote(part, part, wd_send, wd_recv, {"blk": beside})

    def all_sideways(layer, count):
        part = wx.at[pl.ds(0, chips * count * chunk_rows), held_size(layer)]
        return remote(part, part, wd_send, wd_recv, {"blk": beside})

    def owned(owner, count, size):
        first = (owner * units + core * LIGHT) * chunk_rows
        rows_held = pl.ds(pl.multiple_of(first, chunk_rows), count * chunk_rows)
        return wx.at[rows_held, pl.ds(0, size)]

    def send_weights(layer, chunk):
        carried(chunk, lambda: weight_out(layer, chunk).start())

    def spread_held(layer, chunk):
        weight_in(layer, chunk).wait_recv()

        @pl.when(has_above)
        def _():
            upward(layer, chip, chunk).start()

        @pl.when(has_below)
        def _():
            downward(layer, chip, chunk).start()

        sideways(layer, chip, chunk).start()

    def from_below(layer, distance, chunk):
        owner = chip - distance

        @pl.when(owner >= 0)
        def _():
            upward(layer, owner, chunk).wait_recv()

            @pl.when(has_above)
            def _():
                upward(layer, owner, chunk).start()

            sideways(layer, owner, chunk).start()

    def from_above(layer, distance, chunk):
        owner = chip + distance

        @pl.when(owner < chips)
        def _():
            downward(layer, owner, chunk).wait_recv()

            @pl.when(has_below)
            def _():
                downward(layer, owner, chunk).start()

            sideways(layer, owner, chunk).start()

    def pass_held(layer, distance, chunk):
        @pl.when(has_above)
        def _():
            from_below(layer, distance, chunk)

        @pl.when(has_below)
        def _():
            from_above(layer, distance, chunk)

    def collect_held(layer, chunk):
        for distance in range(1, chips):

            @pl.when(jnp.logical_not(has_above))
            def _():
                from_below(layer, distance, chunk)

            @pl.when(jnp.logical_not(has_below))
            def _():
                from_above(layer, distance, chunk)

    def spread(layer, chunk):
        carried(chunk, functools.partial(spread_held, layer, chunk))

    def pass_on(layer, distance, chunk):
        carried(chunk, functools.partial(pass_held, layer, distance, chunk))

    def collect(layer, chunk):
        carried(chunk, functools.partial(collect_held, layer, chunk))

    def gathered(layer):
        by_core(lambda count: all_sideways(layer, units - count).wait_recv())

    def settle_weights(layer):
        by_core(functools.partial(settle_held, layer))

    def settle_held(layer, count):
        held = wide if layer == 1 else span
        mine = owned(chip, count, wide if layer == 0 else span)
        remote(mine, mine, wy_send, wy_recv.at[0], {"section": along}).wait_send()
        all_sideways(layer, count).wait_send()
        for owner in range(chips):
            part = owned(owner, count, held)

            @pl.when(has_above & (owner <= chip))
            def _():
                remote(
                    part, part, up_send.at[owner], up_recv.at[owner, 0], {"blk": above}
                ).wait_send()

            @pl.when(has_below & (owner >= chip))
            def _():
                remote(
                    part, part, dn_send.at[owner], dn_recv.at[owner, 0], {"blk": below}
                ).wait_send()

    def sent(part, send, receive):
        remote(part, part, send, receive.at[0], {"section": along}).wait_send()

    def hidden_copy(i):
        return remote(
            hidden.at[pl.ds(i * BLOCK, BLOCK)],
            stage.at[half + i],
            h_send,
            h_recv.at[i],
            {"section": along},
        )

    def low_copy(i, size):
        return remote(
            ready.at[i, :, pl.ds(0, size)],
            stage.at[i, :, pl.ds(0, size)],
            lo_send.at[0 if size == span else 1],
            lo_recv.at[i],
            {"section": along},
        )

    def high_copy(i):
        cols = pl.ds(span, span)
        return remote(
            ready.at[i, :, cols],
            stage.at[i, :, cols],
            hi_send,
            hi_recv.at[i],
            {"section": along},
        )

    def high_part(part):
        cols = pl.ds(span + part * (span // 2), span // 2)
        return remote(
            ready.at[half - 1, :, cols],
            stage.at[half - 1, :, cols],
            hi_send,
            hi_recv.at[half - 1 + part],
            {"section": along},
        )

    def low_part(part):
        cols = pl.ds(part * (span // 2), span // 2)
        return remote(
            ready.at[half - 1, :, cols],
            stage.at[half - 1, :, cols],
            lo_send.at[0],
            lo_recv.at[half - 1 if part else MICRO],
            {"section": along},
        )

    def echo_copy(i):
        return remote(
            att_in.at[i, other_rows],
            att.at[i, other_rows],
            e_send,
            a_recv.at[i],
            {"section": along},
        )

    def branch_copy(i, sent_rows):
        return remote(
            att.at[i, sent_rows],
            att_in.at[i, sent_rows],
            r_send,
            r_recv.at[i],
            {"section": along},
        )

    def corner_copy(i, sent_rows):
        return remote(
            att.at[i, sent_rows],
            att_in.at[i, sent_rows],
            d_send.at[0 if i == half - 1 else 1],
            d_recv.at[0 if i == half - 1 else 1],
            {"section": corner},
        )

    def relay_copy(i, sent_rows):
        return remote(
            att_in.at[i, sent_rows],
            att_in.at[i, sent_rows],
            x_send,
            x_recv.at[i],
            {"section": across},
        )

    def relay(i):
        branch_copy(i, own_rows).wait_recv()
        relay_copy(i, own_rows).start()

    def partial_copy(i):
        return remote(
            psend.at[i], precv.at[i], p_send, p_recv.at[i], {"section": across}
        )

    def attended_copy(i, sent_rows):
        return remote(
            att.at[i, sent_rows],
            att.at[i, sent_rows],
            a_send,
            a_recv.at[i],
            {"section": across},
        )

    def turn(layer, t):
        last = half if layer == 0 else MICRO - 1
        moved = jnp.where((t >= half - 1) & (t < last), t + 1, t)
        return jnp.where(t == last, half - 1, moved)

    def blocks_at(ref, i, count, cols):
        return ref[pl.ds(i, count), :, cols].reshape(count * BLOCK, cols.size)

    def scale(i, count, first, last):
        total = jnp.zeros((count * BLOCK, 1), jnp.float32)
        for start in range(first, last, 512):
            cols = pl.ds(start, min(512, last - start))
            piece = blocks_at(stage, i, count, cols).astype(jnp.float32)
            total = total + jnp.sum(piece * piece, axis=1, keepdims=True)
            scaled[pl.ds(0, count * BLOCK), cols] = (
                piece * gain[:, cols].astype(jnp.float32)
            ).astype(jnp.bfloat16)
        return total

    def multiply(slot, count, first, last, more):
        step = 512
        for start in range(0, columns, step):
            cols = pl.ds(start, min(step, columns - start))
            product = jnp.dot(
                scaled[pl.ds(0, count * BLOCK), pl.ds(first, last - first)],
                wq[pl.ds(first, last - first), cols],
                preferred_element_type=jnp.float32,
            )
            if more:
                product = blocks_at(partial, slot, count, cols) + product
            partial[pl.ds(slot, count), :, cols] = product.reshape(count, BLOCK, cols.size)

    def send_partial(i, slot):
        psend[i, :, pl.ds(0, columns)] = partial[slot, other_rows, :].astype(jnp.bfloat16)
        theirs = squares[slot, other_rows, :]
        coarse = theirs.astype(jnp.bfloat16)
        fine = (theirs - coarse.astype(jnp.float32)).astype(jnp.bfloat16)
        first = lax.broadcasted_iota(jnp.int32, theirs.shape, 1) == 0
        psend[i, :, pl.ds(columns, 128)] = jnp.where(
            first, coarse.astype(jnp.float32), fine.astype(jnp.float32)
        ).astype(jnp.bfloat16)
        partial_copy(i).start()

    def keep_squares(slot, count, total):
        spread_out = jnp.broadcast_to(total, (count * BLOCK, 128))
        squares[pl.ds(slot, count)] = spread_out.reshape(count, BLOCK, 128)

    def project(i, slot):
        keep_squares(slot, 1, scale(i, 1, 0, width))
        multiply(slot, 1, 0, width, False)
        send_partial(i, slot)

    def attend_rows(i, slot):
        partial_copy(i).wait_recv()
        theirs = precv[i, :, pl.ds(columns, 128)].astype(jnp.float32)
        total_squares = squares[slot, own_rows, :][:, :1] + (theirs[:, :1] + theirs[:, 1:2])
        factor = lax.rsqrt(total_squares / (width * shards) + EPSILON)
        fitted = (
            partial[slot, own_rows, :] + precv[i, :, pl.ds(0, columns)].astype(jnp.float32)
        ) * factor
        scale = 1.0 / math.sqrt(head_size)
        query = jnp.concatenate(
            [fitted[:, h * head_size : (h + 1) * head_size] for h in range(heads)], axis=0
        )
        query = (query * scale).astype(jnp.bfloat16)
        key_new = fitted[:, query_width : query_width + head_size].astype(jnp.bfloat16)
        value_new = fitted[:, query_width + head_size :].astype(jnp.bfloat16)
        key_new = jnp.concatenate([key_new.astype(jnp.float32)] * heads, axis=0)
        value_new = jnp.concatenate([value_new.astype(jnp.float32)] * heads, axis=0)
        start = pl.multiple_of(place(i) * rows, rows)
        held = cache[pl.ds(start, rows)].reshape(rows * context, 2 * head_size)
        scores = lax.dot_general(
            query,
            held[:, :head_size],
            (((1,), (1,)), ((), ())),
            preferred_element_type=jnp.float32,
        )
        own = jnp.sum(query.astype(jnp.float32) * key_new, axis=1, keepdims=True)
        limits = table[pl.ds(pl.multiple_of(place(i) * BLOCK + shard * rows, rows), rows), :][:, 1:2]
        row = lax.broadcasted_iota(jnp.int32, (rows, 1), 0) * context
        first = jnp.concatenate([row] * heads, axis=0)
        last = jnp.concatenate([row + limits] * heads, axis=0)
        column = lax.broadcasted_iota(jnp.int32, scores.shape, 1)
        usable = (column >= first) & (column < last)
        scores = jnp.where(usable, scores, NEGATIVE)
        row_top = jnp.maximum(jnp.max(scores, axis=1, keepdims=True), own)
        raw = jnp.where(usable, jnp.exp(scores - row_top), 0.0)
        raw_own = jnp.exp(own - row_top)
        total = jnp.sum(raw, axis=1, keepdims=True) + raw_own
        weights = (raw / total).astype(jnp.bfloat16)
        own_weight = (raw_own / total).astype(jnp.bfloat16).astype(jnp.float32)
        attended = jnp.dot(
            weights, held[:, head_size:], preferred_element_type=jnp.float32
        )
        attended = (attended + own_weight * value_new).astype(jnp.bfloat16)
        att[i, own_rows, :] = jnp.concatenate(
            [attended[h * rows : (h + 1) * rows] for h in range(heads)], axis=1
        )

    def added(source, weight, before, chosen, target, first, last, shift_weight, shift):
        for start in range(first, last, 512):
            size = min(512, last - start)
            branch = jnp.dot(
                source,
                weight[:, pl.ds(start + shift_weight, size)],
                preferred_element_type=jnp.float32,
            )
            kept = before[:, pl.ds(start, size)].astype(jnp.float32)
            target[:, pl.ds(start + shift, size)] = jnp.where(
                chosen, kept + branch, kept
            ).astype(jnp.bfloat16)

    neighbours = has_above.astype(jnp.int32) + has_below.astype(jnp.int32)
    pl.semaphore_wait(barrier, 4 + neighbours)

    def first_layer():
        for chunk in range(CHUNKS):
            send_weights(0, chunk)
        for i in range(1, half):
            own_copy(i).start()
        load_wo.start()

        def update(i):
            attended_copy(i, other_rows).wait_recv()
            active = depths(i) > 0
            fill = functools.partial(added, att[i], wo, stage.at[i], active, ready.at[i])
            fill(0, span, 0, 0)

            @pl.when(i < half - 2)
            def _():
                low_copy(i, span).start()

            @pl.when(i < half)
            def _():
                fill(span, width, 0, 0)

            @pl.when(i < half - 2)
            def _():
                high_copy(i).start()

            if low:

                @pl.when(i >= half)
                def _():
                    low_copy(i, low).start()

            @pl.when(i == MICRO - 1)
            def _():
                low_part(1).start()
                for part in range(2):
                    high_part(part).start()

        def step(t, carry):
            i = turn(0, t)

            @pl.when(i < half)
            def _():
                own_copy(i).wait()

            @pl.when(i >= half)
            def _():
                hidden_copy(i - half).wait_recv()

            @pl.when(t == half - 1)
            def _():
                for chunk in range(EARLY):
                    spread(0, chunk)

            for distance in range(1, chips - 1):

                @pl.when(t == min(half + distance, MICRO - 1))
                def _():
                    for chunk in range(EARLY):
                        pass_on(0, distance, chunk)

            @pl.when(t == 0)
            def _():
                load_wq.wait()

            project(i, 0)

            @pl.when(t == MICRO - 1)
            def _():
                for chunk in range(EARLY, CHUNKS):
                    spread(0, chunk)

            @pl.when(t == 1)
            def _():
                load_wo.wait()

            @pl.when((t > 0) & (t < MICRO - 1))
            def _():
                update(turn(0, t - 1))

            @pl.when(t == 0)
            def _():
                load_cache.wait()

            attend_rows(i, 0)

            @pl.when(i >= half)
            def _():
                branch_copy(i, own_rows).start()

            @pl.when(i == MICRO - 1)
            def _():
                low_part(0).start()

            @pl.when(i == half + 1)
            def _():
                low_copy(half - 2, span).start()

            @pl.when(i == half + 2)
            def _():
                high_copy(half - 2).start()

            attended_copy(i, own_rows).start()

            @pl.when(t == MICRO - 1)
            def _():
                for chunk in range(EARLY, CHUNKS):
                    pass_on(0, 1, chunk)

            @pl.when(t >= MICRO - 2)
            def _():
                update(i)

            return carry

        lax.fori_loop(0, MICRO, step, 0)
        relay(0)
        for chunk in range(EARLY):
            pass_on(0, chips - 1, chunk)
            collect(0, chunk)
        relay(1)
        for distance in range(2, chips):
            for chunk in range(EARLY, CHUNKS):
                pass_on(0, distance, chunk)
        for chunk in range(EARLY, CHUNKS):
            collect(0, chunk)
        for i in range(2, half - 1):
            relay(i)
        gathered(0)

        def finish(i, count):
            for j in range(i, i + count):
                if j in (half - 1, MICRO - 1):
                    branch_copy(j, own_rows).wait_recv()
                    corner_copy(j, other_rows).wait_recv()
                elif j not in (half, half + 1):
                    relay_copy(j, other_rows).wait_recv()
            source = att_in[pl.ds(i, count)].reshape(count * BLOCK, query_width)
            deep = jnp.concatenate([depths(j) for j in range(i, i + count)], axis=0) > 1
            for start in range(0, span, 512):
                cols = pl.ds(start, min(512, span - start))
                branch = jnp.dot(source, wx[:, cols], preferred_element_type=jnp.float32)
                kept = blocks_at(ready, i, count, cols).astype(jnp.float32)
                now = jnp.where(deep, kept + branch, kept).astype(jnp.bfloat16)
                for j in range(count):
                    out[token_rows(i + j), cols] = now[j * BLOCK : (j + 1) * BLOCK]

        finish(0, 2)
        settle_weights(0)
        relay(half)
        relay(half + 1)
        finish(2, 1)
        for j in (half, half + 1):
            relay_copy(j, other_rows).wait_recv()
            echo_copy(j).start()
        relay(half + 2)
        finish(half, 2)
        sent(psend, p_send, p_recv)
        sent(att.at[:, own_rows], a_send, a_recv)
        sent(att.at[pl.ds(half, half), own_rows], r_send, r_recv)
        early = pl.ds(0, half)
        sent(ready.at[early, :, pl.ds(0, span)], lo_send.at[0], lo_recv)
        sent(ready.at[early, :, pl.ds(span, span)], hi_send, hi_recv)
        if low:
            sent(ready.at[early, :, pl.ds(0, low)], lo_send.at[1], lo_recv)
        finish(half + 2, 2)
        finish(half - 1, 1)
        sent(att_in.at[pl.ds(0, MICRO - 2), own_rows], x_send, x_recv)
        sent(att_in.at[pl.ds(half, 2), other_rows], e_send, a_recv)

    def second_layer():
        hidden_copy(0).start()
        for chunk in range(EARLY):
            send_weights(1, chunk)
        for i in range(1, half):
            hidden_copy(i).start()
        for chunk in range(EARLY, CHUNKS):
            send_weights(1, chunk)
        for i in range(half):
            rest_copy(i).start()
        load_wo.start()
        load_wq.wait()
        load_cache.wait()
        for chunk in range(CHUNKS):
            spread(1, chunk)

        def first_half(i, slot):
            if isinstance(i, int):
                for part in range(2):
                    low_part(part).wait_recv()
            else:
                low_copy(i, span).wait_recv()
            keep_squares(slot, 1, scale(i, 1, 0, span))
            multiply(slot, 1, 0, span, False)

        def second_half(i, slot):
            high_copy(i).wait_recv()
            total = squares[slot][:, :1] + scale(i, 1, span, width)
            multiply(slot, 1, span, width, True)
            keep_squares(slot, 1, total)
            send_partial(i, slot)

        def late(i, slot):
            for j in range(2):
                relay_copy(i + j, other_rows).wait_recv()
            source = att_in[pl.ds(i, 2)].reshape(2 * BLOCK, query_width)
            active = jnp.concatenate([depths(i), depths(i + 1)], axis=0) > 0
            for start in range(low, width, 512):
                size = min(512, width - start)
                cols = pl.ds(start, size)
                branch = jnp.dot(
                    source, wx[:, pl.ds(start - low, size)], preferred_element_type=jnp.float32
                )
                kept = blocks_at(stage, i, 2, cols).astype(jnp.float32)
                now = jnp.where(active, kept + branch, kept).astype(jnp.bfloat16)
                stage[pl.ds(i, 2), :, cols] = now.reshape(2, BLOCK, size)

            @pl.when(i == half)
            def _():
                relay(half + 3)

            total = scale(i, 2, low, width)
            multiply(slot, 2, low, width, False)
            if low:
                for j in range(2):
                    low_copy(i + j, low).wait_recv()
                total = total + scale(i, 2, 0, low)
                multiply(slot, 2, 0, low, True)
            keep_squares(slot, 2, total)
            for j in range(2):
                send_partial(i + j, slot + j)

        def update(i):
            attended_copy(i, other_rows).wait_recv()
            added(
                att[i],
                wo,
                stage.at[i],
                depths(i) > 1,
                out.at[token_rows(i)],
                span,
                width,
                0,
                -span,
            )

        def attend(i, slot):
            attend_rows(i, slot)
            branch_copy(i, own_rows).start()
            attended_copy(i, own_rows).start()

        def early(t, carry):
            for distance in range(1, chips):

                @pl.when(t == min(distance - 1, half - 2))
                def _():
                    for chunk in range(CHUNKS):
                        pass_on(1, distance, chunk)

            @pl.when(t == half - 2)
            def _():
                for j in range(2):
                    relay(half + j)

            first_half(t, t % 2)

            @pl.when(t == half - 2)
            def _():
                relay(half + 2)
                for chunk in range(CHUNKS):
                    collect(1, chunk)

            second_half(t, t % 2)

            @pl.when(t > 0)
            def _():
                attend(t - 1, (t - 1) % 2)

            return carry

        lax.fori_loop(0, half - 1, early, 0)
        load_wo.wait()
        update(0)
        gathered(1)
        for i in range(half):
            rest_copy(i).wait()

        def pair(t, carry):
            late(half + 2 * t, 2 - 2 * t)

            @pl.when(t == 0)
            def _():
                attend(half - 2, (half - 2) % 2)
                update(1)

            return carry

        lax.fori_loop(0, half // 2, pair, 0)
        def next_part(part):
            high_part(part).wait_recv()
            first = span + part * (span // 2)
            total = squares[4][:, :1] + scale(half - 1, 1, first, first + span // 2)
            multiply(4, 1, first, first + span // 2, True)
            keep_squares(4, 1, total)

        def last(t, carry):
            i = jnp.where(t < half, half + t, half - 1)

            @pl.when(t == 2)
            def _():
                first_half(half - 1, 4)
                for part in range(2):
                    next_part(part)
                send_partial(half - 1, 4)

            attend_rows(i, jnp.where(t < half, (t + 2) % 4, 4))

            for j, when in ((MICRO - 1, half - 1), (half - 1, half)):

                @pl.when(t == when)
                def _():
                    corner_copy(j, own_rows).start()

            branch_copy(i, own_rows).start()

            @pl.when(t == 2)
            def _():
                attended_copy(i, own_rows).start()

            @pl.when(t == half - 1)
            def _():
                update(half - 2)

            return carry

        lax.fori_loop(0, half + 1, last, 0)
        for j in (half + 3, half - 1):
            attended_copy(j, own_rows).start()
        settle_weights(1)
        sent(psend, p_send, p_recv)
        sent(stage.at[pl.ds(half, half)], h_send, h_recv)
        sent(att_in.at[pl.ds(half, half), own_rows], x_send, x_recv)
        lax.fori_loop(half, MICRO, lambda i, carry: update(i), None)
        update(half - 1)
        sent(att.at[:, own_rows], r_send, r_recv)
        sent(att.at[pl.ds(0, MICRO - 2), own_rows], a_send, a_recv)
        for i in (MICRO - 1, half - 1):
            corner_copy(i, own_rows).wait_send()

    @pl.when(seg == 0)
    def _():
        first_layer()

    @pl.when(seg == 1)
    def _():
        second_layer()


def cycle_of_two(chips, hidden, exit_layer, lengths, kv_cache, norm_gain, w_qkv, w_out):
    shards = 2
    width = w_qkv.shape[1]
    columns = w_qkv.shape[2]
    query_width = w_out.shape[1]
    head_size = (columns - query_width) // 2
    heads = query_width // head_size
    rows = BLOCK // shards
    span = width // 2
    wide = span + span * 5 // 8
    tokens = exit_layer.shape[0]
    hbm = pl.BlockSpec(memory_space=pltpu.HBM)
    vmem = pl.BlockSpec(memory_space=pltpu.VMEM)
    one = pltpu.SemaphoreType.DMA
    few = pltpu.SemaphoreType.DMA((MICRO // 2,))
    dma = pltpu.SemaphoreType.DMA((MICRO,))
    pieces = pltpu.SemaphoreType.DMA((chips, CHUNKS))
    bf16 = jnp.bfloat16
    return pl.pallas_call(
        functools.partial(cycle_kernel, (shards, head_size, heads)),
        out_shape=pltpu.VMEM((MICRO * BLOCK, span), bf16),
        in_specs=[hbm, vmem, vmem, hbm, vmem, hbm, hbm],
        out_specs=vmem,
        scratch_shapes=[
            pltpu.VMEM(w_qkv.shape[1:], bf16),
            pltpu.VMEM(w_out.shape[1:], bf16),
            pltpu.VMEM(kv_cache.shape[1:], bf16),
            pltpu.VMEM((MICRO, BLOCK, width), bf16),
            pltpu.VMEM((MICRO, BLOCK, width), bf16),
            pltpu.VMEM((MICRO * BLOCK, 128), jnp.int32),
            pltpu.VMEM((2 * BLOCK, width), bf16),
            pltpu.VMEM((5, BLOCK, columns), jnp.float32),
            pltpu.VMEM((5, BLOCK, 128), jnp.float32),
            pltpu.VMEM((MICRO, rows, columns + 128), bf16),
            pltpu.VMEM((MICRO, rows, columns + 128), bf16),
            pltpu.VMEM((MICRO, BLOCK, query_width), bf16),
            pltpu.VMEM((query_width, wide), bf16),
            pltpu.VMEM((MICRO, BLOCK, query_width), bf16),
            pltpu.SemaphoreType.DMA((3,)),
            few,
            one,
            pltpu.SemaphoreType.DMA((CHUNKS,)),
            pltpu.SemaphoreType.DMA((chips,)),
            pieces,
            pltpu.SemaphoreType.DMA((chips,)),
            pieces,
            one,
            one,
            one,
            few,
            pltpu.SemaphoreType.DMA((2,)),
            pltpu.SemaphoreType.DMA((MICRO + 1,)),
            one,
            pltpu.SemaphoreType.DMA((MICRO // 2 + 1,)),
            one,
            dma,
            one,
            dma,
            one,
            dma,
            pltpu.SemaphoreType.DMA((2,)),
            pltpu.SemaphoreType.DMA((2,)),
            one,
            dma,
            one,
        ],
        compiler_params=pltpu.CompilerParams(
            collective_id=0, has_side_effects=True, vmem_limit_bytes=VMEM_LIMIT
        ),
        name="cycle",
    )(
        hidden[0],
        exit_layer.reshape(1, tokens),
        lengths.reshape(1, tokens),
        kv_cache[0],
        norm_gain,
        w_qkv[0],
        w_out[0],
    )


def chosen(batches, devices, *arguments):
    shards = max(2, devices // 4)
    if shards == 2 and devices // shards == 2:
        return cycle_of_two(batches // 2, *arguments)
    return body(*arguments)


def solution(mesh):
    return jax.shard_map(
        functools.partial(chosen, mesh.shape["blk"], mesh.shape["section"]),
        mesh=mesh,
        in_specs=(
            P("section", "blk", None),
            P("blk"),
            P("blk"),
            P("section", "blk", None, None),
            P("section", None),
            P("section", None, None),
            P("section", None, None),
        ),
        out_specs=P("blk", "section"),
        check_vma=False,
    )
```
